128 devices in a mesh: tp: 4 (over x), fsdp: 32 (over z, y, core).
Axes of the slice: x: 4, y: 4, z: 4, core: 2. Of those that a mesh axis runs over, the one named last changes fastest.
Arguments:
- x_in: bfloat16 [384, 256, 768], P('fsdp')
- dy_out: bfloat16 [384, 256, 768], P('fsdp')
- ln_gain: float32 [768], P('fsdp')
- w_q: bfloat16 [768, 768], P('fsdp', 'tp')
- w_k: bfloat16 [768, 64], P('fsdp')
- w_v: bfloat16 [768, 64], P('fsdp')
- w_o: bfloat16 [768, 768], P('tp', 'fsdp')
- w_gate: bfloat16 [768, 3072], P('fsdp', 'tp')
- w_up: bfloat16 [768, 3072], P('fsdp', 'tp')
- w_down: bfloat16 [3072, 768], P('tp', 'fsdp')
Outputs:
- output 1: bfloat16 [384, 256, 768], P('fsdp')
- output 2: bfloat16 [384, 256, 768], P('fsdp')
- output 3: float32 [768], P('fsdp')
- output 4: float32 [768, 768], P('fsdp', 'tp')
- output 5: float32 [768, 64], P('fsdp')
- output 6: float32 [768, 64], P('fsdp')
- output 7: float32 [768, 768], P('tp', 'fsdp')
- output 8: float32 [768, 3072], P('fsdp', 'tp')
- output 9: float32 [768, 3072], P('fsdp', 'tp')
- output 10: float32 [3072, 768], P('tp', 'fsdp')
All inputs are finite; a program needn't handle non-finite values.
Results may differ from the reference program's by a relative error of at most 0.0154874.
Values are sent between devices in bfloat16 or wider.
A program may use at most 1 GiB of HBM per device.

```python
import math
import jax
import jax.numpy as jnp
from jax import lax

D_MODEL = 768
N_HEADS = 12
HEAD_DIM = 64
D_FF = 3072
N_BATCH = 384
SEQ_LEN = 256


def setup_inputs(seed: int = 0) -> dict:
    keys = jax.random.split(jax.random.key(seed), 10)
    inner = N_HEADS * HEAD_DIM
    scale_model = 1.0 / math.sqrt(D_MODEL)

    def draw_normal(slot, shape, scale):
        return (jax.random.normal(keys[slot], shape, jnp.float32) * scale).astype(jnp.bfloat16)

    return {
        'x_in': draw_normal(0, (N_BATCH, SEQ_LEN, D_MODEL), 1.0),
        'dy_out': draw_normal(1, (N_BATCH, SEQ_LEN, D_MODEL), 1.0),
        'ln_gain': jax.random.uniform(keys[2], (D_MODEL,), jnp.float32, 0.5, 1.5),
        'w_q': draw_normal(3, (D_MODEL, inner), scale_model),
        'w_k': draw_normal(4, (D_MODEL, HEAD_DIM), scale_model),
        'w_v': draw_normal(5, (D_MODEL, HEAD_DIM), scale_model),
        'w_o': draw_normal(6, (inner, D_MODEL), 1.0 / math.sqrt(inner)),
        'w_gate': draw_normal(7, (D_MODEL, D_FF), scale_model),
        'w_up': draw_normal(8, (D_MODEL, D_FF), scale_model),
        'w_down': draw_normal(9, (D_FF, D_MODEL), 1.0 / math.sqrt(D_FF)),
    }


def to_bf16(vals):
    return vals.astype(jnp.bfloat16).astype(jnp.float32)


def layer_norm(x_f32, gain):
    x_mean = jnp.mean(x_f32, axis=-1, keepdims=True)
    x_cent = x_f32 - x_mean
    x_var = jnp.mean(x_cent * x_cent, axis=-1, keepdims=True)
    return to_bf16(x_cent * lax.rsqrt(x_var + 1e-5) * gain)


def rope_tables():
    half_dim = HEAD_DIM // 2
    inv_freq = jnp.power(10000.0, -2.0 * jnp.arange(half_dim, dtype=jnp.float32) / HEAD_DIM)
    angle = jnp.arange(SEQ_LEN, dtype=jnp.float32)[:, None] * inv_freq[None, :]
    return jnp.cos(angle), jnp.sin(angle)


def rotate(vals, cos_t, sin_t):
    half_dim = vals.shape[-1] // 2
    first = vals[..., :half_dim]
    second = vals[..., half_dim:]
    return jnp.concatenate([first * cos_t - second * sin_t, second * cos_t + first * sin_t], axis=-1)


def attend_rows(q_rot, k_rot, v_val):
    causal = lax.broadcasted_iota(jnp.int32, (SEQ_LEN, SEQ_LEN), 0) >= lax.broadcasted_iota(jnp.int32, (SEQ_LEN, SEQ_LEN), 1)

    def one_head(q_head, k_row, v_row):
        scores = jnp.dot(q_head, k_row.T, preferred_element_type=jnp.float32)
        scores = jnp.where(causal, scores, -1e30)
        row_max = lax.stop_gradient(jnp.max(scores, axis=-1, keepdims=True))
        exp_val = jnp.exp(scores - row_max)
        att_prob = to_bf16(exp_val / jnp.sum(exp_val, axis=-1, keepdims=True))
        return to_bf16(jnp.dot(att_prob, v_row, preferred_element_type=jnp.float32))

    head_step = jax.checkpoint(one_head)

    def one_row(row):
        q_row, k_row, v_row = row

        def per_head(q_head):
            return head_step(q_head, k_row, v_row)

        head_outs = lax.map(per_head, jnp.swapaxes(q_row, 0, 1))
        return jnp.swapaxes(head_outs, 0, 1)

    return lax.map(one_row, (q_rot, k_rot, v_val))


def layer_forward(x_f32, gain, w_q, w_k, w_v, w_o, w_gate, w_up, w_down):
    n_batch = x_f32.shape[0]
    h_norm = layer_norm(x_f32, gain)
    q_raw = to_bf16(jnp.einsum('bsd,de->bse', h_norm, w_q))
    k_raw = to_bf16(jnp.einsum('bsd,de->bse', h_norm, w_k))
    v_val = to_bf16(jnp.einsum('bsd,de->bse', h_norm, w_v))
    gate_val = to_bf16(jnp.einsum('bsd,df->bsf', h_norm, w_gate))
    up_val = to_bf16(jnp.einsum('bsd,df->bsf', h_norm, w_up))
    cos_t, sin_t = rope_tables()
    q_heads = q_raw.reshape(n_batch, SEQ_LEN, N_HEADS, HEAD_DIM)
    q_rot = to_bf16(rotate(q_heads, cos_t[:, None, :], sin_t[:, None, :]) * (1.0 / math.sqrt(HEAD_DIM)))
    k_rot = to_bf16(rotate(k_raw, cos_t, sin_t))
    att_out = attend_rows(q_rot, k_rot, v_val).reshape(n_batch, SEQ_LEN, N_HEADS * HEAD_DIM)
    mlp_act = to_bf16(jax.nn.silu(gate_val) * up_val)
    branch = jnp.einsum('bse,ed->bsd', att_out, w_o) + jnp.einsum('bsf,fd->bsd', mlp_act, w_down)
    return x_f32 + branch


def reference(x_in, dy_out, ln_gain, w_q, w_k, w_v, w_o, w_gate, w_up, w_down):
    y_f32, pullback = jax.vjp(layer_forward, x_in.astype(jnp.float32), ln_gain, w_q.astype(jnp.float32), w_k.astype(jnp.float32), w_v.astype(jnp.float32), w_o.astype(jnp.float32), w_gate.astype(jnp.float32), w_up.astype(jnp.float32), w_down.astype(jnp.float32))
    gradients = pullback(dy_out.astype(jnp.float32))
    return (y_f32.astype(jnp.bfloat16), gradients[0].astype(jnp.bfloat16), gradients[1], gradients[2], gradients[3], gradients[4], gradients[5], gradients[6], gradients[7], gradients[8])
```

```python
import math
import jax
import jax.numpy as jnp
from jax import lax
from jax.sharding import PartitionSpec as P


def layer_norm(x_f32, gain):
    x_mean = jnp.mean(x_f32, axis=-1, keepdims=True)
    x_cent = x_f32 - x_mean
    x_var = jnp.mean(x_cent * x_cent, axis=-1, keepdims=True)
    return (x_cent * lax.rsqrt(x_var + 1e-5) * gain).astype(jnp.bfloat16)


def rotate(vals, cos_t, sin_t):
    half_dim = vals.shape[-1] // 2
    first = vals[..., :half_dim]
    second = vals[..., half_dim:]
    return jnp.concatenate([first * cos_t - second * sin_t, second * cos_t + first * sin_t], axis=-1)


def qk_post(q_raw, k_raw):
    seq_len = k_raw.shape[1]
    head_dim = k_raw.shape[2]
    half_dim = head_dim // 2
    inv_freq = jnp.power(10000.0, -2.0 * jnp.arange(half_dim, dtype=jnp.float32) / head_dim)
    angle = jnp.arange(seq_len, dtype=jnp.float32)[:, None] * inv_freq[None, :]
    cos_t = jnp.cos(angle)
    sin_t = jnp.sin(angle)
    q_rot = rotate(q_raw.astype(jnp.float32), cos_t[:, None, :], sin_t[:, None, :]) * (1.0 / math.sqrt(head_dim))
    k_rot = rotate(k_raw.astype(jnp.float32), cos_t, sin_t)
    return q_rot.astype(jnp.bfloat16), k_rot.astype(jnp.bfloat16)


def attend(q_rot, k_rot, v_val):
    seq_len = q_rot.shape[1]
    causal = lax.broadcasted_iota(jnp.int32, (seq_len, 1, seq_len), 0) >= lax.broadcasted_iota(jnp.int32, (seq_len, 1, seq_len), 2)
    scores = jnp.einsum('crie,cle->cril', q_rot, k_rot, preferred_element_type=jnp.float32)
    scores = jnp.where(causal, scores, -1e30)
    row_max = lax.stop_gradient(jnp.max(scores, axis=-1, keepdims=True))
    exp_val = jnp.exp(scores - row_max)
    att_prob = (exp_val / jnp.sum(exp_val, axis=-1, keepdims=True)).astype(jnp.bfloat16)
    return jnp.einsum('cril,cle->crie', att_prob, v_val, preferred_element_type=jnp.float32).astype(jnp.bfloat16)


def swiglu(gate_val, up_val):
    return (jax.nn.silu(gate_val.astype(jnp.float32)) * up_val.astype(jnp.float32)).astype(jnp.bfloat16)


def matmul_f32(form, left, right):
    return jnp.einsum(form, left, right, preferred_element_type=jnp.float32)


def solution(mesh):
    n_tp = mesh.shape['tp']
    n_fsdp = mesh.shape['fsdp']
    both = ('tp', 'fsdp')

    def device_step(x_in, dy_out, ln_gain, w_q, w_k, w_v, w_o, w_gate, w_up, w_down):
        bf16 = jnp.bfloat16
        f32 = jnp.float32
        n_batch, seq_len, width = x_in.shape
        head_dim = w_k.shape[1]
        rows = w_q.shape[0]
        nq = w_q.shape[1]
        nf = w_gate.shape[1]
        mine = n_batch // n_tp
        tp = lax.axis_index('tp')
        gain_hi = lax.reduce_precision(ln_gain, 8, 7)
        gain_mid = lax.reduce_precision(ln_gain - gain_hi, 8, 7)
        gain_lo = ln_gain - gain_hi - gain_mid
        gain_cols = jnp.stack([gain_hi, gain_mid, gain_lo], axis=1).astype(bf16)
        packed = jnp.concatenate([w_q, w_gate, w_up, w_o.T, w_down.T, w_k, w_v, jnp.pad(gain_cols, ((0, 0), (0, 125)))], axis=1)
        cuts = [0, nq, nq + nf, nq + 2 * nf, 2 * nq + 2 * nf, 2 * nq + 3 * nf]
        last = cuts[-1]
        full = lax.all_gather(packed, both, axis=0, tiled=True).reshape(n_tp, n_fsdp * rows, packed.shape[1])
        wq_t = full[:, :, cuts[0]:cuts[1]]
        wg_t = full[:, :, cuts[1]:cuts[2]]
        wu_t = full[:, :, cuts[2]:cuts[3]]
        wo_t = full[:, :, cuts[3]:cuts[4]]
        wd_t = full[:, :, cuts[4]:cuts[5]]
        wk_full = full[0, :, last:last + head_dim]
        wv_full = full[0, :, last + head_dim:last + 2 * head_dim]
        gain3 = full[0, :, last + 2 * head_dim:last + 2 * head_dim + 3].astype(f32)
        gain_full = gain3[:, 0] + gain3[:, 1] + gain3[:, 2]

        x_my = lax.dynamic_slice_in_dim(x_in, tp * mine, mine, 0)
        dy_my = lax.dynamic_slice_in_dim(dy_out, tp * mine, mine, 0)
        tokens = mine * seq_len
        x_f32 = x_my.reshape(tokens, width).astype(f32)
        dy_tok = dy_my.reshape(tokens, width)
        h_norm, norm_pull = jax.vjp(layer_norm, x_f32, gain_full)
        q_raw = matmul_f32('md,tde->mte', h_norm, wq_t).astype(bf16)
        k_raw = matmul_f32('md,de->me', h_norm, wk_full).astype(bf16)
        v_val = matmul_f32('md,de->me', h_norm, wv_full).astype(bf16)
        gate_val = matmul_f32('md,tdf->tmf', h_norm, wg_t).astype(bf16)
        up_val = matmul_f32('md,tdf->tmf', h_norm, wu_t).astype(bf16)
        q_heads = q_raw.reshape(mine, seq_len, -1, head_dim)
        (q_rot, k_rot), rope_pull = jax.vjp(qk_post, q_heads, k_raw.reshape(mine, seq_len, head_dim))
        att_out, att_pull = jax.vjp(attend, q_rot, k_rot, v_val.reshape(mine, seq_len, head_dim))
        mlp_act, act_pull = jax.vjp(swiglu, gate_val, up_val)
        att_flat = att_out.reshape(tokens, n_tp, nq)
        branch = matmul_f32('mte,tde->md', att_flat, wo_t) + matmul_f32('tmf,tdf->md', mlp_act, wd_t)
        y_my = (x_f32 + branch).astype(bf16).reshape(mine, seq_len, width)
        y_out = lax.all_gather(y_my, 'tp', axis=0, tiled=True)

        d_att = matmul_f32('md,tde->mte', dy_tok, wo_t).astype(bf16).reshape(mine, seq_len, -1, head_dim)
        d_act = matmul_f32('md,tdf->tmf', dy_tok, wd_t).astype(bf16)
        d_gate, d_up = act_pull(d_act)
        d_qrot, d_krot, d_val = att_pull(d_att)
        d_qraw, d_kraw = rope_pull((d_qrot, d_krot))
        d_qflat = d_qraw.reshape(tokens, n_tp, nq)
        d_kflat = d_kraw.reshape(tokens, head_dim)
        d_vflat = d_val.reshape(tokens, head_dim)
        dh_full = (matmul_f32('mte,tde->md', d_qflat, wq_t) + matmul_f32('tmf,tdf->md', d_gate, wg_t) + matmul_f32('tmf,tdf->md', d_up, wu_t)
                   + matmul_f32('me,de->md', d_kflat, wk_full) + matmul_f32('me,de->md', d_vflat, wv_full)).astype(bf16)
        dx_norm, gain_part = norm_pull(dh_full)
        gx_my = (dy_tok.astype(f32) + dx_norm).astype(bf16).reshape(mine, seq_len, width)
        grad_x = lax.all_gather(gx_my, 'tp', axis=0, tiled=True)
        g_q = matmul_f32('md,mte->dte', h_norm, d_qflat)
        g_g = matmul_f32('md,tmf->dtf', h_norm, d_gate)
        g_u = matmul_f32('md,tmf->dtf', h_norm, d_up)
        g_o = matmul_f32('md,mte->dte', dy_tok, att_flat)
        g_d = matmul_f32('md,tmf->dtf', dy_tok, mlp_act)
        g_k = matmul_f32('md,me->de', h_norm, d_kflat)
        g_v = matmul_f32('md,me->de', h_norm, d_vflat)
        small = jnp.concatenate([g_k, g_v, jnp.pad(gain_part[:, None], ((0, 0), (0, 127)))], axis=1)
        small = jnp.broadcast_to(small[:, None], (width, n_tp, small.shape[1]))
        g_all = jnp.concatenate([g_q, g_g, g_u, g_o, g_d, small], axis=2).reshape(width, -1)
        g_row = lax.psum_scatter(g_all, 'fsdp', scatter_dimension=0, tiled=True)
        g_row = jnp.swapaxes(g_row.reshape(rows, n_tp, -1), 0, 1).reshape(n_tp * rows, -1)
        g_loc = lax.psum_scatter(g_row, 'tp', scatter_dimension=0, tiled=True)
        grad_wq = g_loc[:, cuts[0]:cuts[1]]
        grad_wgate = g_loc[:, cuts[1]:cuts[2]]
        grad_wup = g_loc[:, cuts[2]:cuts[3]]
        grad_wo = g_loc[:, cuts[3]:cuts[4]].T
        grad_wdown = g_loc[:, cuts[4]:cuts[5]].T
        grad_wk = g_loc[:, last:last + head_dim]
        grad_wv = g_loc[:, last + head_dim:last + 2 * head_dim]
        grad_gain = g_loc[:, last + 2 * head_dim]
        return (y_out, grad_x, grad_gain, grad_wq, grad_wk, grad_wv, grad_wo, grad_wgate, grad_wup, grad_wdown)

    act_spec = P('fsdp', None, None)
    row_spec = P('fsdp', 'tp')
    kv_spec = P('fsdp', None)
    col_spec = P('tp', 'fsdp')
    in_specs = (act_spec, act_spec, P('fsdp'), row_spec, kv_spec, kv_spec, col_spec, row_spec, row_spec, col_spec)
    out_specs = (act_spec, act_spec, P('fsdp'), row_spec, kv_spec, kv_spec, col_spec, row_spec, row_spec, col_spec)
    return jax.shard_map(device_step, mesh=mesh, in_specs=in_specs, out_specs=out_specs, check_vma=False)
```

```python
import jax
import jax.numpy as jnp
from jax import lax
from jax.sharding import PartitionSpec as P
from jax.experimental import pallas as pl
from jax.experimental.pallas import tpu as pltpu


N0, N1, N2, N3 = range(4)
RING = 4
SUB = 8
LANES = 128
PAIR = 256
KIB = 1024
ALL = Ellipsis
KV_AT = 1152
MESH_ID = pl.DeviceIdType.MESH


def gather_kernel(p_ref, g_ref, lsem, s1, r1, s2, r2, s3, r3, ds, dr):
    t = lax.axis_index('tp')
    f = lax.axis_index('fsdp')
    c = lax.rem(f, N2)
    at = {'x': t, 'y': lax.rem(lax.div(f, N2), RING), 'z': lax.div(f, SUB)}

    def up(i, d):
        return lax.rem(i + d, RING)

    def dev(where, cc):
        return {'tp': where['x'], 'fsdp': (where['z'] * RING + where['y']) * N2 + cc}

    def peer(axis, d):
        return dev({**at, axis: up(at[axis], d)}, c)

    partner = dev(at, N1 - c)
    barrier = pltpu.get_barrier_semaphore()
    greeted = [partner] + [peer(axis, d) for axis in 'xyz' for d in (N1, N2, N3)]
    for who in greeted:
        pl.semaphore_signal(barrier, inc=N1, device_id=who, device_id_type=MESH_ID)
    own = pltpu.make_async_copy(p_ref, g_ref.at[:, at['x'], at['z'], at['y'], c], lsem.at[N0])
    own.start()
    pl.semaphore_wait(barrier, len(greeted))

    sent = []

    def push(src, dst, s_sem, r_sem, who):
        copy = pltpu.make_async_remote_copy(src_ref=src, dst_ref=dst, send_sem=s_sem, recv_sem=r_sem, device_id=who, device_id_type=MESH_ID)
        copy.start()
        sent.append(copy)

    def landed(ref, s_sem, r_sem):
        pltpu.make_async_remote_copy(src_ref=ref, dst_ref=ref, send_sem=s_sem, recv_sem=r_sem, device_id=partner, device_id_type=MESH_ID).wait_recv()

    def view(k, h, fixed, core):
        spot = [fixed.get(axis, slice(None)) for axis in 'xzy']
        return g_ref.at[h, spot[N0], spot[N1], spot[N2], core, k]

    orders = ('xyz', 'yzx', 'zxy')
    both = slice(None)
    across = []

    def share(k, h, fixed, n):
        push(view(k, h, fixed, c), view(k, h, fixed, c), ds.at[k, n], dr.at[k, n], partner)
        across.append((k, h, fixed, n))

    def ring_start(k, axis, fixed, ss, rr):
        here = {**fixed, axis: at[axis]}
        for n in range(N2):
            push(view(k, n, here, c), view(k, n, here, c), ss.at[k, n], rr.at[k, n], peer(axis, N1))
            push(view(k, N1 - n, here, c), view(k, N1 - n, here, c), ss.at[k, N3 - n], rr.at[k, N3 - n], peer(axis, N3))

    def ring_forward(k, axis, fixed, ss, rr):
        for h, d, n in ((N0, N3, N0), (N1, N1, N3)):
            there = {**fixed, axis: up(at[axis], d)}
            landed(view(k, h, there, c), ss.at[k, n], rr.at[k, n])
            push(view(k, h, there, c), view(k, h, there, c), ss.at[k, RING + h], rr.at[k, RING + h], peer(axis, RING - d))

    def ring_share(k, axis, fixed, ss, rr, base):
        for m, (h, d, n) in enumerate(((N0, N3, N0), (N1, N1, N3), (N1, N3, N1), (N0, N1, N2), (N0, N2, RING), (N1, N2, 5))):
            there = {**fixed, axis: up(at[axis], d)}
            if n not in (N0, N3):
                landed(view(k, h, there, c), ss.at[k, n], rr.at[k, n])
            share(k, h, there, base + m)

    for k, order in enumerate(orders):
        for d in (N1, N3, N2):
            push(p_ref.at[:, k], view(k, both, at, c), s1.at[k, d - N1], r1.at[k, d - N1], peer(order[N0], d))
    own.wait()
    second = []
    third = []
    for k, order in enumerate(orders):
        for d in (N1, N3, N2):
            landed(view(k, both, {**at, order[N0]: up(at[order[N0]], RING - d)}, c), s1.at[k, d - N1], r1.at[k, d - N1])
        fixed = {order[N2]: at[order[N2]]}
        second.append((k, order[N1], fixed, s2, r2))
        third.append((k, order[N2], {}, s3, r3))
        ring_start(*second[k])
    for k, order in enumerate(orders):
        here = {order[N1]: at[order[N1]], order[N2]: at[order[N2]]}
        share(k, N0, here, N0)
        share(k, N1, here, N1)
    for k in range(N3):
        ring_forward(*second[k])
    for k in range(N3):
        ring_share(*second[k], N2)
        ring_start(*third[k])
    for k in range(N3):
        ring_forward(*third[k])
    for k in range(N3):
        ring_share(*third[k], SUB)
    for k, h, fixed, n in across:
        landed(view(k, h, fixed, N1 - c), ds.at[k, n], dr.at[k, n])
    for copy in sent:
        copy.wait_send()


def gather_weights(packed):
    dma = pltpu.SemaphoreType.DMA
    any_spec = pl.BlockSpec(memory_space=pl.ANY)
    wide = packed.shape[N2]
    return pl.pallas_call(
        gather_kernel,
        name='gather_weights',
        out_shape=jax.ShapeDtypeStruct((N2, RING, RING, RING, N2, N3, SUB, wide), packed.dtype),
        in_specs=[any_spec],
        out_specs=any_spec,
        scratch_shapes=[dma((N1,)), dma((N3, N3)), dma((N3, N3)), dma((N3, 6)), dma((N3, 6)), dma((N3, 6)), dma((N3, 6)), dma((N3, 14)), dma((N3, 14))],
        compiler_params=pltpu.CompilerParams(collective_id=N2, has_side_effects=True, vmem_limit_bytes=32 * KIB * KIB),
    )(packed.reshape(N2, N3, SUB, wide))


NT = (((N1,), (N1,)), ((), ()))
NN = (((N1,), (N0,)), ((), ()))
TN = (((N0,), (N0,)), ((), ()))


def dot(left, right, dims=NN):
    return lax.dot_general(left, right, dims, preferred_element_type=jnp.float32)


def proj_kernel(x_ref, dy_ref, gain_ref, w0_ref, w1_ref, wkv_ref, h_out, q_out, kv_out, do_out, act_out, dg_out, du_out):
    f32 = jnp.float32
    bf16 = jnp.bfloat16
    tokens = x_ref.shape[N0]

    @pl.when(pl.program_id(N0) == N0)
    def _():
        def norm(n, carry):
            at = pl.ds(n * LANES, LANES)
            x_f32 = x_ref[at, :].astype(f32)
            x_cent = x_f32 - jnp.mean(x_f32, axis=-N1, keepdims=True)
            x_var = jnp.mean(x_cent * x_cent, axis=-N1, keepdims=True)
            h_out[at, :] = (x_cent * lax.rsqrt(x_var + 1e-5) * gain_ref[ALL]).astype(bf16)
            return carry
        lax.fori_loop(N0, tokens // LANES, norm, N0)
        kv_out[ALL] = dot(h_out[ALL], wkv_ref[ALL]).astype(bf16)

    for n in range(N3):
        cols = slice(n * PAIR, n * PAIR + PAIR)
        gate = dot(h_out[ALL], w0_ref[N0, N0, :, cols]).astype(bf16).astype(f32)
        up = dot(h_out[ALL], w1_ref[N0, N0, :, cols]).astype(bf16).astype(f32)
        if n == N0:
            d_low = dot(dy_ref[ALL], w0_ref[N0, N0, :, 1280:1408])
            d_act = jnp.concatenate([d_low, dot(dy_ref[ALL], w1_ref[N0, N0, :, 768:896])], axis=N1)
        else:
            d_act = dot(dy_ref[ALL], w1_ref[N0, N0, :, 640 + n * PAIR:896 + n * PAIR])
        d_act = d_act.astype(bf16).astype(f32)
        sig = jax.nn.sigmoid(gate)
        silu = gate * sig
        act_out[N0, :, cols] = (silu * up).astype(bf16)
        du_out[N0, :, cols] = (d_act * silu).astype(bf16)
        dg_out[N0, :, cols] = (d_act * up * (sig * (1.0 + gate * (1.0 - sig)))).astype(bf16)
    q_out[N0] = dot(h_out[ALL], w0_ref[N0, N0, :, 768:KIB]).astype(bf16)
    do_out[N0] = dot(dy_ref[ALL], w0_ref[N0, N0, :, 896:1152]).astype(bf16)


def att_kernel(q_ref, kv_ref, do_ref, cq_ref, sq_ref, ck_ref, sk_ref, o_out, dq_out, dkv_out, dk_lo, dk_hi, dv_lo, dv_hi):
    f32 = jnp.float32
    bf16 = jnp.bfloat16
    seq_len = kv_ref.shape[N0]
    lane = lax.broadcasted_iota(jnp.int32, (seq_len, LANES), N1)
    low = lane < 64
    first = lax.rem(lane, 64) < 32
    causal = lax.broadcasted_iota(jnp.int32, (seq_len, seq_len), N0) >= lax.broadcasted_iota(jnp.int32, (seq_len, seq_len), N1)

    def other(vals):
        return jnp.where(first, pltpu.roll(vals, 96, N1), pltpu.roll(vals, 32, N1))

    kv_f32 = kv_ref[ALL].astype(f32)
    kv_rot = kv_f32 * ck_ref[ALL] + other(kv_f32) * sk_ref[ALL]
    zero = jnp.zeros_like(kv_rot)
    k_lo = jnp.where(low, kv_rot, zero)
    v_hi = jnp.where(low, zero, kv_rot)
    k_hi = pltpu.roll(k_lo, 64, N1).astype(bf16)
    v_lo = pltpu.roll(v_hi, 64, N1).astype(bf16)
    k_lo = k_lo.astype(bf16)
    v_hi = v_hi.astype(bf16)
    for ref in (dk_lo, dk_hi, dv_lo, dv_hi):
        ref[ALL] = jnp.zeros_like(ref)

    def head(q_tile, k_part, v_part, do_tile):
        scores = jnp.where(causal, dot(q_tile, k_part, NT), -1e30)
        exp_val = jnp.exp(scores - jnp.max(scores, axis=-N1, keepdims=True))
        prob = exp_val / jnp.sum(exp_val, axis=-N1, keepdims=True)
        d_prob = dot(do_tile, v_part, NT).astype(bf16).astype(f32)
        d_score = prob * (d_prob - jnp.sum(d_prob * prob, axis=-N1, keepdims=True))
        return prob.astype(bf16), d_score.astype(bf16)

    def block(tt, carry):
        tiles = []
        for n in range(N2):
            cols = slice(n * LANES, n * LANES + LANES)
            vals = q_ref[tt, :, cols].astype(f32)
            tiles.append(((vals * cq_ref[ALL] + other(vals) * sq_ref[ALL]) * 0.125).astype(bf16))
        do0 = do_ref[tt, :, N0:LANES]
        do1 = do_ref[tt, :, LANES:PAIR]
        p0, s0 = head(tiles[N0], k_lo, v_hi, do0)
        p1, s1 = head(tiles[N0], k_hi, v_lo, do1)
        p2, s2 = head(tiles[N1], k_lo, v_hi, do1)
        o_out[tt, :, N0:LANES] = dot(p0, v_hi).astype(bf16)
        o_out[tt, :, LANES:PAIR] = (dot(p1, v_lo) + dot(p2, v_hi)).astype(bf16)
        dv_hi[ALL] += dot(p0, do0, TN) + dot(p2, do1, TN)
        dv_lo[ALL] += dot(p1, do1, TN)
        dk_lo[ALL] += dot(s0, tiles[N0], TN) + dot(s2, tiles[N1], TN)
        dk_hi[ALL] += dot(s1, tiles[N0], TN)
        for n, grad in ((N0, dot(s0, k_lo) + dot(s1, k_hi)), (N1, dot(s2, k_lo))):
            grad = grad.astype(bf16).astype(f32) * 0.125
            dq_out[tt, :, n * LANES:n * LANES + LANES] = (grad * cq_ref[ALL] - other(grad) * sq_ref[ALL]).astype(bf16)
        return carry
    lax.fori_loop(N0, q_ref.shape[N0], block, N0)
    dk = (dk_lo[ALL] + pltpu.roll(dk_hi[ALL], 64, N1)).astype(bf16).astype(f32)
    dk_raw = dk * ck_ref[ALL] - other(dk) * sk_ref[ALL]
    dv = dv_hi[ALL] + pltpu.roll(dv_lo[ALL], 64, N1)
    dkv_out[ALL] = jnp.where(low, dk_raw, dv).astype(bf16)


def back_kernel(x_ref, dy_ref, gain_ref, w0_ref, w1_ref, wkv_ref, o_ref, act_ref, dq_ref, dg_ref, du_ref, dkv_ref, y_out, gx_out, gain_out, y_acc, dh_acc):
    f32 = jnp.float32
    bf16 = jnp.bfloat16
    step = pl.program_id(N0)
    tokens = x_ref.shape[N0]
    y_part = dot(o_ref[N0], w0_ref[N0, N0, :, 896:1152], NT) + dot(act_ref[N0, :, N0:LANES], w0_ref[N0, N0, :, 1280:1408], NT) + dot(act_ref[N0, :, LANES:768], w1_ref[N0, N0, :, 768:1408], NT)
    dh_part = dot(dq_ref[N0], w0_ref[N0, N0, :, 768:KIB], NT) + dot(dg_ref[N0], w0_ref[N0, N0, :, N0:768], NT) + dot(du_ref[N0], w1_ref[N0, N0, :, N0:768], NT)

    @pl.when(step == N0)
    def _():
        y_acc[ALL] = y_part
        dh_acc[ALL] = dh_part + dot(dkv_ref[ALL], wkv_ref[ALL], NT)

    @pl.when(step > N0)
    def _():
        y_acc[ALL] += y_part
        dh_acc[ALL] += dh_part

    @pl.when(step == pl.num_programs(N0) - N1)
    def _():
        gain_out[ALL] = jnp.zeros_like(gain_out)

        def finish(n, carry):
            at = pl.ds(n * LANES, LANES)
            x_f32 = x_ref[at, :].astype(f32)
            y_out[at, :] = (x_f32 + y_acc[at, :]).astype(bf16)
            x_cent = x_f32 - jnp.mean(x_f32, axis=-N1, keepdims=True)
            rstd = lax.rsqrt(jnp.mean(x_cent * x_cent, axis=-N1, keepdims=True) + 1e-5)
            x_hat = x_cent * rstd
            dh = dh_acc[at, :].astype(bf16).astype(f32)
            gain_out[ALL] += jnp.sum(dh * x_hat, axis=N0, keepdims=True)
            d_hat = dh * gain_ref[ALL]
            dx = rstd * (d_hat - jnp.mean(d_hat, axis=-N1, keepdims=True) - x_hat * jnp.mean(d_hat * x_hat, axis=-N1, keepdims=True))
            gx_out[at, :] = (dy_ref[at, :].astype(f32) + dx).astype(bf16)
            return carry
        lax.fori_loop(N0, tokens // LANES, finish, N0)


def wgrad_kernel(ht_ref, dyt_ref, gcol_ref, o_ref, act_ref, dq_ref, dg_ref, du_ref, dkv_ref, own_out, oth_out):
    f32 = jnp.float32
    tt = pl.program_id(N0)
    lane = lax.broadcasted_iota(jnp.int32, (LANES, LANES), N1)

    def chunk(n, carry):
        at = pl.ds(n * LANES, LANES)
        for cls, out in ((N0, own_out), (N1, oth_out)):
            ht = ht_ref[cls, at, :]
            dyt = dyt_ref[cls, at, :]
            for k in range(N3):
                cols = slice(k * PAIR, k * PAIR + PAIR)
                out[N0, N0, at, cols] = dot(ht, dg_ref[N0, :, cols]).astype(out.dtype)
                out[N1, N0, at, cols] = dot(ht, du_ref[N0, :, cols]).astype(out.dtype)
            g_q = dot(ht, dq_ref[N0])
            g_o = dot(dyt, o_ref[N0])
            out[N0, N0, at, 768:896] = g_q[:, N0:LANES].astype(out.dtype)
            out[N0, N0, at, 896:KIB] = (g_q[:, LANES:PAIR] + g_o[:, N0:LANES]).astype(out.dtype)
            out[N0, N0, at, KIB:1152] = g_o[:, LANES:PAIR].astype(out.dtype)
            g_kv = pltpu.roll(dot(ht, dkv_ref[ALL]), lax.rem(LANES - 32 * tt, LANES), N1)
            out[N0, N0, at, 1152:1280] = (jnp.where(lane < 32, g_kv, 0.0) + gcol_ref[cls, at, :]).astype(out.dtype)
            out[N0, N0, at, 1280:1408] = dot(dyt, act_ref[N0, :, N0:LANES]).astype(out.dtype)
            for lo, hi in ((LANES, 384), (384, 640), (640, 768)):
                out[N1, N0, at, lo + 640:hi + 640] = dot(dyt, act_ref[N0, :, lo:hi]).astype(out.dtype)
        return carry
    lax.fori_loop(N0, N3, chunk, N0)


def layer_step(x_tok, dy_tok, gain_row, w_full, w_kv, core, seq_len, head_dim):
    f32 = jnp.float32
    bf16 = jnp.bfloat16
    tokens, width = x_tok.shape
    n_tp = w_full.shape[N1]
    wide = w_full.shape[N3]
    n_seq = tokens // seq_len
    half = width // N2

    def whole(shape):
        return pl.BlockSpec(shape, lambda i: (N0,) * len(shape))

    def per(shape):
        return pl.BlockSpec((N1,) + shape, lambda i: (i,) + (N0,) * len(shape))

    w0_spec = pl.BlockSpec((N1, N1, width, wide), lambda i: (N0, i, N0, N0))
    w1_spec = pl.BlockSpec((N1, N1, width, wide), lambda i: (N1, i, N0, N0))
    tok = whole((tokens, width))
    params = pltpu.CompilerParams(dimension_semantics=('arbitrary',), vmem_limit_bytes=56 * KIB * KIB)
    wide_t = jax.ShapeDtypeStruct((n_tp, tokens, width), bf16)
    pair_t = jax.ShapeDtypeStruct((n_tp, tokens, PAIR), bf16)
    row_t = jax.ShapeDtypeStruct((tokens, width), bf16)
    kv_t = jax.ShapeDtypeStruct((tokens, LANES), bf16)
    h_norm, q_raw, kv_raw, d_o, act, d_gate, d_up = pl.pallas_call(
        proj_kernel, name='proj', grid=(n_tp,),
        in_specs=[tok, tok, whole((N1, width)), w0_spec, w1_spec, whole((width, LANES))],
        out_specs=(tok, per((tokens, PAIR)), whole((tokens, LANES)), per((tokens, PAIR)), per((tokens, width)), per((tokens, width)), per((tokens, width))),
        out_shape=(row_t, pair_t, kv_t, pair_t, wide_t, wide_t, wide_t),
        compiler_params=params,
    )(x_tok, dy_tok, gain_row, w_full, w_full, w_kv)

    half_dim = head_dim // N2
    inv_freq = jnp.power(10000.0, -2.0 * jnp.arange(half_dim, dtype=f32) / head_dim)
    angle = jnp.arange(seq_len, dtype=f32)[:, None] * inv_freq[None, :]
    cos_t = jnp.cos(angle)
    sin_t = jnp.sin(angle)
    cos_h = jnp.concatenate([cos_t, cos_t], axis=N1)
    sin_h = jnp.concatenate([-sin_t, sin_t], axis=N1)
    cos_q = jnp.concatenate([cos_h, cos_h], axis=N1)
    sin_q = jnp.concatenate([sin_h, sin_h], axis=N1)
    cos_k = jnp.concatenate([cos_h, jnp.ones_like(cos_h)], axis=N1)
    sin_k = jnp.concatenate([sin_h, jnp.zeros_like(sin_h)], axis=N1)
    pair_spec = pl.BlockSpec((n_tp, seq_len, PAIR), lambda i: (N0, i, N0))
    kv_spec = pl.BlockSpec((seq_len, LANES), lambda i: (i, N0))
    table = whole((seq_len, LANES))
    att, d_q, d_kv = pl.pallas_call(
        att_kernel, name='attention', grid=(n_seq,),
        in_specs=[pair_spec, kv_spec, pair_spec, table, table, table, table],
        out_specs=(pair_spec, pair_spec, kv_spec),
        out_shape=(pair_t, pair_t, kv_t),
        scratch_shapes=[pltpu.VMEM((seq_len, LANES), f32)] * RING,
        compiler_params=params,
    )(q_raw, kv_raw, d_o, cos_q, sin_q, cos_k, sin_k)

    y_tok, gx_tok, gain_part = pl.pallas_call(
        back_kernel, name='back', grid=(n_tp,),
        in_specs=[tok, tok, whole((N1, width)), w0_spec, w1_spec, whole((width, LANES)), per((tokens, PAIR)), per((tokens, width)), per((tokens, PAIR)),
                  per((tokens, width)), per((tokens, width)), whole((tokens, LANES))],
        out_specs=(tok, tok, whole((N1, width))),
        out_shape=(row_t, row_t, jax.ShapeDtypeStruct((N1, width), f32)),
        scratch_shapes=[pltpu.VMEM((tokens, width), f32)] * N2,
        compiler_params=params,
    )(x_tok, dy_tok, gain_row, w_full, w_full, w_kv, att, act, d_q, d_gate, d_up, d_kv)

    def by_class(vals):
        vals = vals.reshape(16, N2, 24, vals.shape[N1])
        mine = lax.dynamic_index_in_dim(vals, core, N1, keepdims=False)
        theirs = lax.dynamic_index_in_dim(vals, N1 - core, N1, keepdims=False)
        return jnp.stack([mine, theirs]).reshape(N2, half, vals.shape[N3])

    h_t = by_class(h_norm.T)
    dy_t = by_class(dy_tok.T)
    gain_col = jnp.where(jnp.arange(LANES)[None, :] == 32, gain_part.reshape(width, N1), 0.0)
    gain_col = by_class(gain_col)
    class_spec = pl.BlockSpec((N2, N1, half, wide), lambda i: (N0, i, N0, N0))
    own, oth = pl.pallas_call(
        wgrad_kernel, name='wgrad', grid=(n_tp,),
        in_specs=[whole((N2, half, tokens)), whole((N2, half, tokens)), whole((N2, half, LANES)), per((tokens, PAIR)), per((tokens, width)), per((tokens, PAIR)),
                  per((tokens, width)), per((tokens, width)), whole((tokens, LANES))],
        out_specs=(class_spec, class_spec),
        out_shape=(jax.ShapeDtypeStruct((N2, n_tp, half, wide), f32), jax.ShapeDtypeStruct((N2, n_tp, half, wide), bf16)),
        compiler_params=params,
    )(h_t, dy_t, gain_col, att, act, d_q, d_gate, d_up, d_kv)
    return y_tok, gx_tok, own, oth


def sum_kernel(g_ref, gs_ref, gx_ref, w_out, kv_out, gx_out, acc, rp, sa, ra1, ra2, sb, rb1, rb2, sc, rc, kvx, gsem, d2s, d2r, ss, rs, cs, cr, ks, kr, xs, xr, lsem):
    f32 = jnp.float32
    bf16 = jnp.bfloat16
    t = lax.axis_index('tp')
    f = lax.axis_index('fsdp')
    c = lax.rem(f, N2)
    yy = lax.rem(lax.div(f, N2), RING)
    zz = lax.div(f, SUB)

    def dev(tt, zc, yc, cc):
        return {'tp': tt, 'fsdp': (zc * RING + yc) * N2 + cc}

    def up(i, d):
        return lax.rem(i + d, RING)

    partner = dev(t, zz, yy, N1 - c)
    xp = [dev(up(t, d), zz, yy, c) for d in range(RING)]
    z_dev = [dev(t, up(zz, d), yy, c) for d in range(RING)]
    y_dev = [dev(t, zz, up(yy, d), c) for d in range(RING)]
    barrier = pltpu.get_barrier_semaphore()
    peers = [partner, xp[N1], xp[N2], xp[N3], z_dev[N1], z_dev[N3], y_dev[N1], y_dev[N3]]
    for peer in peers:
        pl.semaphore_signal(barrier, inc=N1, device_id=peer, device_id_type=MESH_ID)

    def rcopy(src, dst, s_sem, r_sem, peer):
        return pltpu.make_async_remote_copy(src_ref=src, dst_ref=dst, send_sem=s_sem, recv_sem=r_sem, device_id=peer, device_id_type=MESH_ID)

    ring_a = [zz, yy]
    ring_b = [yy, zz]
    dev_a = [z_dev, y_dev]
    dev_b = [y_dev, z_dev]
    order = [N2, N1, N3, N0]

    def g_view(col, j):
        return g_ref.at[N0, :, j] if col == N0 else g_ref.at[N1, :, :, j]

    def gs_view(col, j):
        return gs_ref.at[N0, :, j] if col == N0 else gs_ref.at[N1, :, :, j]

    load = [[None] * RING for _ in range(N2)]
    pair = [[None] * RING for _ in range(N2)]
    for n, d in enumerate(order):
        for col in range(N2):
            j = up(ring_a[col], d)
            load[col][n] = pltpu.make_async_copy(g_view(col, j), acc.at[col, n], gsem.at[col, n])
            load[col][n].start()
    pl.semaphore_wait(barrier, len(peers))
    for n, d in enumerate(order):
        for col in range(N2):
            j = up(ring_a[col], d)
            pair[col][n] = rcopy(gs_view(col, j), rp.at[col, n], d2s.at[col, n], d2r.at[col, n], partner)
            pair[col][n].start()
    mine = gx_ref.shape[N0]
    my_rows = pl.ds(t * mine, mine)
    x_up = rcopy(gx_ref, gx_out.at[my_rows], xs.at[N0], xr.at[N0], xp[N1])
    x_dn = rcopy(gx_ref, gx_out.at[my_rows], xs.at[N1], xr.at[N1], xp[N3])
    x_up.start()
    x_dn.start()
    x_me = pltpu.make_async_copy(gx_ref, gx_out.at[my_rows], lsem.at[N0])
    x_me.start()

    def each(count, body):
        def step(n, carry):
            body(n)
            return carry
        lax.fori_loop(N0, count, step, N0)

    def arrived(col, n):
        load[col][n].wait()
        pair[col][n].wait_recv()

    sends = []

    def send(src, dst, s_sem, r_sem, peer):
        copy = rcopy(src, dst, s_sem, r_sem, peer)
        copy.start()
        sends.append(copy)
        return copy

    for col in range(N2):
        arrived(col, N0)

        def first(q, col=col):
            tt = lax.div(q, 12)
            a2 = lax.rem(lax.div(q, N3), RING)
            r = lax.rem(q, N3)
            sa[col, N0, a2, tt, r] = (acc[col, N0, tt, a2, r] + rp[col, N0, tt, a2, r].astype(f32)).astype(bf16)
        each(48, first)
        send(sa.at[col, N0, pl.ds(N0, N2)], ra1.at[col, N0], ss.at[col, N0], rs.at[col, N0], dev_a[col][N1])
        send(sa.at[col, N0, pl.ds(N2, N2)], ra1.at[col, N1], ss.at[col, N1], rs.at[col, N1], dev_a[col][N3])
    for col in range(N2):
        for n, base, peer in ((N1, N2, N1), (N2, N0, N3)):
            arrived(col, n)

            def plain(q, col=col, n=n, base=base):
                a2 = base + lax.div(q, 12)
                tt = lax.rem(lax.div(q, N3), RING)
                r = lax.rem(q, N3)
                sa[col, n, a2, tt, r] = (acc[col, n, tt, a2, r] + rp[col, n, tt, a2, r].astype(f32)).astype(bf16)
            each(24, plain)
            send(sa.at[col, n, pl.ds(base, N2)], ra2.at[col, n - N1, pl.ds(base, N2)], ss.at[col, n + N1], rs.at[col, n + N1], dev_a[col][peer])
    for col in range(N2):
        for n, base, peer in ((N1, N0, N1), (N2, N2, N3)):
            rcopy(sa.at[col, N0, pl.ds(N0, N2)], ra1.at[col, n - N1], ss.at[col, n - N1], rs.at[col, n - N1], dev_a[col][peer]).wait_recv()

            def joined(q, col=col, n=n, base=base):
                h = lax.div(q, 12)
                a2 = base + h
                tt = lax.rem(lax.div(q, N3), RING)
                r = lax.rem(q, N3)
                val = acc[col, n, tt, a2, r] + rp[col, n, tt, a2, r].astype(f32) + ra1[col, n - N1, h, tt, r].astype(f32)
                sa[col, n, a2, tt, r] = val.astype(bf16)
            each(24, joined)
            send(sa.at[col, n, pl.ds(base, N2)], ra2.at[col, n - N1, pl.ds(base, N2)], ss.at[col, n + N3], rs.at[col, n + N3], dev_a[col][peer])
    x_up.wait_recv()
    x_dn.wait_recv()
    from_dn = up(t, N3) * mine * N2
    from_up = up(t, N1) * mine * N2
    half_dn = gx_out.at[pl.ds(up(t, N3) * mine, mine), pl.ds(N0, LANES)]
    half_up = gx_out.at[pl.ds(up(t, N1) * mine, mine), pl.ds(LANES, LANES)]
    x_up2 = rcopy(half_dn, half_dn, xs.at[N2], xr.at[N2], xp[N1])
    x_dn2 = rcopy(half_up, half_up, xs.at[N3], xr.at[N3], xp[N3])
    x_up2.start()
    x_dn2.start()
    for col in range(N2):
        arrived(col, N3)
        for n, base, s in ((N1, N2, N2), (N2, N0, N3), (N1, N0, RING), (N2, N2, 5)):
            rcopy(sa.at[col, n, pl.ds(base, N2)], ra2.at[col, n - N1, pl.ds(base, N2)], ss.at[col, s], rs.at[col, s], partner).wait_recv()

        def own(q, col=col):
            a2 = lax.div(q, 12)
            tt = lax.rem(lax.div(q, N3), RING)
            r = lax.rem(q, N3)
            val = acc[col, N3, tt, a2, r] + rp[col, N3, tt, a2, r].astype(f32) + ra2[col, N0, a2, tt, r].astype(f32) + ra2[col, N1, a2, tt, r].astype(f32)
            acc[col, N3, tt, a2, r] = val
        each(48, own)
        far = up(ring_b[col], N2)

        def first_b(q, col=col, far=far):
            tt = lax.div(q, N3)
            r = lax.rem(q, N3)
            sb[col, N0, tt, r] = acc[col, N3, tt, far, r].astype(bf16)
        each(12, first_b)
        send(sb.at[col, N0, pl.ds(N0, N2)], rb1.at[col, N0], ss.at[col, 6], rs.at[col, 6], dev_b[col][N1])
        send(sb.at[col, N0, pl.ds(N2, N2)], rb1.at[col, N1], ss.at[col, 7], rs.at[col, 7], dev_b[col][N3])
        for n, base, peer in ((N1, N2, N1), (N2, N0, N3)):
            pos = up(ring_b[col], peer)

            def plain_b(q, col=col, n=n, base=base, pos=pos):
                tt = base + lax.div(q, N3)
                r = lax.rem(q, N3)
                sb[col, n, tt, r] = acc[col, N3, tt, pos, r].astype(bf16)
            each(6, plain_b)
            send(sb.at[col, n, pl.ds(base, N2)], rb2.at[col, n - N1, pl.ds(base, N2)], ss.at[col, n + 7], rs.at[col, n + 7], dev_b[col][peer])
    for col in range(N2):
        for n, base, peer in ((N1, N0, N1), (N2, N2, N3)):
            rcopy(sb.at[col, N0, pl.ds(N0, N2)], rb1.at[col, n - N1], ss.at[col, n + 5], rs.at[col, n + 5], partner).wait_recv()
            pos = up(ring_b[col], peer)

            def joined_b(q, col=col, n=n, base=base, pos=pos):
                h = lax.div(q, N3)
                tt = base + h
                r = lax.rem(q, N3)
                sb[col, n, tt, r] = (acc[col, N3, tt, pos, r] + rb1[col, n - N1, h, r].astype(f32)).astype(bf16)
            each(6, joined_b)
            send(sb.at[col, n, pl.ds(base, N2)], rb2.at[col, n - N1, pl.ds(base, N2)], ss.at[col, n + 9], rs.at[col, n + 9], dev_b[col][peer])
    for col in range(N2):
        here = ring_b[col]
        for n, base, s in ((N1, N2, SUB), (N2, N0, 9), (N1, N0, 10), (N2, N2, 11)):
            rcopy(sb.at[col, n, pl.ds(base, N2)], rb2.at[col, n - N1, pl.ds(base, N2)], ss.at[col, s], rs.at[col, s], partner).wait_recv()

        def own_b(q, col=col, here=here):
            tt = lax.div(q, N3)
            r = lax.rem(q, N3)
            val = acc[col, N3, tt, here, r] + rb2[col, N0, tt, r].astype(f32) + rb2[col, N1, tt, r].astype(f32)
            acc[col, N3, tt, here, r] = val
            sc[col, tt, r] = val.astype(bf16)
        each(12, own_b)
        for d in (N1, N3, N2):
            to = up(t, d)
            send(sc.at[col, to], rc.at[col, d - N1], cs.at[col, d - N1], cr.at[col, d - N1], xp[d])
        if col == N0:
            def kv_part(q, here=here):
                tt = lax.div(q, N3)
                r = lax.rem(q, N3)
                kvx[t, tt, r] = acc[N0, N3, tt, here, r, :, pl.ds(KV_AT, LANES)]
            each(12, kv_part)
            for d in (N1, N3, N2):
                send(kvx.at[t], kvx.at[t], ks.at[d - N1], kr.at[d - N1], xp[d])
    for col in range(N2):
        here = ring_b[col]
        for d in (N1, N3, N2):
            rcopy(sc.at[col, N0], rc.at[col, d - N1], cs.at[col, d - N1], cr.at[col, d - N1], partner).wait_recv()

        def last(r, col=col, here=here):
            w_out[col, r] = acc[col, N3, t, here, r] + rc[col, N0, r].astype(f32) + rc[col, N1, r].astype(f32) + rc[col, N2, r].astype(f32)
        each(N3, last)
    for d in (N1, N3, N2):
        src = up(t, RING - d)
        rcopy(kvx.at[src], kvx.at[src], ks.at[d - N1], kr.at[d - N1], partner).wait_recv()

    def kv_last(q):
        tt = lax.div(q, N3)
        r = lax.rem(q, N3)
        kv_out[tt, r] = ((kvx[N0, tt, r] + kvx[N1, tt, r]) + kvx[N2, tt, r]) + kvx[N3, tt, r]
    each(12, kv_last)
    for copy in sends:
        copy.wait_send()
    for col in range(N2):
        for n in range(RING):
            pair[col][n].wait_send()
    x_me.wait()
    x_up.wait_send()
    x_dn.wait_send()
    x_up2.wait()
    x_dn2.wait()


def sum_grads(g_pack, g_send, gx_my, n_batch):
    f32 = jnp.float32
    bf16 = jnp.bfloat16
    wide = g_pack.shape[-N1]
    dma = pltpu.SemaphoreType.DMA
    vmem = pl.BlockSpec(memory_space=pltpu.VMEM)
    any_spec = pl.BlockSpec(memory_space=pl.ANY)
    return pl.pallas_call(
        sum_kernel,
        name='sum_grads',
        out_shape=(jax.ShapeDtypeStruct((N2, N3, SUB, wide), f32), jax.ShapeDtypeStruct((RING, N3, SUB, LANES), f32),
                   jax.ShapeDtypeStruct((n_batch,) + gx_my.shape[N1:], bf16)),
        in_specs=[any_spec, any_spec, any_spec],
        out_specs=(vmem, vmem, any_spec),
        scratch_shapes=[
            pltpu.VMEM((N2, RING, RING, RING, N3, SUB, wide), f32), pltpu.VMEM((N2, RING, RING, RING, N3, SUB, wide), bf16),
            pltpu.VMEM((N2, N3, RING, RING, N3, SUB, wide), bf16), pltpu.VMEM((N2, N2, N2, RING, N3, SUB, wide), bf16), pltpu.VMEM((N2, N2, RING, RING, N3, SUB, wide), bf16),
            pltpu.VMEM((N2, N3, RING, N3, SUB, wide), bf16), pltpu.VMEM((N2, N2, N2, N3, SUB, wide), bf16), pltpu.VMEM((N2, N2, RING, N3, SUB, wide), bf16),
            pltpu.VMEM((N2, RING, N3, SUB, wide), bf16), pltpu.VMEM((N2, N3, N3, SUB, wide), bf16), pltpu.VMEM((RING, RING, N3, SUB, LANES), f32),
            dma((N2, RING)), dma((N2, RING)), dma((N2, RING)), dma((N2, 12)), dma((N2, 12)), dma((N2, N3)), dma((N2, N3)), dma((N3,)), dma((N3,)), dma((RING,)), dma((RING,)), dma((N1,)),
        ],
        compiler_params=pltpu.CompilerParams(collective_id=N1, has_side_effects=True, vmem_limit_bytes=60 * KIB * KIB),
    )(g_pack, g_send, gx_my)


def solution(mesh):
    n_tp = mesh.shape['tp']
    n_fsdp = mesh.shape['fsdp']

    def device_step(x_in, dy_out, ln_gain, w_q, w_k, w_v, w_o, w_gate, w_up, w_down):
        bf16 = jnp.bfloat16
        f32 = jnp.float32
        n_batch, seq_len, width = x_in.shape
        head_dim = w_k.shape[N1]
        rows = w_q.shape[N0]
        nq = w_q.shape[N1]
        nf = w_gate.shape[N1]
        part = N2 * head_dim // n_tp
        mine = n_batch // n_tp
        tokens = mine * seq_len
        tp = lax.axis_index('tp')
        core = lax.rem(lax.axis_index('fsdp'), N2)
        gain_hi = lax.reduce_precision(ln_gain, SUB, 7)
        gain_mid = lax.reduce_precision(ln_gain - gain_hi, SUB, 7)
        gain_lo = ln_gain - gain_hi - gain_mid
        gain_cols = jnp.stack([gain_hi, gain_mid, gain_lo], axis=N1).astype(bf16)
        kv_mine = lax.dynamic_slice_in_dim(jnp.concatenate([w_k, w_v], axis=N1), tp * part, part, N1)
        small = jnp.concatenate([kv_mine, gain_cols, jnp.zeros((rows, LANES - part - N3), bf16)], axis=N1)
        down = w_down.T
        packed = jnp.stack([jnp.concatenate([w_gate, w_q, w_o.T, small, down[:, :LANES]], axis=N1), jnp.concatenate([w_up, down[:, LANES:]], axis=N1)])
        wide = packed.shape[N2]
        full = gather_weights(packed).reshape(N2, n_tp, width, wide)
        small_full = full[N0, :, :, KV_AT:KV_AT + LANES]
        w_kv = jnp.concatenate([small_full[n, :, :part] for n in range(n_tp)], axis=N1)
        gain3 = small_full[N0, :, part:part + N3].astype(f32)
        gain_row = (gain3[:, N0] + gain3[:, N1] + gain3[:, N2]).reshape(N1, width)

        x_tok = lax.dynamic_slice_in_dim(x_in, tp * mine, mine, N0).reshape(tokens, width)
        dy_tok = lax.dynamic_slice_in_dim(dy_out, tp * mine, mine, N0).reshape(tokens, width)
        y_tok, gx_tok, g_own, g_oth = layer_step(x_tok, dy_tok, gain_row, full, w_kv, core, seq_len, head_dim)
        y_out = lax.all_gather(y_tok.reshape(mine, seq_len, width), 'tp', axis=N0, tiled=True)
        split = (N2, n_tp, RING, RING, N3, SUB, wide)
        w_sum, kv_sum, grad_x = sum_grads(g_own.reshape(split), g_oth.reshape(split), gx_tok.reshape(mine, seq_len, width), n_batch)
        w0 = w_sum[N0].reshape(rows, wide)
        w1 = w_sum[N1].reshape(rows, wide)
        kv_all = jnp.swapaxes(kv_sum.reshape(n_tp, rows, LANES)[:, :, :part], N0, N1).reshape(rows, N2 * head_dim)
        grad_wgate = w0[:, :nf]
        grad_wq = w0[:, nf:nf + nq]
        grad_wo = w0[:, nf + nq:nf + N2 * nq].T
        grad_wdown = jnp.concatenate([w0[:, wide - LANES:], w1[:, nf:]], axis=N1).T
        grad_wup = w1[:, :nf]
        grad_wk = kv_all[:, :head_dim]
        grad_wv = kv_all[:, head_dim:]
        grad_gain = kv_sum[N0].reshape(rows, LANES)[:, part]
        return (y_out, grad_x, grad_gain, grad_wq, grad_wk, grad_wv, grad_wo, grad_wgate, grad_wup, grad_wdown)

    act_spec = P('fsdp', None, None)
    row_spec = P('fsdp', 'tp')
    kv_spec = P('fsdp', None)
    col_spec = P('tp', 'fsdp')
    in_specs = (act_spec, act_spec, P('fsdp'), row_spec, kv_spec, kv_spec, col_spec, row_spec, row_spec, col_spec)
    out_specs = (act_spec, act_spec, P('fsdp'), row_spec, kv_spec, kv_spec, col_spec, row_spec, row_spec, col_spec)
    return jax.shard_map(device_step, mesh=mesh, in_specs=in_specs, out_specs=out_specs, check_vma=False)
```

```python
import jax
import jax.numpy as jnp
from jax import lax
from jax.sharding import PartitionSpec as P
from jax.experimental import pallas as pl
from jax.experimental.pallas import tpu as pltpu


N0, N1, N2, N3 = range(4)
RING = 4
SUB = 8
LANES = 128
PAIR = 256
KIB = 1024
ALL = Ellipsis
KV_AT = 1152
MESH_ID = pl.DeviceIdType.MESH


def gather_kernel(p_ref, g_ref, lsem, s1, r1, s2, r2, s3, r3, ds, dr):
    t = lax.axis_index('tp')
    f = lax.axis_index('fsdp')
    c = lax.rem(f, N2)
    at = {'x': t, 'y': lax.rem(lax.div(f, N2), RING), 'z': lax.div(f, SUB)}

    def up(i, d):
        return lax.rem(i + d, RING)

    def dev(where, cc):
        return {'tp': where['x'], 'fsdp': (where['z'] * RING + where['y']) * N2 + cc}

    def peer(axis, d):
        return dev({**at, axis: up(at[axis], d)}, c)

    partner = dev(at, N1 - c)
    barrier = pltpu.get_barrier_semaphore()
    greeted = [partner] + [peer(axis, d) for axis in 'xyz' for d in (N1, N2, N3)]
    for who in greeted:
        pl.semaphore_signal(barrier, inc=N1, device_id=who, device_id_type=MESH_ID)
    own = pltpu.make_async_copy(p_ref, g_ref.at[:, at['x'], at['z'], at['y'], c], lsem.at[N0])
    own.start()
    pl.semaphore_wait(barrier, len(greeted))

    sent = []

    def push(src, dst, s_sem, r_sem, who):
        copy = pltpu.make_async_remote_copy(src_ref=src, dst_ref=dst, send_sem=s_sem, recv_sem=r_sem, device_id=who, device_id_type=MESH_ID)
        copy.start()
        sent.append(copy)

    def landed(ref, s_sem, r_sem):
        pltpu.make_async_remote_copy(src_ref=ref, dst_ref=ref, send_sem=s_sem, recv_sem=r_sem, device_id=partner, device_id_type=MESH_ID).wait_recv()

    def view(k, h, fixed, core):
        spot = [fixed.get(axis, slice(None)) for axis in 'xzy']
        return g_ref.at[h, spot[N0], spot[N1], spot[N2], core, k]

    orders = ('xyz', 'yzx', 'zxy')
    both = slice(None)
    across = []

    def share(k, h, fixed, n):
        push(view(k, h, fixed, c), view(k, h, fixed, c), ds.at[k, n], dr.at[k, n], partner)
        across.append((k, h, fixed, n))

    def ring_start(k, axis, fixed, ss, rr):
        here = {**fixed, axis: at[axis]}
        for n in range(N2):
            push(view(k, n, here, c), view(k, n, here, c), ss.at[k, n], rr.at[k, n], peer(axis, N1))
            push(view(k, N1 - n, here, c), view(k, N1 - n, here, c), ss.at[k, N3 - n], rr.at[k, N3 - n], peer(axis, N3))

    def ring_forward(k, axis, fixed, ss, rr):
        for h, d, n in ((N0, N3, N0), (N1, N1, N3)):
            there = {**fixed, axis: up(at[axis], d)}
            landed(view(k, h, there, c), ss.at[k, n], rr.at[k, n])
            push(view(k, h, there, c), view(k, h, there, c), ss.at[k, RING + h], rr.at[k, RING + h], peer(axis, RING - d))

    def ring_share(k, axis, fixed, ss, rr, base):
        for m, (h, d, n) in enumerate(((N0, N3, N0), (N1, N1, N3), (N1, N3, N1), (N0, N1, N2), (N0, N2, RING), (N1, N2, 5))):
            there = {**fixed, axis: up(at[axis], d)}
            if n not in (N0, N3):
                landed(view(k, h, there, c), ss.at[k, n], rr.at[k, n])
            share(k, h, there, base + m)

    for k, order in enumerate(orders):
        for d in (N1, N3, N2):
            push(p_ref.at[:, k], view(k, both, at, c), s1.at[k, d - N1], r1.at[k, d - N1], peer(order[N0], d))
    own.wait()
    second = []
    third = []
    for k, order in enumerate(orders):
        for d in (N1, N3, N2):
            landed(view(k, both, {**at, order[N0]: up(at[order[N0]], RING - d)}, c), s1.at[k, d - N1], r1.at[k, d - N1])
        fixed = {order[N2]: at[order[N2]]}
        second.append((k, order[N1], fixed, s2, r2))
        third.append((k, order[N2], {}, s3, r3))
        ring_start(*second[k])
    for k, order in enumerate(orders):
        here = {order[N1]: at[order[N1]], order[N2]: at[order[N2]]}
        share(k, N0, here, N0)
        share(k, N1, here, N1)
    for k in range(N3):
        ring_forward(*second[k])
    for k in range(N3):
        ring_share(*second[k], N2)
        ring_start(*third[k])
    for k in range(N3):
        ring_forward(*third[k])
    for k in range(N3):
        ring_share(*third[k], SUB)
    for k, h, fixed, n in across:
        landed(view(k, h, fixed, N1 - c), ds.at[k, n], dr.at[k, n])
    for copy in sent:
        copy.wait_send()


def gather_weights(packed):
    dma = pltpu.SemaphoreType.DMA
    any_spec = pl.BlockSpec(memory_space=pl.ANY)
    wide = packed.shape[N2]
    return pl.pallas_call(
        gather_kernel,
        name='gather_weights',
        out_shape=jax.ShapeDtypeStruct((N2, RING, RING, RING, N2, N3, SUB, wide), packed.dtype),
        in_specs=[any_spec],
        out_specs=any_spec,
        scratch_shapes=[dma((N1,)), dma((N3, N3)), dma((N3, N3)), dma((N3, 6)), dma((N3, 6)), dma((N3, 6)), dma((N3, 6)), dma((N3, 14)), dma((N3, 14))],
        compiler_params=pltpu.CompilerParams(collective_id=N2, has_side_effects=True, vmem_limit_bytes=60 * KIB * KIB),
    )(packed.reshape(N2, N3, SUB, wide))


NT = (((N1,), (N1,)), ((), ()))
NN = (((N1,), (N0,)), ((), ()))
TN = (((N0,), (N0,)), ((), ()))


def dot(left, right, dims=NN):
    return lax.dot_general(left, right, dims, preferred_element_type=jnp.float32)


def by_class(out, cols, vals, core):
    for n in range(32):
        out[lax.rem(n % N2 + core, N2), 24 * (n // N2):24 * (n // N2) + 24, cols] = vals[24 * n:24 * n + 24]


def proj_kernel(who_ref, x_ref, dy_ref, gain_ref, w0_ref, w1_ref, wkv_ref, ht_out, dyt_out, q_out, kv_out, do_out, act_out, dg_out, du_out, h_out):
    f32 = jnp.float32
    bf16 = jnp.bfloat16
    tokens, width = h_out.shape
    dy_tok = dy_ref[ALL].reshape(tokens, width)

    @pl.when(pl.program_id(N0) == N0)
    def _():
        for n in range(tokens // LANES):
            at = slice(n * LANES, n * LANES + LANES)
            seq, row = divmod(n * LANES, x_ref.shape[N1])
            x_f32 = x_ref[seq, row:row + LANES, :].astype(f32)
            x_cent = x_f32 - jnp.mean(x_f32, axis=-N1, keepdims=True)
            x_var = jnp.mean(x_cent * x_cent, axis=-N1, keepdims=True)
            h_norm = (x_cent * lax.rsqrt(x_var + 1e-5) * gain_ref[ALL]).astype(bf16)
            h_out[at, :] = h_norm
            by_class(ht_out, at, h_norm.astype(f32).T.astype(bf16), who_ref[N1])
            by_class(dyt_out, at, dy_ref[seq, row:row + LANES, :].astype(f32).T.astype(bf16), who_ref[N1])
        kv_out[ALL] = dot(h_out[ALL], wkv_ref[ALL]).astype(bf16)

    for n in range(N3):
        cols = slice(n * PAIR, n * PAIR + PAIR)
        gate = dot(h_out[ALL], w0_ref[N0, N0, :, cols]).astype(bf16).astype(f32)
        up = dot(h_out[ALL], w1_ref[N0, N0, :, cols]).astype(bf16).astype(f32)
        if n == N0:
            d_low = dot(dy_tok, w0_ref[N0, N0, :, 1280:1408])
            d_act = jnp.concatenate([d_low, dot(dy_tok, w1_ref[N0, N0, :, 768:896])], axis=N1)
        else:
            d_act = dot(dy_tok, w1_ref[N0, N0, :, 640 + n * PAIR:896 + n * PAIR])
        d_act = d_act.astype(bf16).astype(f32)
        sig = 0.5 * jnp.tanh(0.5 * gate) + 0.5
        silu = gate * sig
        act_out[N0, :, cols] = (silu * up).astype(bf16)
        du_out[N0, :, cols] = (d_act * silu).astype(bf16)
        dg_out[N0, :, cols] = (d_act * up * (sig + silu * (1.0 - sig))).astype(bf16)
    q_out[N0] = dot(h_out[ALL], w0_ref[N0, N0, :, 768:KIB]).astype(bf16)
    do_out[N0] = dot(dy_tok, w0_ref[N0, N0, :, 896:1152]).astype(bf16)


def att_kernel(q_ref, kv_ref, do_ref, cq_ref, sq_ref, ck_ref, sk_ref, o_out, dq_out, dkv_out, dk_lo, dk_hi, dv_lo, dv_hi):
    f32 = jnp.float32
    bf16 = jnp.bfloat16
    seq_len = kv_ref.shape[N0]
    lane = lax.broadcasted_iota(jnp.int32, (seq_len, LANES), N1)
    low = lane < 64
    first = lax.rem(lane, 64) < 32
    causal = lax.broadcasted_iota(jnp.int32, (seq_len, seq_len), N0) >= lax.broadcasted_iota(jnp.int32, (seq_len, seq_len), N1)

    def other(vals):
        return jnp.where(first, pltpu.roll(vals, 96, N1), pltpu.roll(vals, 32, N1))

    kv_f32 = kv_ref[ALL].astype(f32)
    kv_rot = kv_f32 * ck_ref[ALL] + other(kv_f32) * sk_ref[ALL]
    zero = jnp.zeros_like(kv_rot)
    k_lo = jnp.where(low, kv_rot, zero)
    v_hi = jnp.where(low, zero, kv_rot)
    k_hi = pltpu.roll(k_lo, 64, N1).astype(bf16)
    v_lo = pltpu.roll(v_hi, 64, N1).astype(bf16)
    k_lo = k_lo.astype(bf16)
    v_hi = v_hi.astype(bf16)
    for ref in (dk_lo, dk_hi, dv_lo, dv_hi):
        ref[ALL] = jnp.zeros_like(ref)

    def head(q_tile, k_part, v_part, do_tile):
        scores = jnp.where(causal, dot(q_tile, k_part, NT), -1e30)
        exp_val = jnp.exp(scores - jnp.max(scores, axis=-N1, keepdims=True))
        prob = exp_val * (1.0 / jnp.sum(exp_val, axis=-N1, keepdims=True))
        d_prob = dot(do_tile, v_part, NT).astype(bf16).astype(f32)
        d_score = prob * (d_prob - jnp.sum(d_prob * prob, axis=-N1, keepdims=True))
        return prob.astype(bf16), d_score.astype(bf16)

    def block(tt, carry):
        tiles = []
        for n in range(N2):
            cols = slice(n * LANES, n * LANES + LANES)
            vals = q_ref[tt, :, cols].astype(f32)
            tiles.append(((vals * cq_ref[ALL] + other(vals) * sq_ref[ALL]) * 0.125).astype(bf16))
        do0 = do_ref[tt, :, N0:LANES]
        do1 = do_ref[tt, :, LANES:PAIR]
        p0, s0 = head(tiles[N0], k_lo, v_hi, do0)
        p1, s1 = head(tiles[N0], k_hi, v_lo, do1)
        p2, s2 = head(tiles[N1], k_lo, v_hi, do1)
        o_out[tt, :, N0:LANES] = dot(p0, v_hi).astype(bf16)
        o_out[tt, :, LANES:PAIR] = (dot(p1, v_lo) + dot(p2, v_hi)).astype(bf16)
        dv_hi[ALL] += dot(p0, do0, TN) + dot(p2, do1, TN)
        dv_lo[ALL] += dot(p1, do1, TN)
        dk_lo[ALL] += dot(s0, tiles[N0], TN) + dot(s2, tiles[N1], TN)
        dk_hi[ALL] += dot(s1, tiles[N0], TN)
        for n, grad in ((N0, dot(s0, k_lo) + dot(s1, k_hi)), (N1, dot(s2, k_lo))):
            grad = grad.astype(bf16).astype(f32) * 0.125
            dq_out[tt, :, n * LANES:n * LANES + LANES] = (grad * cq_ref[ALL] - other(grad) * sq_ref[ALL]).astype(bf16)
        return carry
    lax.fori_loop(N0, q_ref.shape[N0], block, N0)
    dk = (dk_lo[ALL] + pltpu.roll(dk_hi[ALL], 64, N1)).astype(bf16).astype(f32)
    dk_raw = dk * ck_ref[ALL] - other(dk) * sk_ref[ALL]
    dv = dv_hi[ALL] + pltpu.roll(dv_lo[ALL], 64, N1)
    dkv_out[ALL] = jnp.where(low, dk_raw, dv).astype(bf16)


def back_kernel(who_ref, x_ref, dy_ref, gain_ref, w0_ref, w1_ref, wkv_ref, o_ref, act_ref, dq_ref, dg_ref, du_ref, dkv_ref, y_out, gx_out, gcol_out, y_acc, dh_acc):
    f32 = jnp.float32
    bf16 = jnp.bfloat16
    step = pl.program_id(N0)
    tokens, width = y_acc.shape
    y_left = jnp.concatenate([o_ref[N0], act_ref[N0]], axis=N1)
    y_right = jnp.concatenate([w0_ref[N0, N0, :, 896:1152], w0_ref[N0, N0, :, 1280:1408], w1_ref[N0, N0, :, 768:1408]], axis=N1)
    h_left = jnp.concatenate([dg_ref[N0], dq_ref[N0], du_ref[N0]], axis=N1)
    h_right = jnp.concatenate([w0_ref[N0, N0, :, N0:KIB], w1_ref[N0, N0, :, N0:768]], axis=N1)
    y_part = dot(y_left, y_right, NT)
    dh_part = dot(h_left, h_right, NT)

    @pl.when(step == N0)
    def _():
        y_acc[ALL] = y_part
        dh_acc[ALL] = dh_part + dot(dkv_ref[ALL], wkv_ref[ALL], NT)

    @pl.when(step > N0)
    def _():
        y_acc[ALL] += y_part
        dh_acc[ALL] += dh_part

    @pl.when(step == pl.num_programs(N0) - N1)
    def _():
        gain = jnp.zeros((N1, width), f32)
        for n in range(tokens // LANES):
            at = slice(n * LANES, n * LANES + LANES)
            seq, row = divmod(n * LANES, x_ref.shape[N1])
            x_f32 = x_ref[seq, row:row + LANES, :].astype(f32)
            y_out[at, :] = (x_f32 + y_acc[at, :]).astype(bf16)
            x_cent = x_f32 - jnp.mean(x_f32, axis=-N1, keepdims=True)
            rstd = lax.rsqrt(jnp.mean(x_cent * x_cent, axis=-N1, keepdims=True) + 1e-5)
            x_hat = x_cent * rstd
            dh = dh_acc[at, :].astype(bf16).astype(f32)
            gain += jnp.sum(dh * x_hat, axis=N0, keepdims=True)
            d_hat = dh * gain_ref[ALL]
            dx = rstd * (d_hat - jnp.mean(d_hat, axis=-N1, keepdims=True) - x_hat * jnp.mean(d_hat * x_hat, axis=-N1, keepdims=True))
            gx_out[at, :] = (dy_ref[seq, row:row + LANES, :].astype(f32) + dx).astype(bf16)
        lane = lax.broadcasted_iota(jnp.int32, (width, LANES), N1)
        by_class(gcol_out, slice(None), jnp.where(lane == 32, jnp.broadcast_to(gain, (LANES, width)).T, 0.0), who_ref[N1])


def wgrad_kernel(ht_ref, dyt_ref, gcol_ref, o_ref, act_ref, dq_ref, dg_ref, du_ref, dkv_ref, own_out, oth_out):
    tt = pl.program_id(N0)
    half = ht_ref.shape[N1]
    lane = lax.broadcasted_iota(jnp.int32, (half, LANES), N1)
    ht = ht_ref[ALL].reshape(N2 * half, ht_ref.shape[N2])
    dyt = dyt_ref[ALL].reshape(N2 * half, dyt_ref.shape[N2])

    def put(n, cols, vals):
        own_out[n, N0, :, cols] = vals[:half]
        oth_out[n, N0, :, cols] = vals[half:].astype(jnp.bfloat16)

    for k in range(N3):
        cols = slice(k * PAIR, k * PAIR + PAIR)
        put(N0, cols, dot(ht, dg_ref[N0, :, cols]))
        put(N1, cols, dot(ht, du_ref[N0, :, cols]))
    g_q = dot(ht, dq_ref[N0])
    g_o = dot(dyt, o_ref[N0])
    put(N0, slice(768, 896), g_q[:, N0:LANES])
    put(N0, slice(896, KIB), g_q[:, LANES:PAIR] + g_o[:, N0:LANES])
    put(N0, slice(KIB, 1152), g_o[:, LANES:PAIR])
    g_kv = dot(ht, dkv_ref[ALL])
    for cls, out in ((N0, own_out), (N1, oth_out)):
        part = pltpu.roll(g_kv[cls * half:cls * half + half], lax.rem(LANES - 32 * tt, LANES), N1)
        out[N0, N0, :, 1152:1280] = (jnp.where(lane < 32, part, 0.0) + gcol_ref[cls]).astype(out.dtype)
    put(N0, slice(1280, 1408), dot(dyt, act_ref[N0, :, N0:LANES]))
    for lo, hi in ((LANES, 384), (384, 640), (640, 768)):
        put(N1, slice(lo + 640, hi + 640), dot(dyt, act_ref[N0, :, lo:hi]))


def layer_step(x_in, dy_in, gain_row, w_full, w_kv, tables, who, seq_len):
    f32 = jnp.float32
    bf16 = jnp.bfloat16
    n_tp = w_full.shape[N1]
    wide = w_full.shape[N3]
    width = w_full.shape[N2]
    n_seq = x_in.shape[N0] // n_tp
    tokens = n_seq * seq_len
    half = width // N2

    def whole(shape):
        return pl.BlockSpec(shape, lambda i, *_: (N0,) * len(shape))

    def per(shape):
        return pl.BlockSpec((N1,) + shape, lambda i, *_: (i,) + (N0,) * len(shape))

    w0_spec = pl.BlockSpec((N1, N1, width, wide), lambda i, *_: (N0, i, N0, N0))
    w1_spec = pl.BlockSpec((N1, N1, width, wide), lambda i, *_: (N1, i, N0, N0))
    mine = pl.BlockSpec((n_seq, seq_len, width), lambda i, who_ref: (who_ref[N0], N0, N0))
    tok = whole((tokens, width))
    classes = whole((N2, half, tokens))
    params = pltpu.CompilerParams(dimension_semantics=('arbitrary',), vmem_limit_bytes=56 * KIB * KIB)
    wide_t = jax.ShapeDtypeStruct((n_tp, tokens, width), bf16)
    pair_t = jax.ShapeDtypeStruct((n_tp, tokens, PAIR), bf16)
    row_t = jax.ShapeDtypeStruct((tokens, width), bf16)
    class_t = jax.ShapeDtypeStruct((N2, half, tokens), bf16)
    kv_t = jax.ShapeDtypeStruct((tokens, LANES), bf16)
    work = pl.CostEstimate(flops=13 * 10**9, bytes_accessed=40 * 10**6, transcendentals=N0)
    h_t, dy_t, q_raw, kv_raw, d_o, act, d_gate, d_up = pl.pallas_call(
        proj_kernel, name='proj',
        grid_spec=pltpu.PrefetchScalarGridSpec(
            num_scalar_prefetch=N1, grid=(n_tp,),
            in_specs=[mine, mine, whole((N1, width)), w0_spec, w1_spec, whole((width, LANES))],
            out_specs=(classes, classes, per((tokens, PAIR)), whole((tokens, LANES)), per((tokens, PAIR)), per((tokens, width)), per((tokens, width)), per((tokens, width))),
            scratch_shapes=[pltpu.VMEM((tokens, width), bf16)]),
        out_shape=(class_t, class_t, pair_t, kv_t, pair_t, wide_t, wide_t, wide_t),
        compiler_params=params, cost_estimate=work,
    )(who, x_in, dy_in, gain_row, w_full, w_full, w_kv)

    pair_spec = pl.BlockSpec((n_tp, seq_len, PAIR), lambda i: (N0, i, N0))
    kv_spec = pl.BlockSpec((seq_len, LANES), lambda i: (i, N0))
    table = whole((seq_len, LANES))
    att, d_q, d_kv = pl.pallas_call(
        att_kernel, name='attention', grid=(n_seq,),
        in_specs=[pair_spec, kv_spec, pair_spec, table, table, table, table],
        out_specs=(pair_spec, pair_spec, kv_spec),
        out_shape=(pair_t, pair_t, kv_t),
        scratch_shapes=[pltpu.VMEM((seq_len, LANES), f32)] * RING,
        compiler_params=params, cost_estimate=work,
    )(q_raw, kv_raw, d_o, *tables)

    gcol_t = jax.ShapeDtypeStruct((N2, half, LANES), f32)
    y_tok, gx_tok, gain_col = pl.pallas_call(
        back_kernel, name='back',
        grid_spec=pltpu.PrefetchScalarGridSpec(
            num_scalar_prefetch=N1, grid=(n_tp,),
            in_specs=[mine, mine, whole((N1, width)), w0_spec, w1_spec, whole((width, LANES)), per((tokens, PAIR)), per((tokens, width)), per((tokens, PAIR)),
                      per((tokens, width)), per((tokens, width)), whole((tokens, LANES))],
            out_specs=(tok, tok, whole((N2, half, LANES))),
            scratch_shapes=[pltpu.VMEM((tokens, width), f32)] * N2),
        out_shape=(row_t, row_t, gcol_t),
        compiler_params=params, cost_estimate=work,
    )(who, x_in, dy_in, gain_row, w_full, w_full, w_kv, att, act, d_q, d_gate, d_up, d_kv)

    class_spec = pl.BlockSpec((N2, N1, half, wide), lambda i: (N0, i, N0, N0))
    own, oth = pl.pallas_call(
        wgrad_kernel, name='wgrad', grid=(n_tp,),
        in_specs=[classes, classes, whole((N2, half, LANES)), per((tokens, PAIR)), per((tokens, width)), per((tokens, PAIR)),
                  per((tokens, width)), per((tokens, width)), whole((tokens, LANES))],
        out_specs=(class_spec, class_spec),
        out_shape=(jax.ShapeDtypeStruct((N2, n_tp, half, wide), f32), jax.ShapeDtypeStruct((N2, n_tp, half, wide), bf16)),
        compiler_params=params, cost_estimate=work,
    )(h_t, dy_t, gain_col, att, act, d_q, d_gate, d_up, d_kv)
    return y_tok, gx_tok, own, oth


def rope_tables(seq_len, head_dim):
    f32 = jnp.float32
    half_dim = head_dim // N2
    inv_freq = jnp.power(10000.0, -2.0 * jnp.arange(half_dim, dtype=f32) / head_dim)
    angle = jnp.arange(seq_len, dtype=f32)[:, None] * inv_freq[None, :]
    cos_t = jnp.cos(angle)
    sin_t = jnp.sin(angle)
    cos_h = jnp.concatenate([cos_t, cos_t], axis=N1)
    sin_h = jnp.concatenate([-sin_t, sin_t], axis=N1)
    cos_q = jnp.concatenate([cos_h, cos_h], axis=N1)
    sin_q = jnp.concatenate([sin_h, sin_h], axis=N1)
    cos_k = jnp.concatenate([cos_h, jnp.ones_like(cos_h)], axis=N1)
    sin_k = jnp.concatenate([sin_h, jnp.zeros_like(sin_h)], axis=N1)
    return cos_q, sin_q, cos_k, sin_k


def sum_kernel(g_ref, gs_ref, gx_ref, y_ref, below_ref, above_ref, w_out, kv_out, gx_out, y_out, acc, rp, sa, ra1, ra2, sb, rb1, rb2, sc, rc, kvx, gsem, d2s, d2r, ss, rs, cs, cr, ks, kr, xs, xr, lsem):
    f32 = jnp.float32
    bf16 = jnp.bfloat16
    t = lax.axis_index('tp')
    f = lax.axis_index('fsdp')
    c = lax.rem(f, N2)
    yy = lax.rem(lax.div(f, N2), RING)
    zz = lax.div(f, SUB)

    def dev(tt, zc, yc, cc):
        return {'tp': tt, 'fsdp': (zc * RING + yc) * N2 + cc}

    def up(i, d):
        return lax.rem(i + d, RING)

    partner = dev(t, zz, yy, N1 - c)
    xp = [dev(up(t, d), zz, yy, c) for d in range(RING)]
    z_dev = [dev(t, up(zz, d), yy, c) for d in range(RING)]
    y_dev = [dev(t, zz, up(yy, d), c) for d in range(RING)]
    barrier = pltpu.get_barrier_semaphore()
    peers = [partner, xp[N1], xp[N2], xp[N3], z_dev[N1], z_dev[N3], y_dev[N1], y_dev[N3]]
    for peer in peers:
        pl.semaphore_signal(barrier, inc=N1, device_id=peer, device_id_type=MESH_ID)

    def rcopy(src, dst, s_sem, r_sem, peer):
        return pltpu.make_async_remote_copy(src_ref=src, dst_ref=dst, send_sem=s_sem, recv_sem=r_sem, device_id=peer, device_id_type=MESH_ID)

    ring_a = [zz, yy]
    ring_b = [yy, zz]
    dev_a = [z_dev, y_dev]
    dev_b = [y_dev, z_dev]
    order = [N2, N1, N3, N0]

    def g_view(col, j):
        return g_ref.at[N0, :, j] if col == N0 else g_ref.at[N1, :, :, j]

    def gs_view(col, j):
        return gs_ref.at[N0, :, j] if col == N0 else gs_ref.at[N1, :, :, j]

    load = [[None] * RING for _ in range(N2)]
    pair = [[None] * RING for _ in range(N2)]
    for n, d in enumerate(order):
        for col in range(N2):
            j = up(ring_a[col], d)
            load[col][n] = pltpu.make_async_copy(g_view(col, j), acc.at[col, n], gsem.at[col, n])
            load[col][n].start()
    pl.semaphore_wait(barrier, len(peers))
    for n, d in enumerate(order):
        for col in range(N2):
            j = up(ring_a[col], d)
            pair[col][n] = rcopy(gs_view(col, j), rp.at[col, n], d2s.at[col, n], d2r.at[col, n], partner)
            pair[col][n].start()
    mine = gx_ref.shape[N0]
    my_rows = pl.ds(t * mine, mine)
    lower = pl.ds(up(t, N3) * mine, mine)
    upper = pl.ds(up(t, N1) * mine, mine)
    y_up = rcopy(below_ref.at[:, pl.ds(N0, LANES)], y_out.at[lower, pl.ds(N0, LANES)], xs.at[RING], xr.at[RING], xp[N1])
    y_dn = rcopy(above_ref.at[:, pl.ds(LANES, LANES)], y_out.at[upper, pl.ds(LANES, LANES)], xs.at[5], xr.at[5], xp[N3])
    y_up.start()
    y_dn.start()
    y_keep = []
    for n, (ref, place) in enumerate(((y_ref, my_rows), (below_ref, lower), (above_ref, upper))):
        y_keep.append(pltpu.make_async_copy(ref, y_out.at[place], lsem.at[n + N1]))
        y_keep[n].start()
    x_up = rcopy(gx_ref, gx_out.at[my_rows], xs.at[N0], xr.at[N0], xp[N1])
    x_dn = rcopy(gx_ref, gx_out.at[my_rows], xs.at[N1], xr.at[N1], xp[N3])
    x_up.start()
    x_dn.start()
    x_me = pltpu.make_async_copy(gx_ref, gx_out.at[my_rows], lsem.at[N0])
    x_me.start()

    def each(count, body):
        def step(n, carry):
            body(n)
            return carry
        lax.fori_loop(N0, count, step, N0)

    def arrived(col, n):
        load[col][n].wait()
        pair[col][n].wait_recv()

    sends = []

    def send(src, dst, s_sem, r_sem, peer):
        copy = rcopy(src, dst, s_sem, r_sem, peer)
        copy.start()
        sends.append(copy)
        return copy

    for col in range(N2):
        arrived(col, N0)

        def first(q, col=col):
            tt = lax.div(q, 12)
            a2 = lax.rem(lax.div(q, N3), RING)
            r = lax.rem(q, N3)
            sa[col, N0, a2, tt, r] = (acc[col, N0, tt, a2, r] + rp[col, N0, tt, a2, r].astype(f32)).astype(bf16)
        each(48, first)
        send(sa.at[col, N0, pl.ds(N0, N2)], ra1.at[col, N0], ss.at[col, N0], rs.at[col, N0], dev_a[col][N1])
        send(sa.at[col, N0, pl.ds(N2, N2)], ra1.at[col, N1], ss.at[col, N1], rs.at[col, N1], dev_a[col][N3])
    for col in range(N2):
        for n, base, peer in ((N1, N2, N1), (N2, N0, N3)):
            arrived(col, n)

            def plain(q, col=col, n=n, base=base):
                a2 = base + lax.div(q, 12)
                tt = lax.rem(lax.div(q, N3), RING)
                r = lax.rem(q, N3)
                sa[col, n, a2, tt, r] = (acc[col, n, tt, a2, r] + rp[col, n, tt, a2, r].astype(f32)).astype(bf16)
            each(24, plain)
            send(sa.at[col, n, pl.ds(base, N2)], ra2.at[col, n - N1, pl.ds(base, N2)], ss.at[col, n + N1], rs.at[col, n + N1], dev_a[col][peer])
    for col in range(N2):
        for n, base, peer in ((N1, N0, N1), (N2, N2, N3)):
            rcopy(sa.at[col, N0, pl.ds(N0, N2)], ra1.at[col, n - N1], ss.at[col, n - N1], rs.at[col, n - N1], dev_a[col][peer]).wait_recv()

            def joined(q, col=col, n=n, base=base):
                h = lax.div(q, 12)
                a2 = base + h
                tt = lax.rem(lax.div(q, N3), RING)
                r = lax.rem(q, N3)
                val = acc[col, n, tt, a2, r] + rp[col, n, tt, a2, r].astype(f32) + ra1[col, n - N1, h, tt, r].astype(f32)
                sa[col, n, a2, tt, r] = val.astype(bf16)
            each(24, joined)
            send(sa.at[col, n, pl.ds(base, N2)], ra2.at[col, n - N1, pl.ds(base, N2)], ss.at[col, n + N3], rs.at[col, n + N3], dev_a[col][peer])
    x_up.wait_recv()
    x_dn.wait_recv()
    half_dn = gx_out.at[lower, pl.ds(N0, LANES)]
    half_up = gx_out.at[upper, pl.ds(LANES, LANES)]
    x_up2 = rcopy(half_dn, half_dn, xs.at[N2], xr.at[N2], xp[N1])
    x_dn2 = rcopy(half_up, half_up, xs.at[N3], xr.at[N3], xp[N3])
    x_up2.start()
    x_dn2.start()
    for col in range(N2):
        arrived(col, N3)
        for n, base, s in ((N1, N2, N2), (N2, N0, N3), (N1, N0, RING), (N2, N2, 5)):
            rcopy(sa.at[col, n, pl.ds(base, N2)], ra2.at[col, n - N1, pl.ds(base, N2)], ss.at[col, s], rs.at[col, s], partner).wait_recv()

        def own(q, col=col):
            a2 = lax.div(q, 12)
            tt = lax.rem(lax.div(q, N3), RING)
            r = lax.rem(q, N3)
            val = acc[col, N3, tt, a2, r] + rp[col, N3, tt, a2, r].astype(f32) + ra2[col, N0, a2, tt, r].astype(f32) + ra2[col, N1, a2, tt, r].astype(f32)
            acc[col, N3, tt, a2, r] = val
        each(48, own)
        far = up(ring_b[col], N2)

        def first_b(q, col=col, far=far):
            tt = lax.div(q, N3)
            r = lax.rem(q, N3)
            sb[col, N0, tt, r] = acc[col, N3, tt, far, r].astype(bf16)
        each(12, first_b)
        send(sb.at[col, N0, pl.ds(N0, N2)], rb1.at[col, N0], ss.at[col, 6], rs.at[col, 6], dev_b[col][N1])
        send(sb.at[col, N0, pl.ds(N2, N2)], rb1.at[col, N1], ss.at[col, 7], rs.at[col, 7], dev_b[col][N3])
        for n, base, peer in ((N1, N2, N1), (N2, N0, N3)):
            pos = up(ring_b[col], peer)

            def plain_b(q, col=col, n=n, base=base, pos=pos):
                tt = base + lax.div(q, N3)
                r = lax.rem(q, N3)
                sb[col, n, tt, r] = acc[col, N3, tt, pos, r].astype(bf16)
            each(6, plain_b)
            send(sb.at[col, n, pl.ds(base, N2)], rb2.at[col, n - N1, pl.ds(base, N2)], ss.at[col, n + 7], rs.at[col, n + 7], dev_b[col][peer])
    for col in range(N2):
        for n, base, peer in ((N1, N0, N1), (N2, N2, N3)):
            rcopy(sb.at[col, N0, pl.ds(N0, N2)], rb1.at[col, n - N1], ss.at[col, n + 5], rs.at[col, n + 5], partner).wait_recv()
            pos = up(ring_b[col], peer)

            def joined_b(q, col=col, n=n, base=base, pos=pos):
                h = lax.div(q, N3)
                tt = base + h
                r = lax.rem(q, N3)
                sb[col, n, tt, r] = (acc[col, N3, tt, pos, r] + rb1[col, n - N1, h, r].astype(f32)).astype(bf16)
            each(6, joined_b)
            send(sb.at[col, n, pl.ds(base, N2)], rb2.at[col, n - N1, pl.ds(base, N2)], ss.at[col, n + 9], rs.at[col, n + 9], dev_b[col][peer])
    for col in range(N2):
        here = ring_b[col]
        for n, base, s in ((N1, N2, SUB), (N2, N0, 9), (N1, N0, 10), (N2, N2, 11)):
            rcopy(sb.at[col, n, pl.ds(base, N2)], rb2.at[col, n - N1, pl.ds(base, N2)], ss.at[col, s], rs.at[col, s], partner).wait_recv()

        def own_b(q, col=col, here=here):
            tt = lax.div(q, N3)
            r = lax.rem(q, N3)
            val = acc[col, N3, tt, here, r] + rb2[col, N0, tt, r].astype(f32) + rb2[col, N1, tt, r].astype(f32)
            acc[col, N3, tt, here, r] = val
            sc[col, tt, r] = val.astype(bf16)
        each(12, own_b)
        for d in (N1, N3, N2):
            to = up(t, d)
            send(sc.at[col, to], rc.at[col, d - N1], cs.at[col, d - N1], cr.at[col, d - N1], xp[d])
        if col == N0:
            def kv_part(q, here=here):
                tt = lax.div(q, N3)
                r = lax.rem(q, N3)
                kvx[t, tt, r] = acc[N0, N3, tt, here, r, :, pl.ds(KV_AT, LANES)]
            each(12, kv_part)
            for d in (N1, N3, N2):
                send(kvx.at[t], kvx.at[t], ks.at[d - N1], kr.at[d - N1], xp[d])
    for col in range(N2):
        here = ring_b[col]
        for d in (N1, N3, N2):
            rcopy(sc.at[col, N0], rc.at[col, d - N1], cs.at[col, d - N1], cr.at[col, d - N1], partner).wait_recv()

        def last(r, col=col, here=here):
            w_out[col, r] = acc[col, N3, t, here, r] + rc[col, N0, r].astype(f32) + rc[col, N1, r].astype(f32) + rc[col, N2, r].astype(f32)
        each(N3, last)
    for d in (N1, N3, N2):
        src = up(t, RING - d)
        rcopy(kvx.at[src], kvx.at[src], ks.at[d - N1], kr.at[d - N1], partner).wait_recv()

    def kv_last(q):
        tt = lax.div(q, N3)
        r = lax.rem(q, N3)
        kv_out[tt, r] = ((kvx[N0, tt, r] + kvx[N1, tt, r]) + kvx[N2, tt, r]) + kvx[N3, tt, r]
    each(12, kv_last)
    for copy in sends:
        copy.wait_send()
    for col in range(N2):
        for n in range(RING):
            pair[col][n].wait_send()
    x_me.wait()
    x_up.wait_send()
    x_dn.wait_send()
    x_up2.wait()
    x_dn2.wait()
    y_up.wait()
    y_dn.wait()
    for copy in y_keep:
        copy.wait()


def sum_grads(g_pack, g_send, gx_my, y_blocks, n_batch):
    f32 = jnp.float32
    bf16 = jnp.bfloat16
    wide = g_pack.shape[-N1]
    dma = pltpu.SemaphoreType.DMA
    vmem = pl.BlockSpec(memory_space=pltpu.VMEM)
    any_spec = pl.BlockSpec(memory_space=pl.ANY)
    return pl.pallas_call(
        sum_kernel,
        name='sum_grads',
        out_shape=(jax.ShapeDtypeStruct((N2, N3, SUB, wide), f32), jax.ShapeDtypeStruct((RING, N3, SUB, LANES), f32),
                   jax.ShapeDtypeStruct((n_batch,) + gx_my.shape[N1:], bf16), jax.ShapeDtypeStruct((n_batch,) + gx_my.shape[N1:], bf16)),
        in_specs=[any_spec] * 6,
        out_specs=(vmem, vmem, any_spec, any_spec),
        scratch_shapes=[
            pltpu.VMEM((N2, RING, RING, RING, N3, SUB, wide), f32), pltpu.VMEM((N2, RING, RING, RING, N3, SUB, wide), bf16),
            pltpu.VMEM((N2, N3, RING, RING, N3, SUB, wide), bf16), pltpu.VMEM((N2, N2, N2, RING, N3, SUB, wide), bf16), pltpu.VMEM((N2, N2, RING, RING, N3, SUB, wide), bf16),
            pltpu.VMEM((N2, N3, RING, N3, SUB, wide), bf16), pltpu.VMEM((N2, N2, N2, N3, SUB, wide), bf16), pltpu.VMEM((N2, N2, RING, N3, SUB, wide), bf16),
            pltpu.VMEM((N2, RING, N3, SUB, wide), bf16), pltpu.VMEM((N2, N3, N3, SUB, wide), bf16), pltpu.VMEM((RING, RING, N3, SUB, LANES), f32),
            dma((N2, RING)), dma((N2, RING)), dma((N2, RING)), dma((N2, 12)), dma((N2, 12)), dma((N2, N3)), dma((N2, N3)), dma((N3,)), dma((N3,)), dma((6,)), dma((6,)), dma((RING,)),
        ],
        cost_estimate=pl.CostEstimate(flops=60 * 10**9, bytes_accessed=30 * 10**6, transcendentals=N0),
        compiler_params=pltpu.CompilerParams(collective_id=N1, has_side_effects=True, vmem_limit_bytes=60 * KIB * KIB),
    )(g_pack, g_send, gx_my, *y_blocks)


def solution(mesh):
    n_tp = mesh.shape['tp']
    n_fsdp = mesh.shape['fsdp']

    def device_step(x_in, dy_out, ln_gain, w_q, w_k, w_v, w_o, w_gate, w_up, w_down):
        bf16 = jnp.bfloat16
        f32 = jnp.float32
        n_batch, seq_len, width = x_in.shape
        head_dim = w_k.shape[N1]
        rows = w_q.shape[N0]
        nq = w_q.shape[N1]
        nf = w_gate.shape[N1]
        part = N2 * head_dim // n_tp
        mine = n_batch // n_tp
        tp = lax.axis_index('tp')
        core = lax.rem(lax.axis_index('fsdp'), N2)
        gain_hi = lax.reduce_precision(ln_gain, SUB, 7)
        gain_mid = lax.reduce_precision(ln_gain - gain_hi, SUB, 7)
        gain_lo = ln_gain - gain_hi - gain_mid
        gain_cols = jnp.stack([gain_hi, gain_mid, gain_lo], axis=N1).astype(bf16)
        kv_mine = lax.dynamic_slice_in_dim(jnp.concatenate([w_k, w_v], axis=N1), tp * part, part, N1)
        small = jnp.concatenate([kv_mine, gain_cols, jnp.zeros((rows, LANES - part - N3), bf16)], axis=N1)
        down = w_down.T
        packed = jnp.stack([jnp.concatenate([w_gate, w_q, w_o.T, small, down[:, :LANES]], axis=N1), jnp.concatenate([w_up, down[:, LANES:]], axis=N1)])
        wide = packed.shape[N2]
        tables = rope_tables(seq_len, head_dim)
        full = gather_weights(packed).reshape(N2, n_tp, width, wide)
        small_full = full[N0, :, :, KV_AT:KV_AT + LANES]
        w_kv = jnp.concatenate([small_full[n, :, :part] for n in range(n_tp)], axis=N1)
        gain3 = small_full[N0, :, part:part + N3].astype(f32)
        gain_row = (gain3[:, N0] + gain3[:, N1] + gain3[:, N2]).reshape(N1, width)

        who = jnp.stack([tp, core]).astype(jnp.int32)
        y_tok, gx_tok, g_own, g_oth = layer_step(x_in, dy_out, gain_row, full, w_kv, tables, who, seq_len)
        y_my = y_tok.reshape(mine, seq_len, width)
        below = lax.ppermute(y_my, 'tp', [(n, (n + N1) % n_tp) for n in range(n_tp)])
        above = lax.ppermute(y_my, 'tp', [(n, (n - N1) % n_tp) for n in range(n_tp)])
        split = (N2, n_tp, RING, RING, N3, SUB, wide)
        w_sum, kv_sum, grad_x, y_out = sum_grads(g_own.reshape(split), g_oth.reshape(split), gx_tok.reshape(mine, seq_len, width), (y_my, below, above), n_batch)
        w0 = w_sum[N0].reshape(rows, wide)
        w1 = w_sum[N1].reshape(rows, wide)
        kv_all = jnp.swapaxes(kv_sum.reshape(n_tp, rows, LANES)[:, :, :part], N0, N1).reshape(rows, N2 * head_dim)
        grad_wgate = w0[:, :nf]
        grad_wq = w0[:, nf:nf + nq]
        grad_wo = w0[:, nf + nq:nf + N2 * nq].T
        grad_wdown = jnp.concatenate([w0[:, wide - LANES:], w1[:, nf:]], axis=N1).T
        grad_wup = w1[:, :nf]
        grad_wk = kv_all[:, :head_dim]
        grad_wv = kv_all[:, head_dim:]
        grad_gain = kv_sum[N0].reshape(rows, LANES)[:, part]
        return (y_out, grad_x, grad_gain, grad_wq, grad_wk, grad_wv, grad_wo, grad_wgate, grad_wup, grad_wdown)

    act_spec = P('fsdp', None, None)
    row_spec = P('fsdp', 'tp')
    kv_spec = P('fsdp', None)
    col_spec = P('tp', 'fsdp')
    in_specs = (act_spec, act_spec, P('fsdp'), row_spec, kv_spec, kv_spec, col_spec, row_spec, row_spec, col_spec)
    out_specs = (act_spec, act_spec, P('fsdp'), row_spec, kv_spec, kv_spec, col_spec, row_spec, row_spec, col_spec)
    return jax.shard_map(device_step, mesh=mesh, in_specs=in_specs, out_specs=out_specs, check_vma=False)
```

```python
import jax
import jax.numpy as jnp
from jax import lax
from jax.sharding import PartitionSpec as P
from jax.experimental import pallas as pl
from jax.experimental.pallas import tpu as pltpu


N0, N1, N2, N3 = range(4)
RING = 4
SUB = 8
LANES = 128
PAIR = 256
KIB = 1024
ALL = Ellipsis
KV_AT = 1152
MESH_ID = pl.DeviceIdType.MESH


def gather_kernel(p_ref, g_ref, hold, lsem, s1, r1, s2, r2, s3, r3, ds, dr):
    t = lax.axis_index('tp')
    f = lax.axis_index('fsdp')
    c = lax.rem(f, N2)
    at = {'x': t, 'y': lax.rem(lax.div(f, N2), RING), 'z': lax.div(f, SUB)}

    def up(i, d):
        return lax.rem(i + d, RING)

    def dev(where, cc):
        return {'tp': where['x'], 'fsdp': (where['z'] * RING + where['y']) * N2 + cc}

    def peer(axis, d):
        return dev({**at, axis: up(at[axis], d)}, c)

    partner = dev(at, N1 - c)
    barrier = pltpu.get_barrier_semaphore()
    greeted = [partner] + [peer(axis, d) for axis in 'xyz' for d in (N1, N2, N3)]
    for who in greeted:
        pl.semaphore_signal(barrier, inc=N1, device_id=who, device_id_type=MESH_ID)
    own = pltpu.make_async_copy(p_ref, hold, lsem.at[N0])
    own.start()
    pl.semaphore_wait(barrier, len(greeted))

    sent = []

    def push(src, dst, s_sem, r_sem, who):
        copy = pltpu.make_async_remote_copy(src_ref=src, dst_ref=dst, send_sem=s_sem, recv_sem=r_sem, device_id=who, device_id_type=MESH_ID)
        copy.start()
        sent.append(copy)

    def landed(ref, s_sem, r_sem):
        pltpu.make_async_remote_copy(src_ref=ref, dst_ref=ref, send_sem=s_sem, recv_sem=r_sem, device_id=partner, device_id_type=MESH_ID).wait_recv()

    def view(k, h, fixed, core):
        spot = [fixed.get(axis, slice(None)) for axis in 'xzy']
        return g_ref.at[h, spot[N0], spot[N1], spot[N2], core, k]

    orders = ('xyz', 'yzx', 'zxy')
    both = slice(None)
    across = []

    def share(k, h, fixed, n):
        push(view(k, h, fixed, c), view(k, h, fixed, c), ds.at[k, n], dr.at[k, n], partner)
        across.append((k, h, fixed, n))

    def ring_start(k, axis, fixed, ss, rr):
        here = {**fixed, axis: at[axis]}
        for n in range(N2):
            push(view(k, n, here, c), view(k, n, here, c), ss.at[k, n], rr.at[k, n], peer(axis, N1))
            push(view(k, N1 - n, here, c), view(k, N1 - n, here, c), ss.at[k, N3 - n], rr.at[k, N3 - n], peer(axis, N3))

    def ring_forward(k, axis, fixed, ss, rr):
        for h, d, n in ((N0, N3, N0), (N1, N1, N3)):
            there = {**fixed, axis: up(at[axis], d)}
            landed(view(k, h, there, c), ss.at[k, n], rr.at[k, n])
            push(view(k, h, there, c), view(k, h, there, c), ss.at[k, RING + h], rr.at[k, RING + h], peer(axis, RING - d))

    def ring_share(k, axis, fixed, ss, rr, base):
        for m, (h, d, n) in enumerate(((N0, N3, N0), (N1, N1, N3), (N1, N3, N1), (N0, N1, N2), (N0, N2, RING), (N1, N2, 5))):
            there = {**fixed, axis: up(at[axis], d)}
            if n not in (N0, N3):
                landed(view(k, h, there, c), ss.at[k, n], rr.at[k, n])
            share(k, h, there, base + m)

    own.wait()
    own = pltpu.make_async_copy(hold, g_ref.at[:, at['x'], at['z'], at['y'], c], lsem.at[N0])
    own.start()
    for k, order in enumerate(orders):
        for d in (N1, N3, N2):
            push(hold.at[:, k], view(k, both, at, c), s1.at[k, d - N1], r1.at[k, d - N1], peer(order[N0], d))
    own.wait()
    second = []
    third = []
    for k, order in enumerate(orders):
        for d in (N1, N3, N2):
            landed(view(k, both, {**at, order[N0]: up(at[order[N0]], RING - d)}, c), s1.at[k, d - N1], r1.at[k, d - N1])
        fixed = {order[N2]: at[order[N2]]}
        second.append((k, order[N1], fixed, s2, r2))
        third.append((k, order[N2], {}, s3, r3))
        ring_start(*second[k])
    for k, order in enumerate(orders):
        here = {order[N1]: at[order[N1]], order[N2]: at[order[N2]]}
        share(k, N0, here, N0)
        share(k, N1, here, N1)
    for k in range(N3):
        ring_forward(*second[k])
    for k in range(N3):
        ring_share(*second[k], N2)
        ring_start(*third[k])
    for k in range(N3):
        ring_forward(*third[k])
    for k in range(N3):
        ring_share(*third[k], SUB)
    for k, h, fixed, n in across:
        landed(view(k, h, fixed, N1 - c), ds.at[k, n], dr.at[k, n])
    for copy in sent:
        copy.wait_send()


def gather_weights(packed):
    dma = pltpu.SemaphoreType.DMA
    any_spec = pl.BlockSpec(memory_space=pl.ANY)
    wide = packed.shape[N2]
    return pl.pallas_call(
        gather_kernel,
        name='gather_weights',
        out_shape=jax.ShapeDtypeStruct((N2, RING, RING, RING, N2, N3, SUB, wide), packed.dtype),
        in_specs=[any_spec],
        out_specs=any_spec,
        scratch_shapes=[pltpu.VMEM((N2, N3, SUB, wide), packed.dtype), dma((N1,)), dma((N3, N3)), dma((N3, N3)), dma((N3, 6)), dma((N3, 6)), dma((N3, 6)), dma((N3, 6)), dma((N3, 14)), dma((N3, 14))],
        compiler_params=pltpu.CompilerParams(collective_id=N2, has_side_effects=True, vmem_limit_bytes=60 * KIB * KIB),
    )(packed.reshape(N2, N3, SUB, wide))


NT = (((N1,), (N1,)), ((), ()))
NN = (((N1,), (N0,)), ((), ()))
TN = (((N0,), (N0,)), ((), ()))


def dot(left, right, dims=NN):
    return lax.dot_general(left, right, dims, preferred_element_type=jnp.float32)


def by_class(out, cols, vals, core):
    for n in range(32):
        out[lax.rem(n % N2 + core, N2), 24 * (n // N2):24 * (n // N2) + 24, cols] = vals[24 * n:24 * n + 24]


def proj_kernel(who_ref, x_ref, dy_ref, gain_ref, w0_ref, w1_ref, wkv_ref, ht_out, dyt_out, q_out, kv_out, do_out, act_out, dg_out, du_out, h_out):
    f32 = jnp.float32
    bf16 = jnp.bfloat16
    tokens, width = h_out.shape
    dy_tok = dy_ref[ALL].reshape(tokens, width)

    @pl.when(pl.program_id(N0) == N0)
    def _():
        for n in range(tokens // LANES):
            at = slice(n * LANES, n * LANES + LANES)
            seq, row = divmod(n * LANES, x_ref.shape[N1])
            x_f32 = x_ref[seq, row:row + LANES, :].astype(f32)
            x_cent = x_f32 - jnp.mean(x_f32, axis=-N1, keepdims=True)
            x_var = jnp.mean(x_cent * x_cent, axis=-N1, keepdims=True)
            h_norm = (x_cent * lax.rsqrt(x_var + 1e-5) * gain_ref[ALL]).astype(bf16)
            h_out[at, :] = h_norm
            by_class(ht_out, at, h_norm.astype(f32).T.astype(bf16), who_ref[N1])
            by_class(dyt_out, at, dy_ref[seq, row:row + LANES, :].astype(f32).T.astype(bf16), who_ref[N1])
        kv_out[ALL] = dot(h_out[ALL], wkv_ref[ALL]).astype(bf16)

    for n in range(N3):
        cols = slice(n * PAIR, n * PAIR + PAIR)
        gate = dot(h_out[ALL], w0_ref[N0, N0, :, cols]).astype(bf16).astype(f32)
        up = dot(h_out[ALL], w1_ref[N0, N0, :, cols]).astype(bf16).astype(f32)
        if n == N0:
            d_low = dot(dy_tok, w0_ref[N0, N0, :, 1280:1408])
            d_act = jnp.concatenate([d_low, dot(dy_tok, w1_ref[N0, N0, :, 768:896])], axis=N1)
        else:
            d_act = dot(dy_tok, w1_ref[N0, N0, :, 640 + n * PAIR:896 + n * PAIR])
        d_act = d_act.astype(bf16).astype(f32)
        sig = 0.5 * jnp.tanh(0.5 * gate) + 0.5
        silu = gate * sig
        act_out[N0, :, cols] = (silu * up).astype(bf16)
        du_out[N0, :, cols] = (d_act * silu).astype(bf16)
        dg_out[N0, :, cols] = (d_act * up * (sig + silu * (1.0 - sig))).astype(bf16)
    q_out[N0] = dot(h_out[ALL], w0_ref[N0, N0, :, 768:KIB]).astype(bf16)
    do_out[N0] = dot(dy_tok, w0_ref[N0, N0, :, 896:1152]).astype(bf16)


def att_kernel(q_ref, kv_ref, do_ref, cq_ref, sq_ref, ck_ref, sk_ref, o_out, dq_out, dkv_out, dk_lo, dk_hi, dv_lo, dv_hi):
    f32 = jnp.float32
    bf16 = jnp.bfloat16
    seq_len = kv_ref.shape[N0]
    lane = lax.broadcasted_iota(jnp.int32, (seq_len, LANES), N1)
    low = lane < 64
    first = lax.rem(lane, 64) < 32
    causal = lax.broadcasted_iota(jnp.int32, (seq_len, seq_len), N0) >= lax.broadcasted_iota(jnp.int32, (seq_len, seq_len), N1)

    def other(vals):
        return jnp.where(first, pltpu.roll(vals, 96, N1), pltpu.roll(vals, 32, N1))

    kv_f32 = kv_ref[ALL].astype(f32)
    kv_rot = kv_f32 * ck_ref[ALL] + other(kv_f32) * sk_ref[ALL]
    zero = jnp.zeros_like(kv_rot)
    k_lo = jnp.where(low, kv_rot, zero)
    v_hi = jnp.where(low, zero, kv_rot)
    k_hi = pltpu.roll(k_lo, 64, N1).astype(bf16)
    v_lo = pltpu.roll(v_hi, 64, N1).astype(bf16)
    k_lo = k_lo.astype(bf16)
    v_hi = v_hi.astype(bf16)
    for ref in (dk_lo, dk_hi, dv_lo, dv_hi):
        ref[ALL] = jnp.zeros_like(ref)

    def head(q_tile, k_part, v_part, do_tile):
        scores = jnp.where(causal, dot(q_tile, k_part, NT), -1e30)
        exp_val = jnp.exp(scores - jnp.max(scores, axis=-N1, keepdims=True))
        prob = exp_val * (1.0 / jnp.sum(exp_val, axis=-N1, keepdims=True))
        d_prob = dot(do_tile, v_part, NT).astype(bf16).astype(f32)
        d_score = prob * (d_prob - jnp.sum(d_prob * prob, axis=-N1, keepdims=True))
        return prob.astype(bf16), d_score.astype(bf16)

    def block(tt, carry):
        tiles = []
        for n in range(N2):
            cols = slice(n * LANES, n * LANES + LANES)
            vals = q_ref[tt, :, cols].astype(f32)
            tiles.append(((vals * cq_ref[ALL] + other(vals) * sq_ref[ALL]) * 0.125).astype(bf16))
        do0 = do_ref[tt, :, N0:LANES]
        do1 = do_ref[tt, :, LANES:PAIR]
        p0, s0 = head(tiles[N0], k_lo, v_hi, do0)
        p1, s1 = head(tiles[N0], k_hi, v_lo, do1)
        p2, s2 = head(tiles[N1], k_lo, v_hi, do1)
        o_out[tt, :, N0:LANES] = dot(p0, v_hi).astype(bf16)
        o_out[tt, :, LANES:PAIR] = (dot(p1, v_lo) + dot(p2, v_hi)).astype(bf16)
        dv_hi[ALL] += dot(p0, do0, TN) + dot(p2, do1, TN)
        dv_lo[ALL] += dot(p1, do1, TN)
        dk_lo[ALL] += dot(s0, tiles[N0], TN) + dot(s2, tiles[N1], TN)
        dk_hi[ALL] += dot(s1, tiles[N0], TN)
        for n, grad in ((N0, dot(s0, k_lo) + dot(s1, k_hi)), (N1, dot(s2, k_lo))):
            grad = grad.astype(bf16).astype(f32) * 0.125
            dq_out[tt, :, n * LANES:n * LANES + LANES] = (grad * cq_ref[ALL] - other(grad) * sq_ref[ALL]).astype(bf16)
        return carry
    lax.fori_loop(N0, q_ref.shape[N0], block, N0)
    dk = (dk_lo[ALL] + pltpu.roll(dk_hi[ALL], 64, N1)).astype(bf16).astype(f32)
    dk_raw = dk * ck_ref[ALL] - other(dk) * sk_ref[ALL]
    dv = dv_hi[ALL] + pltpu.roll(dv_lo[ALL], 64, N1)
    dkv_out[ALL] = jnp.where(low, dk_raw, dv).astype(bf16)


def back_kernel(who_ref, x_ref, dy_ref, gain_ref, w0_ref, w1_ref, wkv_ref, o_ref, act_ref, dq_ref, dg_ref, du_ref, dkv_ref, y_out, gx_out, gcol_out, y_acc, dh_acc):
    f32 = jnp.float32
    bf16 = jnp.bfloat16
    step = pl.program_id(N0)
    tokens, width = y_acc.shape
    y_left = jnp.concatenate([o_ref[N0], act_ref[N0]], axis=N1)
    y_right = jnp.concatenate([w0_ref[N0, N0, :, 896:1152], w0_ref[N0, N0, :, 1280:1408], w1_ref[N0, N0, :, 768:1408]], axis=N1)
    h_left = jnp.concatenate([dg_ref[N0], dq_ref[N0], du_ref[N0]], axis=N1)
    h_right = jnp.concatenate([w0_ref[N0, N0, :, N0:KIB], w1_ref[N0, N0, :, N0:768]], axis=N1)
    y_part = dot(y_left, y_right, NT)
    dh_part = dot(h_left, h_right, NT)

    @pl.when(step == N0)
    def _():
        y_acc[ALL] = y_part
        dh_acc[ALL] = dh_part + dot(dkv_ref[ALL], wkv_ref[ALL], NT)

    @pl.when(step > N0)
    def _():
        y_acc[ALL] += y_part
        dh_acc[ALL] += dh_part

    @pl.when(step == pl.num_programs(N0) - N1)
    def _():
        gain = jnp.zeros((N1, width), f32)
        for n in range(tokens // LANES):
            at = slice(n * LANES, n * LANES + LANES)
            seq, row = divmod(n * LANES, x_ref.shape[N1])
            x_f32 = x_ref[seq, row:row + LANES, :].astype(f32)
            y_out[at, :] = (x_f32 + y_acc[at, :]).astype(bf16)
            x_cent = x_f32 - jnp.mean(x_f32, axis=-N1, keepdims=True)
            rstd = lax.rsqrt(jnp.mean(x_cent * x_cent, axis=-N1, keepdims=True) + 1e-5)
            x_hat = x_cent * rstd
            dh = dh_acc[at, :].astype(bf16).astype(f32)
            gain += jnp.sum(dh * x_hat, axis=N0, keepdims=True)
            d_hat = dh * gain_ref[ALL]
            dx = rstd * (d_hat - jnp.mean(d_hat, axis=-N1, keepdims=True) - x_hat * jnp.mean(d_hat * x_hat, axis=-N1, keepdims=True))
            gx_out[at, :] = (dy_ref[seq, row:row + LANES, :].astype(f32) + dx).astype(bf16)
        lane = lax.broadcasted_iota(jnp.int32, (width, LANES), N1)
        by_class(gcol_out, slice(None), jnp.where(lane == 32, jnp.broadcast_to(gain, (LANES, width)).T, 0.0), who_ref[N1])


def wgrad_kernel(ht_ref, dyt_ref, gcol_ref, o_ref, act_ref, dq_ref, dg_ref, du_ref, dkv_ref, own_out, oth_out):
    tt = pl.program_id(N0)
    half = ht_ref.shape[N1]
    lane = lax.broadcasted_iota(jnp.int32, (half, LANES), N1)
    ht = ht_ref[ALL].reshape(N2 * half, ht_ref.shape[N2])
    dyt = dyt_ref[ALL].reshape(N2 * half, dyt_ref.shape[N2])

    def put(n, cols, vals):
        own_out[n, N0, :, cols] = vals[:half]
        oth_out[n, N0, :, cols] = vals[half:].astype(jnp.bfloat16)

    for k in range(N3):
        cols = slice(k * PAIR, k * PAIR + PAIR)
        put(N0, cols, dot(ht, dg_ref[N0, :, cols]))
        put(N1, cols, dot(ht, du_ref[N0, :, cols]))
    g_q = dot(ht, dq_ref[N0])
    g_o = dot(dyt, o_ref[N0])
    put(N0, slice(768, 896), g_q[:, N0:LANES])
    put(N0, slice(896, KIB), g_q[:, LANES:PAIR] + g_o[:, N0:LANES])
    put(N0, slice(KIB, 1152), g_o[:, LANES:PAIR])
    g_kv = dot(ht, dkv_ref[ALL])
    for cls, out in ((N0, own_out), (N1, oth_out)):
        part = pltpu.roll(g_kv[cls * half:cls * half + half], lax.rem(LANES - 32 * tt, LANES), N1)
        out[N0, N0, :, 1152:1280] = (jnp.where(lane < 32, part, 0.0) + gcol_ref[cls]).astype(out.dtype)
    put(N0, slice(1280, 1408), dot(dyt, act_ref[N0, :, N0:LANES]))
    for lo, hi in ((LANES, 384), (384, 640), (640, 768)):
        put(N1, slice(lo + 640, hi + 640), dot(dyt, act_ref[N0, :, lo:hi]))


def layer_step(x_in, dy_in, gain_row, w_full, w_kv, tables, who, seq_len):
    f32 = jnp.float32
    bf16 = jnp.bfloat16
    n_tp = w_full.shape[N1]
    wide = w_full.shape[N3]
    width = w_full.shape[N2]
    n_seq = x_in.shape[N0] // n_tp
    tokens = n_seq * seq_len
    half = width // N2

    def whole(shape):
        return pl.BlockSpec(shape, lambda i, *_: (N0,) * len(shape))

    def per(shape):
        return pl.BlockSpec((N1,) + shape, lambda i, *_: (i,) + (N0,) * len(shape))

    w0_spec = pl.BlockSpec((N1, N1, width, wide), lambda i, *_: (N0, i, N0, N0))
    w1_spec = pl.BlockSpec((N1, N1, width, wide), lambda i, *_: (N1, i, N0, N0))
    mine = pl.BlockSpec((n_seq, seq_len, width), lambda i, who_ref: (who_ref[N0], N0, N0))
    tok = whole((tokens, width))
    classes = whole((N2, half, tokens))
    params = pltpu.CompilerParams(dimension_semantics=('arbitrary',), vmem_limit_bytes=56 * KIB * KIB)
    wide_t = jax.ShapeDtypeStruct((n_tp, tokens, width), bf16)
    pair_t = jax.ShapeDtypeStruct((n_tp, tokens, PAIR), bf16)
    row_t = jax.ShapeDtypeStruct((tokens, width), bf16)
    class_t = jax.ShapeDtypeStruct((N2, half, tokens), bf16)
    kv_t = jax.ShapeDtypeStruct((tokens, LANES), bf16)
    work = pl.CostEstimate(flops=13 * 10**9, bytes_accessed=40 * 10**6, transcendentals=N0)
    h_t, dy_t, q_raw, kv_raw, d_o, act, d_gate, d_up = pl.pallas_call(
        proj_kernel, name='proj',
        grid_spec=pltpu.PrefetchScalarGridSpec(
            num_scalar_prefetch=N1, grid=(n_tp,),
            in_specs=[mine, mine, whole((N1, width)), w0_spec, w1_spec, whole((width, LANES))],
            out_specs=(classes, classes, per((tokens, PAIR)), whole((tokens, LANES)), per((tokens, PAIR)), per((tokens, width)), per((tokens, width)), per((tokens, width))),
            scratch_shapes=[pltpu.VMEM((tokens, width), bf16)]),
        out_shape=(class_t, class_t, pair_t, kv_t, pair_t, wide_t, wide_t, wide_t),
        compiler_params=params, cost_estimate=work,
    )(who, x_in, dy_in, gain_row, w_full, w_full, w_kv)

    pair_spec = pl.BlockSpec((n_tp, seq_len, PAIR), lambda i: (N0, i, N0))
    kv_spec = pl.BlockSpec((seq_len, LANES), lambda i: (i, N0))
    table = whole((seq_len, LANES))
    att, d_q, d_kv = pl.pallas_call(
        att_kernel, name='attention', grid=(n_seq,),
        in_specs=[pair_spec, kv_spec, pair_spec, table, table, table, table],
        out_specs=(pair_spec, pair_spec, kv_spec),
        out_shape=(pair_t, pair_t, kv_t),
        scratch_shapes=[pltpu.VMEM((seq_len, LANES), f32)] * RING,
        compiler_params=params, cost_estimate=work,
    )(q_raw, kv_raw, d_o, *tables)

    gcol_t = jax.ShapeDtypeStruct((N2, half, LANES), f32)
    y_tok, gx_tok, gain_col = pl.pallas_call(
        back_kernel, name='back',
        grid_spec=pltpu.PrefetchScalarGridSpec(
            num_scalar_prefetch=N1, grid=(n_tp,),
            in_specs=[mine, mine, whole((N1, width)), w0_spec, w1_spec, whole((width, LANES)), per((tokens, PAIR)), per((tokens, width)), per((tokens, PAIR)),
                      per((tokens, width)), per((tokens, width)), whole((tokens, LANES))],
            out_specs=(tok, tok, whole((N2, half, LANES))),
            scratch_shapes=[pltpu.VMEM((tokens, width), f32)] * N2),
        out_shape=(row_t, row_t, gcol_t),
        compiler_params=params, cost_estimate=work,
    )(who, x_in, dy_in, gain_row, w_full, w_full, w_kv, att, act, d_q, d_gate, d_up, d_kv)

    class_spec = pl.BlockSpec((N2, N1, half, wide), lambda i: (N0, i, N0, N0))
    own, oth = pl.pallas_call(
        wgrad_kernel, name='wgrad', grid=(n_tp,),
        in_specs=[classes, classes, whole((N2, half, LANES)), per((tokens, PAIR)), per((tokens, width)), per((tokens, PAIR)),
                  per((tokens, width)), per((tokens, width)), whole((tokens, LANES))],
        out_specs=(class_spec, class_spec),
        out_shape=(jax.ShapeDtypeStruct((N2, n_tp, half, wide), f32), jax.ShapeDtypeStruct((N2, n_tp, half, wide), bf16)),
        compiler_params=params, cost_estimate=work,
    )(h_t, dy_t, gain_col, att, act, d_q, d_gate, d_up, d_kv)
    return y_tok, gx_tok, own, oth


def rope_tables(seq_len, head_dim):
    f32 = jnp.float32
    half_dim = head_dim // N2
    inv_freq = jnp.power(10000.0, -2.0 * jnp.arange(half_dim, dtype=f32) / head_dim)
    angle = jnp.arange(seq_len, dtype=f32)[:, None] * inv_freq[None, :]
    cos_t = jnp.cos(angle)
    sin_t = jnp.sin(angle)
    cos_h = jnp.concatenate([cos_t, cos_t], axis=N1)
    sin_h = jnp.concatenate([-sin_t, sin_t], axis=N1)
    cos_q = jnp.concatenate([cos_h, cos_h], axis=N1)
    sin_q = jnp.concatenate([sin_h, sin_h], axis=N1)
    cos_k = jnp.concatenate([cos_h, jnp.ones_like(cos_h)], axis=N1)
    sin_k = jnp.concatenate([sin_h, jnp.zeros_like(sin_h)], axis=N1)
    return cos_q, sin_q, cos_k, sin_k


def sum_kernel(g_ref, gs_ref, gx_ref, y_ref, below_ref, above_ref, w_out, kv_out, gx_out, y_out, acc, rp, sa, ra1, ra2, sb, rb1, rb2, sc, rc, kvx, gsem, d2s, d2r, ss, rs, cs, cr, ks, kr, xs, xr, lsem, keep):
    f32 = jnp.float32
    bf16 = jnp.bfloat16
    t = lax.axis_index('tp')
    f = lax.axis_index('fsdp')
    c = lax.rem(f, N2)
    yy = lax.rem(lax.div(f, N2), RING)
    zz = lax.div(f, SUB)

    def dev(tt, zc, yc, cc):
        return {'tp': tt, 'fsdp': (zc * RING + yc) * N2 + cc}

    def up(i, d):
        return lax.rem(i + d, RING)

    partner = dev(t, zz, yy, N1 - c)
    xp = [dev(up(t, d), zz, yy, c) for d in range(RING)]
    z_dev = [dev(t, up(zz, d), yy, c) for d in range(RING)]
    y_dev = [dev(t, zz, up(yy, d), c) for d in range(RING)]
    barrier = pltpu.get_barrier_semaphore()
    peers = [partner, xp[N1], xp[N2], xp[N3], z_dev[N1], z_dev[N3], y_dev[N1], y_dev[N3]]
    for peer in peers:
        pl.semaphore_signal(barrier, inc=N1, device_id=peer, device_id_type=MESH_ID)

    def rcopy(src, dst, s_sem, r_sem, peer):
        return pltpu.make_async_remote_copy(src_ref=src, dst_ref=dst, send_sem=s_sem, recv_sem=r_sem, device_id=peer, device_id_type=MESH_ID)

    ring_a = [zz, yy]
    ring_b = [yy, zz]
    dev_a = [z_dev, y_dev]
    dev_b = [y_dev, z_dev]
    order = [N2, N1, N3, N0]

    def g_view(col, j):
        return g_ref.at[N0, :, j] if col == N0 else g_ref.at[N1, :, :, j]

    def gs_view(col, j):
        return gs_ref.at[N0, :, j] if col == N0 else gs_ref.at[N1, :, :, j]

    load = [[None] * RING for _ in range(N2)]
    pair = [[None] * RING for _ in range(N2)]
    for n, d in enumerate(order):
        for col in range(N2):
            j = up(ring_a[col], d)
            load[col][n] = pltpu.make_async_copy(g_view(col, j), acc.at[col, n], gsem.at[col, n])
            load[col][n].start()
    pl.semaphore_wait(barrier, len(peers))
    for n, d in enumerate(order):
        for col in range(N2):
            j = up(ring_a[col], d)
            pair[col][n] = rcopy(gs_view(col, j), rp.at[col, n], d2s.at[col, n], d2r.at[col, n], partner)
            pair[col][n].start()
    mine = gx_ref.shape[N0]
    my_rows = pl.ds(t * mine, mine)
    lower = pl.ds(up(t, N3) * mine, mine)
    upper = pl.ds(up(t, N1) * mine, mine)
    y_up = rcopy(below_ref.at[:, pl.ds(N0, LANES)], y_out.at[lower, pl.ds(N0, LANES)], xs.at[RING], xr.at[RING], xp[N1])
    y_dn = rcopy(above_ref.at[:, pl.ds(LANES, LANES)], y_out.at[upper, pl.ds(LANES, LANES)], xs.at[5], xr.at[5], xp[N3])
    y_up.start()
    y_dn.start()
    x_up = rcopy(gx_ref, gx_out.at[my_rows], xs.at[N0], xr.at[N0], xp[N1])
    x_dn = rcopy(gx_ref, gx_out.at[my_rows], xs.at[N1], xr.at[N1], xp[N3])
    x_up.start()
    x_dn.start()
    local = ((gx_ref, gx_out, my_rows), (y_ref, y_out, my_rows), (below_ref, y_out, lower), (above_ref, y_out, upper))
    taken = [pltpu.make_async_copy(ref, keep.at[n], lsem.at[n]) for n, (ref, _, _) in enumerate(local)]
    placed = [pltpu.make_async_copy(keep.at[n], out.at[place], lsem.at[n]) for n, (_, out, place) in enumerate(local)]
    for copy in taken:
        copy.start()

    def each(count, body):
        def step(n, carry):
            body(n)
            return carry
        lax.fori_loop(N0, count, step, N0)

    def arrived(col, n):
        load[col][n].wait()
        pair[col][n].wait_recv()

    sends = []

    def send(src, dst, s_sem, r_sem, peer):
        copy = rcopy(src, dst, s_sem, r_sem, peer)
        copy.start()
        sends.append(copy)
        return copy

    for col in range(N2):
        arrived(col, N0)

        def first(q, col=col):
            tt = lax.div(q, 12)
            a2 = lax.rem(lax.div(q, N3), RING)
            r = lax.rem(q, N3)
            sa[col, N0, a2, tt, r] = (acc[col, N0, tt, a2, r] + rp[col, N0, tt, a2, r].astype(f32)).astype(bf16)
        each(48, first)
        send(sa.at[col, N0, pl.ds(N0, N2)], ra1.at[col, N0], ss.at[col, N0], rs.at[col, N0], dev_a[col][N1])
        send(sa.at[col, N0, pl.ds(N2, N2)], ra1.at[col, N1], ss.at[col, N1], rs.at[col, N1], dev_a[col][N3])
    for col in range(N2):
        for n, base, peer in ((N1, N2, N1), (N2, N0, N3)):
            arrived(col, n)

            def plain(q, col=col, n=n, base=base):
                a2 = base + lax.div(q, 12)
                tt = lax.rem(lax.div(q, N3), RING)
                r = lax.rem(q, N3)
                sa[col, n, a2, tt, r] = (acc[col, n, tt, a2, r] + rp[col, n, tt, a2, r].astype(f32)).astype(bf16)
            each(24, plain)
            send(sa.at[col, n, pl.ds(base, N2)], ra2.at[col, n - N1, pl.ds(base, N2)], ss.at[col, n + N1], rs.at[col, n + N1], dev_a[col][peer])
    for col in range(N2):
        for n, base, peer in ((N1, N0, N1), (N2, N2, N3)):
            rcopy(sa.at[col, N0, pl.ds(N0, N2)], ra1.at[col, n - N1], ss.at[col, n - N1], rs.at[col, n - N1], dev_a[col][peer]).wait_recv()

            def joined(q, col=col, n=n, base=base):
                h = lax.div(q, 12)
                a2 = base + h
                tt = lax.rem(lax.div(q, N3), RING)
                r = lax.rem(q, N3)
                val = acc[col, n, tt, a2, r] + rp[col, n, tt, a2, r].astype(f32) + ra1[col, n - N1, h, tt, r].astype(f32)
                sa[col, n, a2, tt, r] = val.astype(bf16)
            each(24, joined)
            send(sa.at[col, n, pl.ds(base, N2)], ra2.at[col, n - N1, pl.ds(base, N2)], ss.at[col, n + N3], rs.at[col, n + N3], dev_a[col][peer])
    for n in range(RING):
        taken[n].wait()
        placed[n].start()
    x_up.wait_recv()
    x_dn.wait_recv()
    half_dn = gx_out.at[lower, pl.ds(N0, LANES)]
    half_up = gx_out.at[upper, pl.ds(LANES, LANES)]
    x_up2 = rcopy(half_dn, half_dn, xs.at[N2], xr.at[N2], xp[N1])
    x_dn2 = rcopy(half_up, half_up, xs.at[N3], xr.at[N3], xp[N3])
    x_up2.start()
    x_dn2.start()
    for col in range(N2):
        arrived(col, N3)
        for n, base, s in ((N1, N2, N2), (N2, N0, N3), (N1, N0, RING), (N2, N2, 5)):
            rcopy(sa.at[col, n, pl.ds(base, N2)], ra2.at[col, n - N1, pl.ds(base, N2)], ss.at[col, s], rs.at[col, s], partner).wait_recv()

        def own(q, col=col):
            a2 = lax.div(q, 12)
            tt = lax.rem(lax.div(q, N3), RING)
            r = lax.rem(q, N3)
            val = acc[col, N3, tt, a2, r] + rp[col, N3, tt, a2, r].astype(f32) + ra2[col, N0, a2, tt, r].astype(f32) + ra2[col, N1, a2, tt, r].astype(f32)
            acc[col, N3, tt, a2, r] = val
        each(48, own)
        far = up(ring_b[col], N2)

        def first_b(q, col=col, far=far):
            tt = lax.div(q, N3)
            r = lax.rem(q, N3)
            sb[col, N0, tt, r] = acc[col, N3, tt, far, r].astype(bf16)
        each(12, first_b)
        send(sb.at[col, N0, pl.ds(N0, N2)], rb1.at[col, N0], ss.at[col, 6], rs.at[col, 6], dev_b[col][N1])
        send(sb.at[col, N0, pl.ds(N2, N2)], rb1.at[col, N1], ss.at[col, 7], rs.at[col, 7], dev_b[col][N3])
        for n, base, peer in ((N1, N2, N1), (N2, N0, N3)):
            pos = up(ring_b[col], peer)

            def plain_b(q, col=col, n=n, base=base, pos=pos):
                tt = base + lax.div(q, N3)
                r = lax.rem(q, N3)
                sb[col, n, tt, r] = acc[col, N3, tt, pos, r].astype(bf16)
            each(6, plain_b)
            send(sb.at[col, n, pl.ds(base, N2)], rb2.at[col, n - N1, pl.ds(base, N2)], ss.at[col, n + 7], rs.at[col, n + 7], dev_b[col][peer])
    for col in range(N2):
        for n, base, peer in ((N1, N0, N1), (N2, N2, N3)):
            rcopy(sb.at[col, N0, pl.ds(N0, N2)], rb1.at[col, n - N1], ss.at[col, n + 5], rs.at[col, n + 5], partner).wait_recv()
            pos = up(ring_b[col], peer)

            def joined_b(q, col=col, n=n, base=base, pos=pos):
                h = lax.div(q, N3)
                tt = base + h
                r = lax.rem(q, N3)
                sb[col, n, tt, r] = (acc[col, N3, tt, pos, r] + rb1[col, n - N1, h, r].astype(f32)).astype(bf16)
            each(6, joined_b)
            send(sb.at[col, n, pl.ds(base, N2)], rb2.at[col, n - N1, pl.ds(base, N2)], ss.at[col, n + 9], rs.at[col, n + 9], dev_b[col][peer])
    for col in range(N2):
        here = ring_b[col]
        for n, base, s in ((N1, N2, SUB), (N2, N0, 9), (N1, N0, 10), (N2, N2, 11)):
            rcopy(sb.at[col, n, pl.ds(base, N2)], rb2.at[col, n - N1, pl.ds(base, N2)], ss.at[col, s], rs.at[col, s], partner).wait_recv()

        def own_b(q, col=col, here=here):
            tt = lax.div(q, N3)
            r = lax.rem(q, N3)
            val = acc[col, N3, tt, here, r] + rb2[col, N0, tt, r].astype(f32) + rb2[col, N1, tt, r].astype(f32)
            acc[col, N3, tt, here, r] = val
            sc[col, tt, r] = val.astype(bf16)
        each(12, own_b)
        for d in (N1, N3, N2):
            to = up(t, d)
            send(sc.at[col, to], rc.at[col, d - N1], cs.at[col, d - N1], cr.at[col, d - N1], xp[d])
        if col == N0:
            def kv_part(q, here=here):
                tt = lax.div(q, N3)
                r = lax.rem(q, N3)
                kvx[t, tt, r] = acc[N0, N3, tt, here, r, :, pl.ds(KV_AT, LANES)]
            each(12, kv_part)
            for d in (N1, N3, N2):
                send(kvx.at[t], kvx.at[t], ks.at[d - N1], kr.at[d - N1], xp[d])
    for col in range(N2):
        here = ring_b[col]
        for d in (N1, N3, N2):
            rcopy(sc.at[col, N0], rc.at[col, d - N1], cs.at[col, d - N1], cr.at[col, d - N1], partner).wait_recv()

        def last(r, col=col, here=here):
            w_out[col, r] = acc[col, N3, t, here, r] + rc[col, N0, r].astype(f32) + rc[col, N1, r].astype(f32) + rc[col, N2, r].astype(f32)
        each(N3, last)
    for d in (N1, N3, N2):
        src = up(t, RING - d)
        rcopy(kvx.at[src], kvx.at[src], ks.at[d - N1], kr.at[d - N1], partner).wait_recv()

    def kv_last(q):
        tt = lax.div(q, N3)
        r = lax.rem(q, N3)
        kv_out[tt, r] = ((kvx[N0, tt, r] + kvx[N1, tt, r]) + kvx[N2, tt, r]) + kvx[N3, tt, r]
    each(12, kv_last)
    for copy in sends:
        copy.wait_send()
    for col in range(N2):
        for n in range(RING):
            pair[col][n].wait_send()
    x_up.wait_send()
    x_dn.wait_send()
    x_up2.wait()
    x_dn2.wait()
    y_up.wait()
    y_dn.wait()
    for copy in placed:
        copy.wait()


def sum_grads(g_pack, g_send, gx_my, y_blocks, n_batch):
    f32 = jnp.float32
    bf16 = jnp.bfloat16
    wide = g_pack.shape[-N1]
    dma = pltpu.SemaphoreType.DMA
    vmem = pl.BlockSpec(memory_space=pltpu.VMEM)
    any_spec = pl.BlockSpec(memory_space=pl.ANY)
    return pl.pallas_call(
        sum_kernel,
        name='sum_grads',
        out_shape=(jax.ShapeDtypeStruct((N2, N3, SUB, wide), f32), jax.ShapeDtypeStruct((RING, N3, SUB, LANES), f32),
                   jax.ShapeDtypeStruct((n_batch,) + gx_my.shape[N1:], bf16), jax.ShapeDtypeStruct((n_batch,) + gx_my.shape[N1:], bf16)),
        in_specs=[any_spec] * 6,
        out_specs=(vmem, vmem, any_spec, any_spec),
        scratch_shapes=[
            pltpu.VMEM((N2, RING, RING, RING, N3, SUB, wide), f32), pltpu.VMEM((N2, RING, RING, RING, N3, SUB, wide), bf16),
            pltpu.VMEM((N2, N3, RING, RING, N3, SUB, wide), bf16), pltpu.VMEM((N2, N2, N2, RING, N3, SUB, wide), bf16), pltpu.VMEM((N2, N2, RING, RING, N3, SUB, wide), bf16),
            pltpu.VMEM((N2, N3, RING, N3, SUB, wide), bf16), pltpu.VMEM((N2, N2, N2, N3, SUB, wide), bf16), pltpu.VMEM((N2, N2, RING, N3, SUB, wide), bf16),
            pltpu.VMEM((N2, RING, N3, SUB, wide), bf16), pltpu.VMEM((N2, N3, N3, SUB, wide), bf16), pltpu.VMEM((RING, RING, N3, SUB, LANES), f32),
            dma((N2, RING)), dma((N2, RING)), dma((N2, RING)), dma((N2, 12)), dma((N2, 12)), dma((N2, N3)), dma((N2, N3)), dma((N3,)), dma((N3,)), dma((6,)), dma((6,)), dma((RING,)), pltpu.VMEM((RING,) + gx_my.shape, bf16),
        ],
        cost_estimate=pl.CostEstimate(flops=60 * 10**9, bytes_accessed=30 * 10**6, transcendentals=N0),
        compiler_params=pltpu.CompilerParams(collective_id=N1, has_side_effects=True, vmem_limit_bytes=60 * KIB * KIB),
    )(g_pack, g_send, gx_my, *y_blocks)


def solution(mesh):
    n_tp = mesh.shape['tp']
    n_fsdp = mesh.shape['fsdp']

    def device_step(x_in, dy_out, ln_gain, w_q, w_k, w_v, w_o, w_gate, w_up, w_down):
        bf16 = jnp.bfloat16
        f32 = jnp.float32
        n_batch, seq_len, width = x_in.shape
        head_dim = w_k.shape[N1]
        rows = w_q.shape[N0]
        nq = w_q.shape[N1]
        nf = w_gate.shape[N1]
        part = N2 * head_dim // n_tp
        mine = n_batch // n_tp
        tp = lax.axis_index('tp')
        core = lax.rem(lax.axis_index('fsdp'), N2)
        gain_hi = lax.reduce_precision(ln_gain, SUB, 7)
        gain_mid = lax.reduce_precision(ln_gain - gain_hi, SUB, 7)
        gain_lo = ln_gain - gain_hi - gain_mid
        gain_cols = jnp.stack([gain_hi, gain_mid, gain_lo], axis=N1).astype(bf16)
        kv_mine = lax.dynamic_slice_in_dim(jnp.concatenate([w_k, w_v], axis=N1), tp * part, part, N1)
        small = jnp.concatenate([kv_mine, gain_cols, jnp.zeros((rows, LANES - part - N3), bf16)], axis=N1)
        down = w_down.T
        packed = jnp.stack([jnp.concatenate([w_gate, w_q, w_o.T, small, down[:, :LANES]], axis=N1), jnp.concatenate([w_up, down[:, LANES:]], axis=N1)])
        wide = packed.shape[N2]
        tables = rope_tables(seq_len, head_dim)
        full = gather_weights(packed).reshape(N2, n_tp, width, wide)
        small_full = full[N0, :, :, KV_AT:KV_AT + LANES]
        w_kv = jnp.concatenate([small_full[n, :, :part] for n in range(n_tp)], axis=N1)
        gain3 = small_full[N0, :, part:part + N3].astype(f32)
        gain_row = (gain3[:, N0] + gain3[:, N1] + gain3[:, N2]).reshape(N1, width)

        who = jnp.stack([tp, core]).astype(jnp.int32)
        y_tok, gx_tok, g_own, g_oth = layer_step(x_in, dy_out, gain_row, full, w_kv, tables, who, seq_len)
        y_my = y_tok.reshape(mine, seq_len, width)
        below = lax.ppermute(y_my, 'tp', [(n, (n + N1) % n_tp) for n in range(n_tp)])
        above = lax.ppermute(y_my, 'tp', [(n, (n - N1) % n_tp) for n in range(n_tp)])
        split = (N2, n_tp, RING, RING, N3, SUB, wide)
        w_sum, kv_sum, grad_x, y_out = sum_grads(g_own.reshape(split), g_oth.reshape(split), gx_tok.reshape(mine, seq_len, width), (y_my, below, above), n_batch)
        w0 = w_sum[N0].reshape(rows, wide)
        w1 = w_sum[N1].reshape(rows, wide)
        kv_all = jnp.swapaxes(kv_sum.reshape(n_tp, rows, LANES)[:, :, :part], N0, N1).reshape(rows, N2 * head_dim)
        grad_wgate = w0[:, :nf]
        grad_wq = w0[:, nf:nf + nq]
        grad_wo = w0[:, nf + nq:nf + N2 * nq].T
        grad_wdown = jnp.concatenate([w0[:, wide - LANES:], w1[:, nf:]], axis=N1).T
        grad_wup = w1[:, :nf]
        grad_wk = kv_all[:, :head_dim]
        grad_wv = kv_all[:, head_dim:]
        grad_gain = kv_sum[N0].reshape(rows, LANES)[:, part]
        return (y_out, grad_x, grad_gain, grad_wq, grad_wk, grad_wv, grad_wo, grad_wgate, grad_wup, grad_wdown)

    act_spec = P('fsdp', None, None)
    row_spec = P('fsdp', 'tp')
    kv_spec = P('fsdp', None)
    col_spec = P('tp', 'fsdp')
    in_specs = (act_spec, act_spec, P('fsdp'), row_spec, kv_spec, kv_spec, col_spec, row_spec, row_spec, col_spec)
    out_specs = (act_spec, act_spec, P('fsdp'), row_spec, kv_spec, kv_spec, col_spec, row_spec, row_spec, col_spec)
    return jax.shard_map(device_step, mesh=mesh, in_specs=in_specs, out_specs=out_specs, check_vma=False)
```

```python
import numpy as np
import jax
import jax.numpy as jnp
from jax import lax
from jax.sharding import PartitionSpec as P
from jax.experimental import pallas as pl
from jax.experimental.pallas import tpu as pltpu


N0, N1, N2, N3 = range(4)
RING = 4
SUB = 8
LANES = 128
PAIR = 256
KIB = 1024
ALL = Ellipsis
KV_AT = 1152
MESH_ID = pl.DeviceIdType.MESH


def gather_kernel(wg_ref, wq_ref, wo_ref, wu_ref, wd_ref, wk_ref, wv_ref, gain_ref, g_ref, hold, lsem, s1, r1, s2, r2, s3, r3, ds, dr):
    t = lax.axis_index('tp')
    f = lax.axis_index('fsdp')
    c = lax.rem(f, N2)
    at = {'x': t, 'y': lax.rem(lax.div(f, N2), RING), 'z': lax.div(f, SUB)}

    def up(i, d):
        return lax.rem(i + d, RING)

    def dev(where, cc):
        return {'tp': where['x'], 'fsdp': (where['z'] * RING + where['y']) * N2 + cc}

    def peer(axis, d):
        return dev({**at, axis: up(at[axis], d)}, c)

    partner = dev(at, N1 - c)
    barrier = pltpu.get_barrier_semaphore()
    greeted = [partner] + [peer(axis, d) for axis in 'xyz' for d in (N1, N2, N3)]
    for who in greeted:
        pl.semaphore_signal(barrier, inc=N1, device_id=who, device_id_type=MESH_ID)
    f32 = jnp.float32
    bf16 = jnp.bfloat16
    rows = wg_ref.shape[N0]
    lane = lax.broadcasted_iota(jnp.int32, (rows, LANES), N1)
    kv = jnp.concatenate([wk_ref[ALL].astype(f32), wv_ref[ALL].astype(f32)], axis=N1)
    kv = pltpu.roll(kv, lax.rem(LANES - 32 * t, LANES), N1)
    diag = lax.broadcasted_iota(jnp.int32, (rows, rows), N0) == lax.broadcasted_iota(jnp.int32, (rows, rows), N1)
    gain = jnp.sum(jnp.where(diag, jnp.broadcast_to(gain_ref[ALL], (rows, rows)), 0.0), axis=N1, keepdims=True)
    gain_hi = gain.astype(bf16).astype(f32)
    gain_mid = (gain - gain_hi).astype(bf16).astype(f32)
    gain_lo = gain - gain_hi - gain_mid
    small = jnp.where(lane < 32, kv, jnp.where(lane == 32, gain_hi, jnp.where(lane == 33, gain_mid, jnp.where(lane == 34, gain_lo, 0.0))))
    middle = jnp.concatenate([wq_ref[ALL].astype(f32), wo_ref[ALL].astype(f32), small], axis=N1)
    for n in range(N3):
        at_rows = slice(SUB * n, SUB * n + SUB)
        hold[N0, n, :, N0:768] = wg_ref[at_rows, :]
        hold[N0, n, :, 768:1280] = middle[at_rows].astype(bf16)
        hold[N0, n, :, 1280:1408] = wd_ref[at_rows, N0:LANES]
        hold[N1, n, :, N0:768] = wu_ref[at_rows, :]
        hold[N1, n, :, 768:1408] = wd_ref[at_rows, LANES:768]
    pl.semaphore_wait(barrier, len(greeted))
    own = pltpu.make_async_copy(hold, g_ref.at[:, at['x'], at['z'], at['y'], c], lsem.at[N0])
    own.start()

    sent = []

    def push(src, dst, s_sem, r_sem, who):
        copy = pltpu.make_async_remote_copy(src_ref=src, dst_ref=dst, send_sem=s_sem, recv_sem=r_sem, device_id=who, device_id_type=MESH_ID)
        copy.start()
        sent.append(copy)

    def landed(ref, s_sem, r_sem):
        pltpu.make_async_remote_copy(src_ref=ref, dst_ref=ref, send_sem=s_sem, recv_sem=r_sem, device_id=partner, device_id_type=MESH_ID).wait_recv()

    parts = (pl.ds(N0, 768), pl.ds(768, 640))

    def view(k, h, fixed, core, cols=None):
        spot = [fixed.get(axis, slice(None)) for axis in 'xzy']
        block = g_ref.at[h, spot[N0], spot[N1], spot[N2], core, k]
        return block if cols is None else g_ref.at[h, spot[N0], spot[N1], spot[N2], core, k, slice(None), cols]

    orders = ('xyz', 'yzx', 'zxy')
    across = []

    def share(k, h, fixed, cols, n):
        push(view(k, h, fixed, c, cols), view(k, h, fixed, c, cols), ds.at[k, h, n], dr.at[k, h, n], partner)
        across.append((k, h, fixed, cols, n))

    def ring_start(k, h, axis, fixed, ss, rr):
        here = {**fixed, axis: at[axis]}
        for n in range(N2):
            ref = view(k, h, here, c, parts[n])
            push(ref, ref, ss.at[k, h, n], rr.at[k, h, n], peer(axis, N1))
            ref = view(k, h, here, c, parts[N1 - n])
            push(ref, ref, ss.at[k, h, N3 - n], rr.at[k, h, N3 - n], peer(axis, N3))

    def ring_forward(k, h, axis, fixed, ss, rr):
        for p, d, n in ((N0, N3, N0), (N1, N1, N3)):
            ref = view(k, h, {**fixed, axis: up(at[axis], d)}, c, parts[p])
            landed(ref, ss.at[k, h, n], rr.at[k, h, n])
            push(ref, ref, ss.at[k, h, RING + p], rr.at[k, h, RING + p], peer(axis, RING - d))

    def ring_share(k, h, axis, fixed, ss, rr, base):
        for m, (p, d, n) in enumerate(((N0, N3, N0), (N1, N1, N3), (N1, N3, N1), (N0, N1, N2), (N0, N2, RING), (N1, N2, 5))):
            there = {**fixed, axis: up(at[axis], d)}
            if n not in (N0, N3):
                landed(view(k, h, there, c, parts[p]), ss.at[k, h, n], rr.at[k, h, n])
            share(k, h, there, parts[p], base + m)

    streams = [(k, h) for h in range(N2) for k in range(N3)]
    for k, h in streams:
        for d in (N1, N3, N2):
            push(hold.at[h, k], view(k, h, at, c), s1.at[k, h, d - N1], r1.at[k, h, d - N1], peer(orders[k][N0], d))
    own.wait()
    second = {}
    third = {}
    for k, h in streams:
        order = orders[k]
        for d in (N1, N3, N2):
            landed(view(k, h, {**at, order[N0]: up(at[order[N0]], RING - d)}, c), s1.at[k, h, d - N1], r1.at[k, h, d - N1])
        second[k, h] = (k, h, order[N1], {order[N2]: at[order[N2]]}, s2, r2)
        third[k, h] = (k, h, order[N2], {}, s3, r3)
        ring_start(*second[k, h])
        share(k, h, {order[N1]: at[order[N1]], order[N2]: at[order[N2]]}, None, N0)
    for stream in streams:
        ring_forward(*second[stream])
    for stream in streams:
        ring_share(*second[stream], N1)
        ring_start(*third[stream])
    for stream in streams:
        ring_forward(*third[stream])
    for stream in streams:
        ring_share(*third[stream], 7)
    for k, h, fixed, cols, n in across:
        landed(view(k, h, fixed, N1 - c, cols), ds.at[k, h, n], dr.at[k, h, n])
    for copy in sent:
        copy.wait_send()


def gather_weights(w_gate, w_q, w_o, w_up, w_down, w_k, w_v, gain):
    dma = pltpu.SemaphoreType.DMA
    rows = w_gate.shape[N0]
    vmem = pl.BlockSpec(memory_space=pltpu.VMEM)
    return pl.pallas_call(
        gather_kernel,
        name='gather_weights',
        out_shape=jax.ShapeDtypeStruct((N2, RING, RING, RING, N2, N3, SUB, 1408), w_gate.dtype),
        in_specs=[vmem] * SUB,
        out_specs=pl.BlockSpec(memory_space=pl.ANY),
        scratch_shapes=[pltpu.VMEM((N2, N3, SUB, 1408), w_gate.dtype), dma((N1,))] + [dma((N3, N2, N3))] * N2 + [dma((N3, N2, 6))] * RING + [dma((N3, N2, 13))] * N2,
        compiler_params=pltpu.CompilerParams(collective_id=N2, has_side_effects=True, vmem_limit_bytes=60 * KIB * KIB),
    )(w_gate, w_q, w_o.T, w_up, w_down.T, w_k, w_v, gain.reshape(N1, rows))


NT = (((N1,), (N1,)), ((), ()))
NN = (((N1,), (N0,)), ((), ()))
TN = (((N0,), (N0,)), ((), ()))


def dot(left, right, dims=NN):
    return lax.dot_general(left, right, dims, preferred_element_type=jnp.float32)


def by_class(out, cols, vals, core):
    for n in range(32):
        out[lax.rem(n % N2 + core, N2), 24 * (n // N2):24 * (n // N2) + 24, cols] = vals[24 * n:24 * n + 24]


def proj_kernel(who_ref, x_ref, dy_ref, w0_ref, w1_ref, small_ref, gain_ref, wkv_ref, ht_out, dyt_out, q_out, kv_out, do_out, act_out, dg_out, du_out, h_out):
    f32 = jnp.float32
    bf16 = jnp.bfloat16
    tokens, width = h_out.shape
    dy_tok = dy_ref[ALL].reshape(tokens, width)

    @pl.when(pl.program_id(N0) == N0)
    def _():
        lane = lax.broadcasted_iota(jnp.int32, (width, LANES), N1)
        first = small_ref[N0, N0].astype(f32)
        w_kv = jnp.where(lane < 32, first, 0.0)
        for n in range(N1, RING):
            w_kv += pltpu.roll(jnp.where(lane < 32, small_ref[N0, n].astype(f32), 0.0), 32 * n, N1)
        wkv_ref[ALL] = w_kv.astype(bf16)
        parts = first.T
        gain_ref[ALL] = (parts[32:33] + parts[33:34]) + parts[34:35]
        for n in range(tokens // LANES):
            at = slice(n * LANES, n * LANES + LANES)
            seq, row = divmod(n * LANES, x_ref.shape[N1])
            x_f32 = x_ref[seq, row:row + LANES, :].astype(f32)
            x_cent = x_f32 - jnp.mean(x_f32, axis=-N1, keepdims=True)
            x_var = jnp.mean(x_cent * x_cent, axis=-N1, keepdims=True)
            h_norm = (x_cent * lax.rsqrt(x_var + 1e-5) * gain_ref[ALL]).astype(bf16)
            h_out[at, :] = h_norm
            by_class(ht_out, at, h_norm.astype(f32).T.astype(bf16), who_ref[N1])
            by_class(dyt_out, at, dy_ref[seq, row:row + LANES, :].astype(f32).T.astype(bf16), who_ref[N1])
        kv_out[ALL] = dot(h_out[ALL], wkv_ref[ALL]).astype(bf16)

    for n in range(N3):
        cols = slice(n * PAIR, n * PAIR + PAIR)
        gate = dot(h_out[ALL], w0_ref[N0, N0, :, cols]).astype(bf16).astype(f32)
        up = dot(h_out[ALL], w1_ref[N0, N0, :, cols]).astype(bf16).astype(f32)
        if n == N0:
            d_low = dot(dy_tok, w0_ref[N0, N0, :, 1280:1408])
            d_act = jnp.concatenate([d_low, dot(dy_tok, w1_ref[N0, N0, :, 768:896])], axis=N1)
        else:
            d_act = dot(dy_tok, w1_ref[N0, N0, :, 640 + n * PAIR:896 + n * PAIR])
        d_act = d_act.astype(bf16).astype(f32)
        sig = 0.5 * jnp.tanh(0.5 * gate) + 0.5
        silu = gate * sig
        act_out[N0, :, cols] = (silu * up).astype(bf16)
        du_out[N0, :, cols] = (d_act * silu).astype(bf16)
        dg_out[N0, :, cols] = (d_act * up * (sig + silu * (1.0 - sig))).astype(bf16)
    q_out[N0] = dot(h_out[ALL], w0_ref[N0, N0, :, 768:KIB]).astype(bf16)
    do_out[N0] = dot(dy_tok, w0_ref[N0, N0, :, 896:1152]).astype(bf16)


def att_kernel(q_ref, kv_ref, do_ref, cq_ref, sq_ref, ck_ref, sk_ref, cqt_ref, sqt_ref, swap_ref, o_out, dq_out, dkv_out, dk_lo, dk_hi, dv_lo, dv_hi):
    f32 = jnp.float32
    bf16 = jnp.bfloat16
    seq_len = kv_ref.shape[N0]
    lane = lax.broadcasted_iota(jnp.int32, (seq_len, LANES), N1)
    low = lane < 64
    first = lax.rem(lane, 64) < 32
    causal = lax.broadcasted_iota(jnp.int32, (seq_len, seq_len), N0) <= lax.broadcasted_iota(jnp.int32, (seq_len, seq_len), N1)

    def other(vals):
        return jnp.where(first, pltpu.roll(vals, 96, N1), pltpu.roll(vals, 32, N1))

    kv_f32 = kv_ref[ALL].astype(f32)
    kv_rot = kv_f32 * ck_ref[ALL] + other(kv_f32) * sk_ref[ALL]
    zero = jnp.zeros_like(kv_rot)
    k_lo = jnp.where(low, kv_rot, zero)
    v_hi = jnp.where(low, zero, kv_rot)
    k_hi = pltpu.roll(k_lo, 64, N1)
    v_lo = pltpu.roll(v_hi, 64, N1)
    k_cols = jnp.concatenate([k_lo.T, k_hi.T], axis=N1).astype(bf16)
    v_cols = jnp.concatenate([v_lo.T, v_hi.T], axis=N1).astype(bf16)
    k_lo, k_hi, v_lo, v_hi = (vals.astype(bf16) for vals in (k_lo, k_hi, v_lo, v_hi))
    for ref in (dk_lo, dk_hi, dv_lo, dv_hi):
        ref[ALL] = jnp.zeros_like(ref)

    def head(q_tile, k_part, v_part, do_tile):
        scores = jnp.where(causal, dot(k_part, q_tile, NT), -1e30)
        exp_val = jnp.exp(scores - jnp.max(scores, axis=N0, keepdims=True))
        prob = exp_val * (1.0 / jnp.sum(exp_val, axis=N0, keepdims=True))
        d_prob = dot(v_part, do_tile, NT).astype(bf16).astype(f32)
        d_score = prob * (d_prob - jnp.sum(d_prob * prob, axis=N0, keepdims=True))
        return prob.astype(bf16), d_score.astype(bf16)

    def block(tt, carry):
        tiles = []
        for n in range(N2):
            cols = slice(n * LANES, n * LANES + LANES)
            vals = q_ref[tt, :, cols]
            tiles.append(((vals.astype(f32) * cq_ref[ALL] + dot(vals, swap_ref[ALL]) * sq_ref[ALL]) * 0.125).astype(bf16))
        do0 = do_ref[tt, :, N0:LANES]
        do1 = do_ref[tt, :, LANES:PAIR]
        p0, s0 = head(tiles[N0], k_lo, v_hi, do0)
        p1, s1 = head(tiles[N0], k_hi, v_lo, do1)
        p2, s2 = head(tiles[N1], k_lo, v_hi, do1)
        o_out[tt, :, N0:LANES] = dot(v_cols[:, PAIR:512], p0).T.astype(bf16)
        o_out[tt, :, LANES:PAIR] = dot(v_cols, jnp.concatenate([p1, p2], axis=N0)).T.astype(bf16)
        dv_hi[ALL] += dot(jnp.concatenate([p0, p2], axis=N1), jnp.concatenate([do0, do1], axis=N0))
        dv_lo[ALL] += dot(p1, do1)
        dk_lo[ALL] += dot(jnp.concatenate([s0, s2], axis=N1), jnp.concatenate(tiles, axis=N0))
        dk_hi[ALL] += dot(s1, tiles[N0])
        for n, grad in ((N0, dot(k_cols, jnp.concatenate([s0, s1], axis=N0))), (N1, dot(k_cols[:, N0:PAIR], s2))):
            grad = grad.astype(bf16).astype(f32) * 0.125
            swapped = jnp.concatenate([grad[32:64], grad[N0:32], grad[96:LANES], grad[64:96]], axis=N0)
            dq_out[tt, :, n * LANES:n * LANES + LANES] = (grad * cqt_ref[ALL] - swapped * sqt_ref[ALL]).T.astype(bf16)
        return carry
    lax.fori_loop(N0, q_ref.shape[N0], block, N0, unroll=True)
    dk = (dk_lo[ALL] + pltpu.roll(dk_hi[ALL], 64, N1)).astype(bf16).astype(f32)
    dk_raw = dk * ck_ref[ALL] - other(dk) * sk_ref[ALL]
    dv = dv_hi[ALL] + pltpu.roll(dv_lo[ALL], 64, N1)
    dkv_out[ALL] = jnp.where(low, dk_raw, dv).astype(bf16)


def back_kernel(who_ref, x_ref, dy_ref, gain_ref, w0_ref, w1_ref, wkv_ref, o_ref, act_ref, dq_ref, dg_ref, du_ref, dkv_ref, y_out, gx_out, gcol_out, y_acc, dh_acc):
    f32 = jnp.float32
    bf16 = jnp.bfloat16
    step = pl.program_id(N0)
    tokens, width = y_acc.shape
    y_left = jnp.concatenate([o_ref[N0], act_ref[N0]], axis=N1)
    y_right = jnp.concatenate([w0_ref[N0, N0, :, 896:1152], w0_ref[N0, N0, :, 1280:1408], w1_ref[N0, N0, :, 768:1408]], axis=N1)
    h_left = jnp.concatenate([dg_ref[N0], dq_ref[N0], du_ref[N0]], axis=N1)
    h_right = jnp.concatenate([w0_ref[N0, N0, :, N0:KIB], w1_ref[N0, N0, :, N0:768]], axis=N1)
    y_part = dot(y_left, y_right, NT)
    dh_part = dot(h_left, h_right, NT)

    @pl.when(step == N0)
    def _():
        y_acc[ALL] = y_part
        dh_acc[ALL] = dh_part + dot(dkv_ref[ALL], wkv_ref[ALL], NT)

    @pl.when(step > N0)
    def _():
        y_acc[ALL] += y_part
        dh_acc[ALL] += dh_part

    @pl.when(step == pl.num_programs(N0) - N1)
    def _():
        gain = jnp.zeros((N1, width), f32)
        for n in range(tokens // LANES):
            at = slice(n * LANES, n * LANES + LANES)
            seq, row = divmod(n * LANES, x_ref.shape[N1])
            x_f32 = x_ref[seq, row:row + LANES, :].astype(f32)
            y_out[at, :] = (x_f32 + y_acc[at, :]).astype(bf16)
            x_cent = x_f32 - jnp.mean(x_f32, axis=-N1, keepdims=True)
            rstd = lax.rsqrt(jnp.mean(x_cent * x_cent, axis=-N1, keepdims=True) + 1e-5)
            x_hat = x_cent * rstd
            dh = dh_acc[at, :].astype(bf16).astype(f32)
            gain += jnp.sum(dh * x_hat, axis=N0, keepdims=True)
            d_hat = dh * gain_ref[ALL]
            dx = rstd * (d_hat - jnp.mean(d_hat, axis=-N1, keepdims=True) - x_hat * jnp.mean(d_hat * x_hat, axis=-N1, keepdims=True))
            gx_out[at, :] = (dy_ref[seq, row:row + LANES, :].astype(f32) + dx).astype(bf16)
        lane = lax.broadcasted_iota(jnp.int32, (width, LANES), N1)
        by_class(gcol_out, slice(None), jnp.where(lane == 32, jnp.broadcast_to(gain, (LANES, width)).T, 0.0), who_ref[N1])


def wgrad_kernel(ht_ref, dyt_ref, gcol_ref, o_ref, act_ref, dq_ref, dg_ref, du_ref, dkv_ref, own_out, oth_out):
    tt = pl.program_id(N0)
    half = ht_ref.shape[N1]
    lane = lax.broadcasted_iota(jnp.int32, (half, LANES), N1)
    ht = ht_ref[ALL].reshape(N2 * half, ht_ref.shape[N2])
    dyt = dyt_ref[ALL].reshape(N2 * half, dyt_ref.shape[N2])

    def put(n, cols, vals):
        own_out[n, N0, :, cols] = vals[:half]
        oth_out[n, N0, :, cols] = vals[half:].astype(jnp.bfloat16)

    for k in range(N3):
        cols = slice(k * PAIR, k * PAIR + PAIR)
        put(N0, cols, dot(ht, dg_ref[N0, :, cols]))
        put(N1, cols, dot(ht, du_ref[N0, :, cols]))
    g_q = dot(ht, dq_ref[N0])
    g_o = dot(dyt, o_ref[N0])
    put(N0, slice(768, 896), g_q[:, N0:LANES])
    put(N0, slice(896, KIB), g_q[:, LANES:PAIR] + g_o[:, N0:LANES])
    put(N0, slice(KIB, 1152), g_o[:, LANES:PAIR])
    g_kv = dot(ht, dkv_ref[ALL])
    for cls, out in ((N0, own_out), (N1, oth_out)):
        part = pltpu.roll(g_kv[cls * half:cls * half + half], lax.rem(LANES - 32 * tt, LANES), N1)
        out[N0, N0, :, 1152:1280] = (jnp.where(lane < 32, part, 0.0) + gcol_ref[cls]).astype(out.dtype)
    put(N0, slice(1280, 1408), dot(dyt, act_ref[N0, :, N0:LANES]))
    for lo, hi in ((LANES, 384), (384, 640), (640, 768)):
        put(N1, slice(lo + 640, hi + 640), dot(dyt, act_ref[N0, :, lo:hi]))


def layer_step(x_in, dy_in, w_full, tables, who, seq_len):
    f32 = jnp.float32
    bf16 = jnp.bfloat16
    n_tp = w_full.shape[N1]
    wide = w_full.shape[N3]
    width = w_full.shape[N2]
    n_seq = x_in.shape[N0] // n_tp
    tokens = n_seq * seq_len
    half = width // N2

    def whole(shape):
        return pl.BlockSpec(shape, lambda i, *_: (N0,) * len(shape))

    def per(shape):
        return pl.BlockSpec((N1,) + shape, lambda i, *_: (i,) + (N0,) * len(shape))

    w0_spec = pl.BlockSpec((N1, N1, width, wide), lambda i, *_: (N0, i, N0, N0))
    w1_spec = pl.BlockSpec((N1, N1, width, wide), lambda i, *_: (N1, i, N0, N0))
    mine = pl.BlockSpec((n_seq, seq_len, width), lambda i, who_ref: (who_ref[N0], N0, N0))
    tok = whole((tokens, width))
    classes = whole((N2, half, tokens))
    params = pltpu.CompilerParams(dimension_semantics=('arbitrary',), vmem_limit_bytes=56 * KIB * KIB)
    wide_t = jax.ShapeDtypeStruct((n_tp, tokens, width), bf16)
    pair_t = jax.ShapeDtypeStruct((n_tp, tokens, PAIR), bf16)
    row_t = jax.ShapeDtypeStruct((tokens, width), bf16)
    class_t = jax.ShapeDtypeStruct((N2, half, tokens), bf16)
    kv_t = jax.ShapeDtypeStruct((tokens, LANES), bf16)
    work = pl.CostEstimate(flops=13 * 10**9, bytes_accessed=40 * 10**6, transcendentals=N0)
    small = pl.BlockSpec((N1, n_tp, width, LANES), lambda i, *_: (N0, N0, N0, KV_AT // LANES))
    gain_row, w_kv, h_t, dy_t, q_raw, kv_raw, d_o, act, d_gate, d_up = pl.pallas_call(
        proj_kernel, name='proj',
        grid_spec=pltpu.PrefetchScalarGridSpec(
            num_scalar_prefetch=N1, grid=(n_tp,),
            in_specs=[mine, mine, w0_spec, w1_spec, small],
            out_specs=(whole((N1, width)), whole((width, LANES)), classes, classes, per((tokens, PAIR)), whole((tokens, LANES)), per((tokens, PAIR)), per((tokens, width)), per((tokens, width)), per((tokens, width))),
            scratch_shapes=[pltpu.VMEM((tokens, width), bf16)]),
        out_shape=(jax.ShapeDtypeStruct((N1, width), f32), jax.ShapeDtypeStruct((width, LANES), bf16), class_t, class_t, pair_t, kv_t, pair_t, wide_t, wide_t, wide_t),
        compiler_params=params, cost_estimate=work,
    )(who, x_in, dy_in, w_full, w_full, w_full)

    pair_spec = pl.BlockSpec((n_tp, seq_len, PAIR), lambda i: (N0, i, N0))
    kv_spec = pl.BlockSpec((seq_len, LANES), lambda i: (i, N0))
    table = whole((seq_len, LANES))
    att, d_q, d_kv = pl.pallas_call(
        att_kernel, name='attention', grid=(n_seq,),
        in_specs=[pair_spec, kv_spec, pair_spec, table, table, table, table, whole((LANES, seq_len)), whole((LANES, seq_len)), whole((LANES, LANES))],
        out_specs=(pair_spec, pair_spec, kv_spec),
        out_shape=(pair_t, pair_t, kv_t),
        scratch_shapes=[pltpu.VMEM((seq_len, LANES), f32)] * RING,
        compiler_params=params, cost_estimate=work,
    )(q_raw, kv_raw, d_o, *tables)

    gcol_t = jax.ShapeDtypeStruct((N2, half, LANES), f32)
    y_tok, gx_tok, gain_col = pl.pallas_call(
        back_kernel, name='back',
        grid_spec=pltpu.PrefetchScalarGridSpec(
            num_scalar_prefetch=N1, grid=(n_tp,),
            in_specs=[mine, mine, whole((N1, width)), w0_spec, w1_spec, whole((width, LANES)), per((tokens, PAIR)), per((tokens, width)), per((tokens, PAIR)),
                      per((tokens, width)), per((tokens, width)), whole((tokens, LANES))],
            out_specs=(tok, tok, whole((N2, half, LANES))),
            scratch_shapes=[pltpu.VMEM((tokens, width), f32)] * N2),
        out_shape=(row_t, row_t, gcol_t),
        compiler_params=params, cost_estimate=work,
    )(who, x_in, dy_in, gain_row, w_full, w_full, w_kv, att, act, d_q, d_gate, d_up, d_kv)

    class_spec = pl.BlockSpec((N2, N1, half, wide), lambda i: (N0, i, N0, N0))
    own, oth = pl.pallas_call(
        wgrad_kernel, name='wgrad', grid=(n_tp,),
        in_specs=[classes, classes, whole((N2, half, LANES)), per((tokens, PAIR)), per((tokens, width)), per((tokens, PAIR)),
                  per((tokens, width)), per((tokens, width)), whole((tokens, LANES))],
        out_specs=(class_spec, class_spec),
        out_shape=(jax.ShapeDtypeStruct((N2, n_tp, half, wide), f32), jax.ShapeDtypeStruct((N2, n_tp, half, wide), bf16)),
        compiler_params=params, cost_estimate=work,
    )(h_t, dy_t, gain_col, att, act, d_q, d_gate, d_up, d_kv)
    return y_tok, gx_tok, own, oth


def rope_tables(seq_len, head_dim):
    half_dim = head_dim // N2
    inv_freq = np.power(np.float32(10000.0), (-2.0 * np.arange(half_dim) / head_dim).astype(np.float32))
    angle = (np.arange(seq_len, dtype=np.float32)[:, None] * inv_freq[None, :]).astype(np.float32)
    cos_t = np.cos(angle)
    sin_t = np.sin(angle)
    cos_h = np.concatenate([cos_t, cos_t], axis=N1)
    sin_h = np.concatenate([-sin_t, sin_t], axis=N1)
    cos_q = np.concatenate([cos_h, cos_h], axis=N1)
    sin_q = np.concatenate([sin_h, sin_h], axis=N1)
    cos_k = np.concatenate([cos_h, np.ones_like(cos_h)], axis=N1)
    sin_k = np.concatenate([sin_h, np.zeros_like(sin_h)], axis=N1)
    swap = np.eye(LANES)[np.arange(LANES) ^ 32]
    return tuple(jnp.asarray(table, jnp.float32) for table in (cos_q, sin_q, cos_k, sin_k, cos_q.T, sin_q.T)) + (jnp.asarray(swap, jnp.bfloat16),)


def sum_kernel(g_ref, gs_ref, gx_ref, y_ref, below_ref, above_ref, w_out, kv_out, gx_out, y_out, acc, rp, sa, ra1, ra2, sb, rb1, rb2, sc, rc, kvx, gsem, d2s, d2r, ss, rs, cs, cr, ks, kr, xs, xr, lsem, keep):
    f32 = jnp.float32
    bf16 = jnp.bfloat16
    t = lax.axis_index('tp')
    f = lax.axis_index('fsdp')
    c = lax.rem(f, N2)
    yy = lax.rem(lax.div(f, N2), RING)
    zz = lax.div(f, SUB)

    def dev(tt, zc, yc, cc):
        return {'tp': tt, 'fsdp': (zc * RING + yc) * N2 + cc}

    def up(i, d):
        return lax.rem(i + d, RING)

    partner = dev(t, zz, yy, N1 - c)
    xp = [dev(up(t, d), zz, yy, c) for d in range(RING)]
    z_dev = [dev(t, up(zz, d), yy, c) for d in range(RING)]
    y_dev = [dev(t, zz, up(yy, d), c) for d in range(RING)]
    barrier = pltpu.get_barrier_semaphore()
    peers = [partner, xp[N1], xp[N2], xp[N3], z_dev[N1], z_dev[N3], y_dev[N1], y_dev[N3]]
    for peer in peers:
        pl.semaphore_signal(barrier, inc=N1, device_id=peer, device_id_type=MESH_ID)

    def rcopy(src, dst, s_sem, r_sem, peer):
        return pltpu.make_async_remote_copy(src_ref=src, dst_ref=dst, send_sem=s_sem, recv_sem=r_sem, device_id=peer, device_id_type=MESH_ID)

    ring_a = [zz, yy]
    ring_b = [yy, zz]
    dev_a = [z_dev, y_dev]
    dev_b = [y_dev, z_dev]
    order = [N2, N1, N3, N0]

    def g_view(col, j):
        return g_ref.at[N0, :, j] if col == N0 else g_ref.at[N1, :, :, j]

    def gs_view(col, j):
        return gs_ref.at[N0, :, j] if col == N0 else gs_ref.at[N1, :, :, j]

    load = [[None] * RING for _ in range(N2)]
    pair = [[None] * RING for _ in range(N2)]
    for n, d in enumerate(order):
        for col in range(N2):
            j = up(ring_a[col], d)
            load[col][n] = pltpu.make_async_copy(g_view(col, j), acc.at[col, n], gsem.at[col, n])
            load[col][n].start()
    pl.semaphore_wait(barrier, len(peers))
    for n, d in enumerate(order):
        for col in range(N2):
            j = up(ring_a[col], d)
            pair[col][n] = rcopy(gs_view(col, j), rp.at[col, n], d2s.at[col, n], d2r.at[col, n], partner)
            pair[col][n].start()
    mine = gx_ref.shape[N0]
    my_rows = pl.ds(t * mine, mine)
    lower = pl.ds(up(t, N3) * mine, mine)
    upper = pl.ds(up(t, N1) * mine, mine)
    y_up = rcopy(below_ref.at[:, pl.ds(N0, LANES)], y_out.at[lower, pl.ds(N0, LANES)], xs.at[RING], xr.at[RING], xp[N1])
    y_dn = rcopy(above_ref.at[:, pl.ds(LANES, LANES)], y_out.at[upper, pl.ds(LANES, LANES)], xs.at[5], xr.at[5], xp[N3])
    y_up.start()
    y_dn.start()
    x_up = rcopy(gx_ref, gx_out.at[my_rows], xs.at[N0], xr.at[N0], xp[N1])
    x_dn = rcopy(gx_ref, gx_out.at[my_rows], xs.at[N1], xr.at[N1], xp[N3])
    x_up.start()
    x_dn.start()
    local = ((gx_ref, gx_out, my_rows), (y_ref, y_out, my_rows), (below_ref, y_out, lower), (above_ref, y_out, upper))
    taken = [pltpu.make_async_copy(ref, keep.at[n], lsem.at[n]) for n, (ref, _, _) in enumerate(local)]
    placed = [pltpu.make_async_copy(keep.at[n], out.at[place], lsem.at[n]) for n, (_, out, place) in enumerate(local)]
    for copy in taken:
        copy.start()

    def each(count, body):
        def step(n, carry):
            body(n)
            return carry
        lax.fori_loop(N0, count, step, N0)

    def arrived(col, n):
        load[col][n].wait()
        pair[col][n].wait_recv()

    sends = []

    def send(src, dst, s_sem, r_sem, peer):
        copy = rcopy(src, dst, s_sem, r_sem, peer)
        copy.start()
        sends.append(copy)
        return copy

    for col in range(N2):
        arrived(col, N0)

        def first(q, col=col):
            tt = lax.div(q, 12)
            a2 = lax.rem(lax.div(q, N3), RING)
            r = lax.rem(q, N3)
            sa[col, N0, a2, tt, r] = (acc[col, N0, tt, a2, r] + rp[col, N0, tt, a2, r].astype(f32)).astype(bf16)
        each(48, first)
        send(sa.at[col, N0, pl.ds(N0, N2)], ra1.at[col, N0], ss.at[col, N0], rs.at[col, N0], dev_a[col][N1])
        send(sa.at[col, N0, pl.ds(N2, N2)], ra1.at[col, N1], ss.at[col, N1], rs.at[col, N1], dev_a[col][N3])
    for col in range(N2):
        for n, base, peer in ((N1, N2, N1), (N2, N0, N3)):
            arrived(col, n)

            def plain(q, col=col, n=n, base=base):
                a2 = base + lax.div(q, 12)
                tt = lax.rem(lax.div(q, N3), RING)
                r = lax.rem(q, N3)
                sa[col, n, a2, tt, r] = (acc[col, n, tt, a2, r] + rp[col, n, tt, a2, r].astype(f32)).astype(bf16)
            each(24, plain)
            send(sa.at[col, n, pl.ds(base, N2)], ra2.at[col, n - N1, pl.ds(base, N2)], ss.at[col, n + N1], rs.at[col, n + N1], dev_a[col][peer])
    for col in range(N2):
        for n, base, peer in ((N1, N0, N1), (N2, N2, N3)):
            rcopy(sa.at[col, N0, pl.ds(N0, N2)], ra1.at[col, n - N1], ss.at[col, n - N1], rs.at[col, n - N1], dev_a[col][peer]).wait_recv()

            def joined(q, col=col, n=n, base=base):
                h = lax.div(q, 12)
                a2 = base + h
                tt = lax.rem(lax.div(q, N3), RING)
                r = lax.rem(q, N3)
                val = acc[col, n, tt, a2, r] + rp[col, n, tt, a2, r].astype(f32) + ra1[col, n - N1, h, tt, r].astype(f32)
                sa[col, n, a2, tt, r] = val.astype(bf16)
            each(24, joined)
            send(sa.at[col, n, pl.ds(base, N2)], ra2.at[col, n - N1, pl.ds(base, N2)], ss.at[col, n + N3], rs.at[col, n + N3], dev_a[col][peer])
    for n in range(RING):
        taken[n].wait()
        placed[n].start()
    x_up.wait_recv()
    x_dn.wait_recv()
    half_dn = gx_out.at[lower, pl.ds(N0, LANES)]
    half_up = gx_out.at[upper, pl.ds(LANES, LANES)]
    x_up2 = rcopy(half_dn, half_dn, xs.at[N2], xr.at[N2], xp[N1])
    x_dn2 = rcopy(half_up, half_up, xs.at[N3], xr.at[N3], xp[N3])
    x_up2.start()
    x_dn2.start()
    for col in range(N2):
        arrived(col, N3)
        for n, base, s in ((N1, N2, N2), (N2, N0, N3), (N1, N0, RING), (N2, N2, 5)):
            rcopy(sa.at[col, n, pl.ds(base, N2)], ra2.at[col, n - N1, pl.ds(base, N2)], ss.at[col, s], rs.at[col, s], partner).wait_recv()

        def own(q, col=col):
            a2 = lax.div(q, 12)
            tt = lax.rem(lax.div(q, N3), RING)
            r = lax.rem(q, N3)
            val = acc[col, N3, tt, a2, r] + rp[col, N3, tt, a2, r].astype(f32) + ra2[col, N0, a2, tt, r].astype(f32) + ra2[col, N1, a2, tt, r].astype(f32)
            acc[col, N3, tt, a2, r] = val
        each(48, own)
        far = up(ring_b[col], N2)

        def first_b(q, col=col, far=far):
            tt = lax.div(q, N3)
            r = lax.rem(q, N3)
            sb[col, N0, tt, r] = acc[col, N3, tt, far, r].astype(bf16)
        each(12, first_b)
        send(sb.at[col, N0, pl.ds(N0, N2)], rb1.at[col, N0], ss.at[col, 6], rs.at[col, 6], dev_b[col][N1])
        send(sb.at[col, N0, pl.ds(N2, N2)], rb1.at[col, N1], ss.at[col, 7], rs.at[col, 7], dev_b[col][N3])
        for n, base, peer in ((N1, N2, N1), (N2, N0, N3)):
            pos = up(ring_b[col], peer)

            def plain_b(q, col=col, n=n, base=base, pos=pos):
                tt = base + lax.div(q, N3)
                r = lax.rem(q, N3)
                sb[col, n, tt, r] = acc[col, N3, tt, pos, r].astype(bf16)
            each(6, plain_b)
            send(sb.at[col, n, pl.ds(base, N2)], rb2.at[col, n - N1, pl.ds(base, N2)], ss.at[col, n + 7], rs.at[col, n + 7], dev_b[col][peer])
    for col in range(N2):
        for n, base, peer in ((N1, N0, N1), (N2, N2, N3)):
            rcopy(sb.at[col, N0, pl.ds(N0, N2)], rb1.at[col, n - N1], ss.at[col, n + 5], rs.at[col, n + 5], partner).wait_recv()
            pos = up(ring_b[col], peer)

            def joined_b(q, col=col, n=n, base=base, pos=pos):
                h = lax.div(q, N3)
                tt = base + h
                r = lax.rem(q, N3)
                sb[col, n, tt, r] = (acc[col, N3, tt, pos, r] + rb1[col, n - N1, h, r].astype(f32)).astype(bf16)
            each(6, joined_b)
            send(sb.at[col, n, pl.ds(base, N2)], rb2.at[col, n - N1, pl.ds(base, N2)], ss.at[col, n + 9], rs.at[col, n + 9], dev_b[col][peer])
    for col in range(N2):
        here = ring_b[col]
        for n, base, s in ((N1, N2, SUB), (N2, N0, 9), (N1, N0, 10), (N2, N2, 11)):
            rcopy(sb.at[col, n, pl.ds(base, N2)], rb2.at[col, n - N1, pl.ds(base, N2)], ss.at[col, s], rs.at[col, s], partner).wait_recv()

        def own_b(q, col=col, here=here):
            tt = lax.div(q, N3)
            r = lax.rem(q, N3)
            val = acc[col, N3, tt, here, r] + rb2[col, N0, tt, r].astype(f32) + rb2[col, N1, tt, r].astype(f32)
            acc[col, N3, tt, here, r] = val
            sc[col, tt, r] = val.astype(bf16)
        each(12, own_b)
        for d in (N1, N3, N2):
            to = up(t, d)
            send(sc.at[col, to], rc.at[col, d - N1], cs.at[col, d - N1], cr.at[col, d - N1], xp[d])
        if col == N0:
            def kv_part(q, here=here):
                tt = lax.div(q, N3)
                r = lax.rem(q, N3)
                kvx[t, tt, r] = acc[N0, N3, tt, here, r, :, pl.ds(KV_AT, LANES)]
            each(12, kv_part)
            for d in (N1, N3, N2):
                send(kvx.at[t], kvx.at[t], ks.at[d - N1], kr.at[d - N1], xp[d])
    for col in range(N2):
        here = ring_b[col]
        for d in (N1, N3, N2):
            rcopy(sc.at[col, N0], rc.at[col, d - N1], cs.at[col, d - N1], cr.at[col, d - N1], partner).wait_recv()

        def last(r, col=col, here=here):
            w_out[col, r] = acc[col, N3, t, here, r] + rc[col, N0, r].astype(f32) + rc[col, N1, r].astype(f32) + rc[col, N2, r].astype(f32)
        each(N3, last)
    for d in (N1, N3, N2):
        src = up(t, RING - d)
        rcopy(kvx.at[src], kvx.at[src], ks.at[d - N1], kr.at[d - N1], partner).wait_recv()

    def kv_last(q):
        tt = lax.div(q, N3)
        r = lax.rem(q, N3)
        kv_out[tt, r] = ((kvx[N0, tt, r] + kvx[N1, tt, r]) + kvx[N2, tt, r]) + kvx[N3, tt, r]
    each(12, kv_last)
    for copy in sends:
        copy.wait_send()
    for col in range(N2):
        for n in range(RING):
            pair[col][n].wait_send()
    x_up.wait_send()
    x_dn.wait_send()
    x_up2.wait()
    x_dn2.wait()
    y_up.wait()
    y_dn.wait()
    for copy in placed:
        copy.wait()


def sum_grads(g_pack, g_send, gx_my, y_blocks, n_batch):
    f32 = jnp.float32
    bf16 = jnp.bfloat16
    wide = g_pack.shape[-N1]
    dma = pltpu.SemaphoreType.DMA
    vmem = pl.BlockSpec(memory_space=pltpu.VMEM)
    any_spec = pl.BlockSpec(memory_space=pl.ANY)
    return pl.pallas_call(
        sum_kernel,
        name='sum_grads',
        out_shape=(jax.ShapeDtypeStruct((N2, N3, SUB, wide), f32), jax.ShapeDtypeStruct((RING, N3, SUB, LANES), f32),
                   jax.ShapeDtypeStruct((n_batch,) + gx_my.shape[N1:], bf16), jax.ShapeDtypeStruct((n_batch,) + gx_my.shape[N1:], bf16)),
        in_specs=[any_spec] * 6,
        out_specs=(vmem, vmem, any_spec, any_spec),
        scratch_shapes=[
            pltpu.VMEM((N2, RING, RING, RING, N3, SUB, wide), f32), pltpu.VMEM((N2, RING, RING, RING, N3, SUB, wide), bf16),
            pltpu.VMEM((N2, N3, RING, RING, N3, SUB, wide), bf16), pltpu.VMEM((N2, N2, N2, RING, N3, SUB, wide), bf16), pltpu.VMEM((N2, N2, RING, RING, N3, SUB, wide), bf16),
            pltpu.VMEM((N2, N3, RING, N3, SUB, wide), bf16), pltpu.VMEM((N2, N2, N2, N3, SUB, wide), bf16), pltpu.VMEM((N2, N2, RING, N3, SUB, wide), bf16),
            pltpu.VMEM((N2, RING, N3, SUB, wide), bf16), pltpu.VMEM((N2, N3, N3, SUB, wide), bf16), pltpu.VMEM((RING, RING, N3, SUB, LANES), f32),
            dma((N2, RING)), dma((N2, RING)), dma((N2, RING)), dma((N2, 12)), dma((N2, 12)), dma((N2, N3)), dma((N2, N3)), dma((N3,)), dma((N3,)), dma((6,)), dma((6,)), dma((RING,)), pltpu.VMEM((RING,) + gx_my.shape, bf16),
        ],
        cost_estimate=pl.CostEstimate(flops=60 * 10**9, bytes_accessed=30 * 10**6, transcendentals=N0),
        compiler_params=pltpu.CompilerParams(collective_id=N1, has_side_effects=True, vmem_limit_bytes=60 * KIB * KIB),
    )(g_pack, g_send, gx_my, *y_blocks)


def solution(mesh):
    n_tp = mesh.shape['tp']

    def device_step(x_in, dy_out, ln_gain, w_q, w_k, w_v, w_o, w_gate, w_up, w_down):
        n_batch, seq_len, width = x_in.shape
        head_dim = w_k.shape[N1]
        rows = w_q.shape[N0]
        nq = w_q.shape[N1]
        nf = w_gate.shape[N1]
        part = N2 * head_dim // n_tp
        mine = n_batch // n_tp
        tp = lax.axis_index('tp')
        core = lax.rem(lax.axis_index('fsdp'), N2)
        full = gather_weights(w_gate, w_q, w_o, w_up, w_down, w_k, w_v, ln_gain).reshape(N2, n_tp, width, -N1)
        wide = full.shape[N3]
        tables = rope_tables(seq_len, head_dim)
        who = jnp.stack([tp, core]).astype(jnp.int32)
        y_tok, gx_tok, g_own, g_oth = layer_step(x_in, dy_out, full, tables, who, seq_len)
        y_my = y_tok.reshape(mine, seq_len, width)
        below = lax.ppermute(y_my, 'tp', [(n, (n + N1) % n_tp) for n in range(n_tp)])
        above = lax.ppermute(y_my, 'tp', [(n, (n - N1) % n_tp) for n in range(n_tp)])
        split = (N2, n_tp, RING, RING, N3, SUB, wide)
        w_sum, kv_sum, grad_x, y_out = sum_grads(g_own.reshape(split), g_oth.reshape(split), gx_tok.reshape(mine, seq_len, width), (y_my, below, above), n_batch)
        w0 = w_sum[N0].reshape(rows, wide)
        w1 = w_sum[N1].reshape(rows, wide)
        kv_all = jnp.swapaxes(kv_sum.reshape(n_tp, rows, LANES)[:, :, :part], N0, N1).reshape(rows, N2 * head_dim)
        grad_wgate = w0[:, :nf]
        grad_wq = w0[:, nf:nf + nq]
        grad_wo = w0[:, nf + nq:nf + N2 * nq].T
        grad_wdown = jnp.concatenate([w0[:, wide - LANES:], w1[:, nf:]], axis=N1).T
        grad_wup = w1[:, :nf]
        grad_wk = kv_all[:, :head_dim]
        grad_wv = kv_all[:, head_dim:]
        grad_gain = kv_sum[N0].reshape(rows, LANES)[:, part]
        return (y_out, grad_x, grad_gain, grad_wq, grad_wk, grad_wv, grad_wo, grad_wgate, grad_wup, grad_wdown)

    act_spec = P('fsdp', None, None)
    row_spec = P('fsdp', 'tp')
    kv_spec = P('fsdp', None)
    col_spec = P('tp', 'fsdp')
    in_specs = (act_spec, act_spec, P('fsdp'), row_spec, kv_spec, kv_spec, col_spec, row_spec, row_spec, col_spec)
    out_specs = (act_spec, act_spec, P('fsdp'), row_spec, kv_spec, kv_spec, col_spec, row_spec, row_spec, col_spec)
    return jax.shard_map(device_step, mesh=mesh, in_specs=in_specs, out_specs=out_specs, check_vma=False)
```

```python
import numpy as np
import jax
import jax.numpy as jnp
from jax import lax
from jax.sharding import PartitionSpec as P
from jax.experimental import pallas as pl
from jax.experimental.pallas import tpu as pltpu


N0, N1, N2, N3 = range(4)
RING = 4
SUB = 8
LANES = 128
PAIR = 256
KIB = 1024
ALL = Ellipsis
KV_AT = 1152
MESH_ID = pl.DeviceIdType.MESH


def gather_kernel(wg_ref, wq_ref, wo_ref, wu_ref, wd_ref, wk_ref, wv_ref, gain_ref, g_ref, hold, lsem, s1, r1, s2, r2, s3, r3, ds, dr):
    t = lax.axis_index('tp')
    f = lax.axis_index('fsdp')
    c = lax.rem(f, N2)
    at = {'x': t, 'y': lax.rem(lax.div(f, N2), RING), 'z': lax.div(f, SUB)}

    def up(i, d):
        return lax.rem(i + d, RING)

    def dev(where, cc):
        return {'tp': where['x'], 'fsdp': (where['z'] * RING + where['y']) * N2 + cc}

    def peer(axis, d):
        return dev({**at, axis: up(at[axis], d)}, c)

    partner = dev(at, N1 - c)
    barrier = pltpu.get_barrier_semaphore()
    greeted = [partner] + [peer(axis, d) for axis in 'xyz' for d in (N1, N2, N3)]
    for who in greeted:
        pl.semaphore_signal(barrier, inc=N1, device_id=who, device_id_type=MESH_ID)
    f32 = jnp.float32
    bf16 = jnp.bfloat16
    rows = wg_ref.shape[N0]
    lane = lax.broadcasted_iota(jnp.int32, (rows, LANES), N1)
    kv = jnp.concatenate([wk_ref[ALL].astype(f32), wv_ref[ALL].astype(f32)], axis=N1)
    kv = pltpu.roll(kv, lax.rem(LANES - 32 * t, LANES), N1)
    diag = lax.broadcasted_iota(jnp.int32, (rows, rows), N0) == lax.broadcasted_iota(jnp.int32, (rows, rows), N1)
    gain = jnp.sum(jnp.where(diag, jnp.broadcast_to(gain_ref[ALL], (rows, rows)), 0.0), axis=N1, keepdims=True)
    gain_hi = gain.astype(bf16).astype(f32)
    gain_mid = (gain - gain_hi).astype(bf16).astype(f32)
    gain_lo = gain - gain_hi - gain_mid
    small = jnp.where(lane < 32, kv, jnp.where(lane == 32, gain_hi, jnp.where(lane == 33, gain_mid, jnp.where(lane == 34, gain_lo, 0.0))))
    middle = jnp.concatenate([wq_ref[ALL].astype(f32), wo_ref[ALL].astype(f32), small], axis=N1)
    for n in range(N3):
        at_rows = slice(SUB * n, SUB * n + SUB)
        hold[N0, n, :, N0:768] = wg_ref[at_rows, :]
        hold[N0, n, :, 768:1280] = middle[at_rows].astype(bf16)
        hold[N0, n, :, 1280:1408] = wd_ref[at_rows, N0:LANES]
        hold[N1, n, :, N0:768] = wu_ref[at_rows, :]
        hold[N1, n, :, 768:1408] = wd_ref[at_rows, LANES:768]
    pl.semaphore_wait(barrier, len(greeted))
    own = pltpu.make_async_copy(hold, g_ref.at[:, at['x'], at['z'], at['y'], c], lsem.at[N0])
    own.start()

    sent = []

    def push(src, dst, s_sem, r_sem, who):
        copy = pltpu.make_async_remote_copy(src_ref=src, dst_ref=dst, send_sem=s_sem, recv_sem=r_sem, device_id=who, device_id_type=MESH_ID)
        copy.start()
        sent.append(copy)

    def landed(ref, s_sem, r_sem):
        pltpu.make_async_remote_copy(src_ref=ref, dst_ref=ref, send_sem=s_sem, recv_sem=r_sem, device_id=partner, device_id_type=MESH_ID).wait_recv()

    parts = (pl.ds(N0, 768), pl.ds(768, 640))

    def view(k, h, fixed, core, cols=None):
        spot = [fixed.get(axis, slice(None)) for axis in 'xzy']
        block = g_ref.at[h, spot[N0], spot[N1], spot[N2], core, k]
        return block if cols is None else g_ref.at[h, spot[N0], spot[N1], spot[N2], core, k, slice(None), cols]

    orders = ('xyz', 'yzx', 'zxy')
    across = []

    def share(k, h, fixed, cols, n):
        push(view(k, h, fixed, c, cols), view(k, h, fixed, c, cols), ds.at[k, h, n], dr.at[k, h, n], partner)
        across.append((k, h, fixed, cols, n))

    def ring_start(k, h, axis, fixed, ss, rr):
        here = {**fixed, axis: at[axis]}
        for n in range(N2):
            ref = view(k, h, here, c, parts[n])
            push(ref, ref, ss.at[k, h, n], rr.at[k, h, n], peer(axis, N1))
            ref = view(k, h, here, c, parts[N1 - n])
            push(ref, ref, ss.at[k, h, N3 - n], rr.at[k, h, N3 - n], peer(axis, N3))

    def ring_forward(k, h, axis, fixed, ss, rr):
        for p, d, n in ((N0, N3, N0), (N1, N1, N3)):
            ref = view(k, h, {**fixed, axis: up(at[axis], d)}, c, parts[p])
            landed(ref, ss.at[k, h, n], rr.at[k, h, n])
            push(ref, ref, ss.at[k, h, RING + p], rr.at[k, h, RING + p], peer(axis, RING - d))

    def ring_share(k, h, axis, fixed, ss, rr, base):
        for m, (p, d, n) in enumerate(((N0, N3, N0), (N1, N1, N3), (N1, N3, N1), (N0, N1, N2), (N0, N2, RING), (N1, N2, 5))):
            there = {**fixed, axis: up(at[axis], d)}
            if n not in (N0, N3):
                landed(view(k, h, there, c, parts[p]), ss.at[k, h, n], rr.at[k, h, n])
            share(k, h, there, parts[p], base + m)

    streams = [(k, h) for h in range(N2) for k in range(N3)]
    for k, h in streams:
        for d in (N1, N3, N2):
            push(hold.at[h, k], view(k, h, at, c), s1.at[k, h, d - N1], r1.at[k, h, d - N1], peer(orders[k][N0], d))
    own.wait()
    second = {}
    third = {}
    for k, h in streams:
        order = orders[k]
        for d in (N1, N3, N2):
            landed(view(k, h, {**at, order[N0]: up(at[order[N0]], RING - d)}, c), s1.at[k, h, d - N1], r1.at[k, h, d - N1])
        second[k, h] = (k, h, order[N1], {order[N2]: at[order[N2]]}, s2, r2)
        third[k, h] = (k, h, order[N2], {}, s3, r3)
        ring_start(*second[k, h])
        share(k, h, {order[N1]: at[order[N1]], order[N2]: at[order[N2]]}, None, N0)
    for stream in streams:
        ring_forward(*second[stream])
    for stream in streams:
        ring_share(*second[stream], N1)
        ring_start(*third[stream])
    for stream in streams:
        ring_forward(*third[stream])
    for stream in streams:
        ring_share(*third[stream], 7)
    for k, h, fixed, cols, n in across:
        landed(view(k, h, fixed, N1 - c, cols), ds.at[k, h, n], dr.at[k, h, n])
    for copy in sent:
        copy.wait_send()


def gather_weights(w_gate, w_q, w_o, w_up, w_down, w_k, w_v, gain):
    dma = pltpu.SemaphoreType.DMA
    rows = w_gate.shape[N0]
    vmem = pl.BlockSpec(memory_space=pltpu.VMEM)
    return pl.pallas_call(
        gather_kernel,
        name='gather_weights',
        out_shape=jax.ShapeDtypeStruct((N2, RING, RING, RING, N2, N3, SUB, 1408), w_gate.dtype),
        in_specs=[vmem] * SUB,
        out_specs=pl.BlockSpec(memory_space=pl.ANY),
        scratch_shapes=[pltpu.VMEM((N2, N3, SUB, 1408), w_gate.dtype), dma((N1,))] + [dma((N3, N2, N3))] * N2 + [dma((N3, N2, 6))] * RING + [dma((N3, N2, 13))] * N2,
        compiler_params=pltpu.CompilerParams(collective_id=N2, has_side_effects=True, vmem_limit_bytes=60 * KIB * KIB),
    )(w_gate, w_q, w_o.T, w_up, w_down.T, w_k, w_v, gain.reshape(N1, rows))


NT = (((N1,), (N1,)), ((), ()))
NN = (((N1,), (N0,)), ((), ()))
TN = (((N0,), (N0,)), ((), ()))


def dot(left, right, dims=NN):
    return lax.dot_general(left, right, dims, preferred_element_type=jnp.float32)


def by_class(out, cols, vals, core):
    for n in range(32):
        out[lax.rem(n % N2 + core, N2), 24 * (n // N2):24 * (n // N2) + 24, cols] = vals[24 * n:24 * n + 24]


def proj_kernel(who_ref, x_ref, dy_ref, w0_ref, w1_ref, small_ref, gain_ref, wkv_ref, ht_out, dyt_out, q_out, kv_out, do_out, act_out, dg_out, du_out, h_out):
    f32 = jnp.float32
    bf16 = jnp.bfloat16
    tokens, width = h_out.shape
    dy_tok = dy_ref[ALL].reshape(tokens, width)

    @pl.when(pl.program_id(N0) == N0)
    def _():
        lane = lax.broadcasted_iota(jnp.int32, (width, LANES), N1)
        first = small_ref[N0, N0].astype(f32)
        w_kv = jnp.where(lane < 32, first, 0.0)
        for n in range(N1, RING):
            w_kv += pltpu.roll(jnp.where(lane < 32, small_ref[N0, n].astype(f32), 0.0), 32 * n, N1)
        wkv_ref[ALL] = w_kv.astype(bf16)
        parts = first.T
        gain_ref[ALL] = (parts[32:33] + parts[33:34]) + parts[34:35]
        for n in range(tokens // LANES):
            at = slice(n * LANES, n * LANES + LANES)
            seq, row = divmod(n * LANES, x_ref.shape[N1])
            x_f32 = x_ref[seq, row:row + LANES, :].astype(f32)
            x_cent = x_f32 - jnp.mean(x_f32, axis=-N1, keepdims=True)
            x_var = jnp.mean(x_cent * x_cent, axis=-N1, keepdims=True)
            h_norm = (x_cent * lax.rsqrt(x_var + 1e-5) * gain_ref[ALL]).astype(bf16)
            h_out[at, :] = h_norm
            by_class(ht_out, at, h_norm.astype(f32).T.astype(bf16), who_ref[N1])
            by_class(dyt_out, at, dy_ref[seq, row:row + LANES, :].astype(f32).T.astype(bf16), who_ref[N1])
        kv_out[ALL] = dot(h_out[ALL], wkv_ref[ALL]).astype(bf16)

    for n in range(N3):
        cols = slice(n * PAIR, n * PAIR + PAIR)
        gate = dot(h_out[ALL], w0_ref[N0, N0, :, cols]).astype(bf16).astype(f32)
        up = dot(h_out[ALL], w1_ref[N0, N0, :, cols]).astype(bf16).astype(f32)
        if n == N0:
            d_low = dot(dy_tok, w0_ref[N0, N0, :, 1280:1408])
            d_act = jnp.concatenate([d_low, dot(dy_tok, w1_ref[N0, N0, :, 768:896])], axis=N1)
        else:
            d_act = dot(dy_tok, w1_ref[N0, N0, :, 640 + n * PAIR:896 + n * PAIR])
        d_act = d_act.astype(bf16).astype(f32)
        sig = 0.5 * jnp.tanh(0.5 * gate) + 0.5
        silu = gate * sig
        act_out[N0, :, cols] = (silu * up).astype(bf16)
        du_out[N0, :, cols] = (d_act * silu).astype(bf16)
        dg_out[N0, :, cols] = (d_act * up * (sig + silu * (1.0 - sig))).astype(bf16)
    q_out[N0] = dot(h_out[ALL], w0_ref[N0, N0, :, 768:KIB]).astype(bf16)
    do_out[N0] = dot(dy_tok, w0_ref[N0, N0, :, 896:1152]).astype(bf16)


def att_kernel(q_ref, kv_ref, do_ref, cq_ref, sq_ref, ck_ref, sk_ref, cqt_ref, sqt_ref, swap_ref, o_out, dq_out, dkv_out, dk_lo, dk_hi, dv_lo, dv_hi):
    f32 = jnp.float32
    bf16 = jnp.bfloat16
    seq_len = kv_ref.shape[N0]
    lane = lax.broadcasted_iota(jnp.int32, (seq_len, LANES), N1)
    low = lane < 64
    first = lax.rem(lane, 64) < 32
    causal = lax.broadcasted_iota(jnp.int32, (seq_len, seq_len), N0) <= lax.broadcasted_iota(jnp.int32, (seq_len, seq_len), N1)

    def other(vals):
        return jnp.where(first, pltpu.roll(vals, 96, N1), pltpu.roll(vals, 32, N1))

    kv_f32 = kv_ref[ALL].astype(f32)
    kv_rot = kv_f32 * ck_ref[ALL] + other(kv_f32) * sk_ref[ALL]
    zero = jnp.zeros_like(kv_rot)
    k_lo = jnp.where(low, kv_rot, zero)
    v_hi = jnp.where(low, zero, kv_rot)
    k_hi = pltpu.roll(k_lo, 64, N1)
    v_lo = pltpu.roll(v_hi, 64, N1)
    k_cols = jnp.concatenate([k_lo.T, k_hi.T], axis=N1).astype(bf16)
    v_cols = jnp.concatenate([v_lo.T, v_hi.T], axis=N1).astype(bf16)
    k_lo, k_hi, v_lo, v_hi = (vals.astype(bf16) for vals in (k_lo, k_hi, v_lo, v_hi))
    for ref in (dk_lo, dk_hi, dv_lo, dv_hi):
        ref[ALL] = jnp.zeros_like(ref)

    def head(q_tile, k_part, v_part, do_tile):
        scores = jnp.where(causal, dot(k_part, q_tile, NT), -1e30)
        exp_val = jnp.exp(scores - jnp.max(scores, axis=N0, keepdims=True))
        prob = exp_val * (1.0 / jnp.sum(exp_val, axis=N0, keepdims=True))
        d_prob = dot(v_part, do_tile, NT).astype(bf16).astype(f32)
        d_score = prob * (d_prob - jnp.sum(d_prob * prob, axis=N0, keepdims=True))
        return prob.astype(bf16), d_score.astype(bf16)

    def block(tt, carry):
        tiles = []
        for n in range(N2):
            cols = slice(n * LANES, n * LANES + LANES)
            vals = q_ref[tt, :, cols]
            tiles.append(((vals.astype(f32) * cq_ref[ALL] + dot(vals, swap_ref[ALL]) * sq_ref[ALL]) * 0.125).astype(bf16))
        do0 = do_ref[tt, :, N0:LANES]
        do1 = do_ref[tt, :, LANES:PAIR]
        p0, s0 = head(tiles[N0], k_lo, v_hi, do0)
        p1, s1 = head(tiles[N0], k_hi, v_lo, do1)
        p2, s2 = head(tiles[N1], k_lo, v_hi, do1)
        o_out[tt, :, N0:LANES] = dot(v_cols[:, PAIR:512], p0).T.astype(bf16)
        o_out[tt, :, LANES:PAIR] = dot(v_cols, jnp.concatenate([p1, p2], axis=N0)).T.astype(bf16)
        dv_hi[ALL] += dot(jnp.concatenate([p0, p2], axis=N1), jnp.concatenate([do0, do1], axis=N0))
        dv_lo[ALL] += dot(p1, do1)
        dk_lo[ALL] += dot(jnp.concatenate([s0, s2], axis=N1), jnp.concatenate(tiles, axis=N0))
        dk_hi[ALL] += dot(s1, tiles[N0])
        for n, grad in ((N0, dot(k_cols, jnp.concatenate([s0, s1], axis=N0))), (N1, dot(k_cols[:, N0:PAIR], s2))):
            grad = grad.astype(bf16).astype(f32) * 0.125
            swapped = jnp.concatenate([grad[32:64], grad[N0:32], grad[96:LANES], grad[64:96]], axis=N0)
            dq_out[tt, :, n * LANES:n * LANES + LANES] = (grad * cqt_ref[ALL] - swapped * sqt_ref[ALL]).T.astype(bf16)
        return carry
    lax.fori_loop(N0, q_ref.shape[N0], block, N0, unroll=True)
    dk = (dk_lo[ALL] + pltpu.roll(dk_hi[ALL], 64, N1)).astype(bf16).astype(f32)
    dk_raw = dk * ck_ref[ALL] - other(dk) * sk_ref[ALL]
    dv = dv_hi[ALL] + pltpu.roll(dv_lo[ALL], 64, N1)
    dkv_out[ALL] = jnp.where(low, dk_raw, dv).astype(bf16)


def back_kernel(who_ref, x_ref, dy_ref, gain_ref, w0_ref, w1_ref, wkv_ref, o_ref, act_ref, dq_ref, dg_ref, du_ref, dkv_ref, y_out, gx_out, gcol_out, y_acc, dh_acc):
    f32 = jnp.float32
    bf16 = jnp.bfloat16
    step = pl.program_id(N0)
    tokens, width = y_acc.shape
    y_left = jnp.concatenate([o_ref[N0], act_ref[N0]], axis=N1)
    y_right = jnp.concatenate([w0_ref[N0, N0, :, 896:1152], w0_ref[N0, N0, :, 1280:1408], w1_ref[N0, N0, :, 768:1408]], axis=N1)
    h_left = jnp.concatenate([dg_ref[N0], dq_ref[N0], du_ref[N0]], axis=N1)
    h_right = jnp.concatenate([w0_ref[N0, N0, :, N0:KIB], w1_ref[N0, N0, :, N0:768]], axis=N1)
    y_part = dot(y_left, y_right, NT)
    dh_part = dot(h_left, h_right, NT)

    @pl.when(step == N0)
    def _():
        y_acc[ALL] = y_part
        dh_acc[ALL] = dh_part + dot(dkv_ref[ALL], wkv_ref[ALL], NT)

    @pl.when(step > N0)
    def _():
        y_acc[ALL] += y_part
        dh_acc[ALL] += dh_part

    @pl.when(step == pl.num_programs(N0) - N1)
    def _():
        gain = jnp.zeros((N1, width), f32)
        for n in range(tokens // LANES):
            at = slice(n * LANES, n * LANES + LANES)
            seq, row = divmod(n * LANES, x_ref.shape[N1])
            x_f32 = x_ref[seq, row:row + LANES, :].astype(f32)
            y_out[at, :] = (x_f32 + y_acc[at, :]).astype(bf16)
            x_cent = x_f32 - jnp.mean(x_f32, axis=-N1, keepdims=True)
            rstd = lax.rsqrt(jnp.mean(x_cent * x_cent, axis=-N1, keepdims=True) + 1e-5)
            x_hat = x_cent * rstd
            dh = dh_acc[at, :].astype(bf16).astype(f32)
            gain += jnp.sum(dh * x_hat, axis=N0, keepdims=True)
            d_hat = dh * gain_ref[ALL]
            dx = rstd * (d_hat - jnp.mean(d_hat, axis=-N1, keepdims=True) - x_hat * jnp.mean(d_hat * x_hat, axis=-N1, keepdims=True))
            gx_out[at, :] = (dy_ref[seq, row:row + LANES, :].astype(f32) + dx).astype(bf16)
        lane = lax.broadcasted_iota(jnp.int32, (width, LANES), N1)
        by_class(gcol_out, slice(None), jnp.where(lane == 32, jnp.broadcast_to(gain, (LANES, width)).T, 0.0), who_ref[N1])


def wgrad_kernel(ht_ref, dyt_ref, gcol_ref, o_ref, act_ref, dq_ref, dg_ref, du_ref, dkv_ref, own_out, oth_out):
    tt = pl.program_id(N0)
    half = ht_ref.shape[N1]
    lane = lax.broadcasted_iota(jnp.int32, (half, LANES), N1)
    ht = ht_ref[ALL].reshape(N2 * half, ht_ref.shape[N2])
    dyt = dyt_ref[ALL].reshape(N2 * half, dyt_ref.shape[N2])

    def put(n, cols, vals):
        own_out[n, N0, :, cols] = vals[:half]
        oth_out[n, N0, :, cols] = vals[half:].astype(jnp.bfloat16)

    for k in range(N3):
        cols = slice(k * PAIR, k * PAIR + PAIR)
        put(N0, cols, dot(ht, dg_ref[N0, :, cols]))
        put(N1, cols, dot(ht, du_ref[N0, :, cols]))
    g_q = dot(ht, dq_ref[N0])
    g_o = dot(dyt, o_ref[N0])
    put(N0, slice(768, 896), g_q[:, N0:LANES])
    put(N0, slice(896, KIB), g_q[:, LANES:PAIR] + g_o[:, N0:LANES])
    put(N0, slice(KIB, 1152), g_o[:, LANES:PAIR])
    g_kv = dot(ht, dkv_ref[ALL])
    for cls, out in ((N0, own_out), (N1, oth_out)):
        part = pltpu.roll(g_kv[cls * half:cls * half + half], lax.rem(LANES - 32 * tt, LANES), N1)
        out[N0, N0, :, 1152:1280] = (jnp.where(lane < 32, part, 0.0) + gcol_ref[cls]).astype(out.dtype)
    put(N0, slice(1280, 1408), dot(dyt, act_ref[N0, :, N0:LANES]))
    for lo, hi in ((LANES, 384), (384, 640), (640, 768)):
        put(N1, slice(lo + 640, hi + 640), dot(dyt, act_ref[N0, :, lo:hi]))


def layer_step(x_in, dy_in, w_full, tables, who, seq_len):
    f32 = jnp.float32
    bf16 = jnp.bfloat16
    n_tp = w_full.shape[N1]
    wide = w_full.shape[N3]
    width = w_full.shape[N2]
    n_seq = x_in.shape[N0] // n_tp
    tokens = n_seq * seq_len
    half = width // N2

    def whole(shape):
        return pl.BlockSpec(shape, lambda i, *_: (N0,) * len(shape))

    def per(shape):
        return pl.BlockSpec((N1,) + shape, lambda i, *_: (i,) + (N0,) * len(shape))

    w0_spec = pl.BlockSpec((N1, N1, width, wide), lambda i, *_: (N0, i, N0, N0))
    w1_spec = pl.BlockSpec((N1, N1, width, wide), lambda i, *_: (N1, i, N0, N0))
    mine = pl.BlockSpec((n_seq, seq_len, width), lambda i, who_ref: (who_ref[N0], N0, N0))
    tok = whole((tokens, width))
    classes = whole((N2, half, tokens))
    params = pltpu.CompilerParams(dimension_semantics=('arbitrary',), vmem_limit_bytes=56 * KIB * KIB)
    wide_t = jax.ShapeDtypeStruct((n_tp, tokens, width), bf16)
    pair_t = jax.ShapeDtypeStruct((n_tp, tokens, PAIR), bf16)
    row_t = jax.ShapeDtypeStruct((tokens, width), bf16)
    class_t = jax.ShapeDtypeStruct((N2, half, tokens), bf16)
    kv_t = jax.ShapeDtypeStruct((tokens, LANES), bf16)
    work = pl.CostEstimate(flops=13 * 10**9, bytes_accessed=40 * 10**6, transcendentals=N0)
    small = pl.BlockSpec((N1, n_tp, width, LANES), lambda i, *_: (N0, N0, N0, KV_AT // LANES))
    gain_row, w_kv, h_t, dy_t, q_raw, kv_raw, d_o, act, d_gate, d_up = pl.pallas_call(
        proj_kernel, name='proj',
        grid_spec=pltpu.PrefetchScalarGridSpec(
            num_scalar_prefetch=N1, grid=(n_tp,),
            in_specs=[mine, mine, w0_spec, w1_spec, small],
            out_specs=(whole((N1, width)), whole((width, LANES)), classes, classes, per((tokens, PAIR)), whole((tokens, LANES)), per((tokens, PAIR)), per((tokens, width)), per((tokens, width)), per((tokens, width))),
            scratch_shapes=[pltpu.VMEM((tokens, width), bf16)]),
        out_shape=(jax.ShapeDtypeStruct((N1, width), f32), jax.ShapeDtypeStruct((width, LANES), bf16), class_t, class_t, pair_t, kv_t, pair_t, wide_t, wide_t, wide_t),
        compiler_params=params, cost_estimate=work,
    )(who, x_in, dy_in, w_full, w_full, w_full)

    pair_spec = pl.BlockSpec((n_tp, seq_len, PAIR), lambda i: (N0, i, N0))
    kv_spec = pl.BlockSpec((seq_len, LANES), lambda i: (i, N0))
    table = whole((seq_len, LANES))
    att, d_q, d_kv = pl.pallas_call(
        att_kernel, name='attention', grid=(n_seq,),
        in_specs=[pair_spec, kv_spec, pair_spec, table, table, table, table, whole((LANES, seq_len)), whole((LANES, seq_len)), whole((LANES, LANES))],
        out_specs=(pair_spec, pair_spec, kv_spec),
        out_shape=(pair_t, pair_t, kv_t),
        scratch_shapes=[pltpu.VMEM((seq_len, LANES), f32)] * RING,
        compiler_params=params, cost_estimate=work,
    )(q_raw, kv_raw, d_o, *tables)

    gcol_t = jax.ShapeDtypeStruct((N2, half, LANES), f32)
    y_tok, gx_tok, gain_col = pl.pallas_call(
        back_kernel, name='back',
        grid_spec=pltpu.PrefetchScalarGridSpec(
            num_scalar_prefetch=N1, grid=(n_tp,),
            in_specs=[mine, mine, whole((N1, width)), w0_spec, w1_spec, whole((width, LANES)), per((tokens, PAIR)), per((tokens, width)), per((tokens, PAIR)),
                      per((tokens, width)), per((tokens, width)), whole((tokens, LANES))],
            out_specs=(tok, tok, whole((N2, half, LANES))),
            scratch_shapes=[pltpu.VMEM((tokens, width), f32)] * N2),
        out_shape=(row_t, row_t, gcol_t),
        compiler_params=params, cost_estimate=work,
    )(who, x_in, dy_in, gain_row, w_full, w_full, w_kv, att, act, d_q, d_gate, d_up, d_kv)

    class_spec = pl.BlockSpec((N2, N1, half, wide), lambda i: (N0, i, N0, N0))
    own, oth = pl.pallas_call(
        wgrad_kernel, name='wgrad', grid=(n_tp,),
        in_specs=[classes, classes, whole((N2, half, LANES)), per((tokens, PAIR)), per((tokens, width)), per((tokens, PAIR)),
                  per((tokens, width)), per((tokens, width)), whole((tokens, LANES))],
        out_specs=(class_spec, class_spec),
        out_shape=(jax.ShapeDtypeStruct((N2, n_tp, half, wide), f32), jax.ShapeDtypeStruct((N2, n_tp, half, wide), bf16)),
        compiler_params=params, cost_estimate=work,
    )(h_t, dy_t, gain_col, att, act, d_q, d_gate, d_up, d_kv)
    return y_tok, gx_tok, own, oth


def rope_tables(seq_len, head_dim):
    half_dim = head_dim // N2
    inv_freq = np.power(np.float32(10000.0), (-2.0 * np.arange(half_dim) / head_dim).astype(np.float32))
    angle = (np.arange(seq_len, dtype=np.float32)[:, None] * inv_freq[None, :]).astype(np.float32)
    cos_t = np.cos(angle)
    sin_t = np.sin(angle)
    cos_h = np.concatenate([cos_t, cos_t], axis=N1)
    sin_h = np.concatenate([-sin_t, sin_t], axis=N1)
    cos_q = np.concatenate([cos_h, cos_h], axis=N1)
    sin_q = np.concatenate([sin_h, sin_h], axis=N1)
    cos_k = np.concatenate([cos_h, np.ones_like(cos_h)], axis=N1)
    sin_k = np.concatenate([sin_h, np.zeros_like(sin_h)], axis=N1)
    swap = np.eye(LANES)[np.arange(LANES) ^ 32]
    return tuple(jnp.asarray(table, jnp.float32) for table in (cos_q, sin_q, cos_k, sin_k, cos_q.T, sin_q.T)) + (jnp.asarray(swap, jnp.bfloat16),)


def sum_kernel(g_ref, gs_ref, gx_ref, y_ref, below_ref, above_ref, w_out, kv_out, gx_out, y_out, acc, rp, sa, ra1, ra2, sb, rb1, rb2, sc, rc, kvx, gsem, d2s, d2r, ss, rs, cs, cr, ks, kr, xs, xr, lsem, keep):
    f32 = jnp.float32
    bf16 = jnp.bfloat16
    t = lax.axis_index('tp')
    f = lax.axis_index('fsdp')
    c = lax.rem(f, N2)
    yy = lax.rem(lax.div(f, N2), RING)
    zz = lax.div(f, SUB)

    def dev(tt, zc, yc, cc):
        return {'tp': tt, 'fsdp': (zc * RING + yc) * N2 + cc}

    def up(i, d):
        return lax.rem(i + d, RING)

    partner = dev(t, zz, yy, N1 - c)
    xp = [dev(up(t, d), zz, yy, c) for d in range(RING)]
    z_dev = [dev(t, up(zz, d), yy, c) for d in range(RING)]
    y_dev = [dev(t, zz, up(yy, d), c) for d in range(RING)]
    barrier = pltpu.get_barrier_semaphore()
    peers = [partner, xp[N1], xp[N2], xp[N3], z_dev[N1], z_dev[N3], y_dev[N1], y_dev[N3]]
    for peer in peers:
        pl.semaphore_signal(barrier, inc=N1, device_id=peer, device_id_type=MESH_ID)

    def rcopy(src, dst, s_sem, r_sem, peer):
        return pltpu.make_async_remote_copy(src_ref=src, dst_ref=dst, send_sem=s_sem, recv_sem=r_sem, device_id=peer, device_id_type=MESH_ID)

    ring_a = [zz, yy]
    ring_b = [yy, zz]
    dev_a = [z_dev, y_dev]
    dev_b = [y_dev, z_dev]
    order = [N2, N1, N3, N0]

    def g_view(col, j):
        return g_ref.at[N0, :, j] if col == N0 else g_ref.at[N1, :, :, j]

    def gs_view(col, j):
        return gs_ref.at[N0, :, j] if col == N0 else gs_ref.at[N1, :, :, j]

    load = [[None] * RING for _ in range(N2)]
    pair = [[None] * RING for _ in range(N2)]
    for n, d in enumerate(order):
        for col in range(N2):
            j = up(ring_a[col], d)
            load[col][n] = pltpu.make_async_copy(g_view(col, j), acc.at[col, n], gsem.at[col, n])
            load[col][n].start()
    pl.semaphore_wait(barrier, len(peers))
    for n, d in enumerate(order):
        for col in range(N2):
            j = up(ring_a[col], d)
            pair[col][n] = rcopy(gs_view(col, j), rp.at[col, n], d2s.at[col, n], d2r.at[col, n], partner)
            pair[col][n].start()
    mine = gx_ref.shape[N0]
    my_rows = pl.ds(t * mine, mine)
    lower = pl.ds(up(t, N3) * mine, mine)
    upper = pl.ds(up(t, N1) * mine, mine)
    y_up = rcopy(below_ref.at[:, pl.ds(N0, LANES)], y_out.at[lower, pl.ds(N0, LANES)], xs.at[RING], xr.at[RING], xp[N1])
    y_dn = rcopy(above_ref.at[:, pl.ds(LANES, LANES)], y_out.at[upper, pl.ds(LANES, LANES)], xs.at[5], xr.at[5], xp[N3])
    y_up.start()
    y_dn.start()
    x_up = rcopy(gx_ref, gx_out.at[my_rows], xs.at[N0], xr.at[N0], xp[N1])
    x_dn = rcopy(gx_ref, gx_out.at[my_rows], xs.at[N1], xr.at[N1], xp[N3])
    x_up.start()
    x_dn.start()
    local = ((gx_ref, gx_out, my_rows), (y_ref, y_out, my_rows))
    taken = [pltpu.make_async_copy(ref, keep.at[n], lsem.at[n]) for n, (ref, _, _) in enumerate(local)]
    placed = [pltpu.make_async_copy(keep.at[n], out.at[place], lsem.at[n]) for n, (_, out, place) in enumerate(local)]
    for n, (ref, place) in enumerate(((below_ref, lower), (above_ref, upper))):
        placed.append(pltpu.make_async_copy(ref, y_out.at[place], lsem.at[n + N2]))
        placed[n + N2].start()
    for copy in taken:
        copy.start()

    def each(count, body):
        def step(n, carry):
            body(n)
            return carry
        lax.fori_loop(N0, count, step, N0)

    def arrived(col, n):
        load[col][n].wait()
        pair[col][n].wait_recv()

    sends = []

    def send(src, dst, s_sem, r_sem, peer):
        copy = rcopy(src, dst, s_sem, r_sem, peer)
        copy.start()
        sends.append(copy)
        return copy

    for col in range(N2):
        arrived(col, N0)

        def first(q, col=col):
            tt = lax.div(q, 12)
            a2 = lax.rem(lax.div(q, N3), RING)
            r = lax.rem(q, N3)
            sa[col, N0, a2, tt, r] = (acc[col, N0, tt, a2, r] + rp[col, N0, tt, a2, r].astype(f32)).astype(bf16)
        each(48, first)
        send(sa.at[col, N0, pl.ds(N0, N2)], ra1.at[col, N0], ss.at[col, N0], rs.at[col, N0], dev_a[col][N1])
        send(sa.at[col, N0, pl.ds(N2, N2)], ra1.at[col, N1], ss.at[col, N1], rs.at[col, N1], dev_a[col][N3])
    for col in range(N2):
        for n, base, peer in ((N1, N2, N1), (N2, N0, N3)):
            arrived(col, n)

            def plain(q, col=col, n=n, base=base):
                a2 = base + lax.div(q, 12)
                tt = lax.rem(lax.div(q, N3), RING)
                r = lax.rem(q, N3)
                sa[col, n, a2, tt, r] = (acc[col, n, tt, a2, r] + rp[col, n, tt, a2, r].astype(f32)).astype(bf16)
            each(24, plain)
            send(sa.at[col, n, pl.ds(base, N2)], ra2.at[col, n - N1, pl.ds(base, N2)], ss.at[col, n + N1], rs.at[col, n + N1], dev_a[col][peer])
    for col in range(N2):
        for n, base, peer in ((N1, N0, N1), (N2, N2, N3)):
            rcopy(sa.at[col, N0, pl.ds(N0, N2)], ra1.at[col, n - N1], ss.at[col, n - N1], rs.at[col, n - N1], dev_a[col][peer]).wait_recv()

            def joined(q, col=col, n=n, base=base):
                h = lax.div(q, 12)
                a2 = base + h
                tt = lax.rem(lax.div(q, N3), RING)
                r = lax.rem(q, N3)
                val = acc[col, n, tt, a2, r] + rp[col, n, tt, a2, r].astype(f32) + ra1[col, n - N1, h, tt, r].astype(f32)
                sa[col, n, a2, tt, r] = val.astype(bf16)
            each(24, joined)
            send(sa.at[col, n, pl.ds(base, N2)], ra2.at[col, n - N1, pl.ds(base, N2)], ss.at[col, n + N3], rs.at[col, n + N3], dev_a[col][peer])
    for n in range(N2):
        taken[n].wait()
        placed[n].start()
    x_up.wait_recv()
    x_dn.wait_recv()
    half_dn = gx_out.at[lower, pl.ds(N0, LANES)]
    half_up = gx_out.at[upper, pl.ds(LANES, LANES)]
    x_up2 = rcopy(half_dn, half_dn, xs.at[N2], xr.at[N2], xp[N1])
    x_dn2 = rcopy(half_up, half_up, xs.at[N3], xr.at[N3], xp[N3])
    x_up2.start()
    x_dn2.start()
    for col in range(N2):
        arrived(col, N3)
        for n, base, s in ((N1, N2, N2), (N2, N0, N3), (N1, N0, RING), (N2, N2, 5)):
            rcopy(sa.at[col, n, pl.ds(base, N2)], ra2.at[col, n - N1, pl.ds(base, N2)], ss.at[col, s], rs.at[col, s], partner).wait_recv()

        def own(q, col=col):
            a2 = lax.div(q, 12)
            tt = lax.rem(lax.div(q, N3), RING)
            r = lax.rem(q, N3)
            val = acc[col, N3, tt, a2, r] + rp[col, N3, tt, a2, r].astype(f32) + ra2[col, N0, a2, tt, r].astype(f32) + ra2[col, N1, a2, tt, r].astype(f32)
            acc[col, N3, tt, a2, r] = val
        each(48, own)
        far = up(ring_b[col], N2)

        def first_b(q, col=col, far=far):
            tt = lax.div(q, N3)
            r = lax.rem(q, N3)
            sb[col, N0, tt, r] = acc[col, N3, tt, far, r].astype(bf16)
        each(12, first_b)
        send(sb.at[col, N0, pl.ds(N0, N2)], rb1.at[col, N0], ss.at[col, 6], rs.at[col, 6], dev_b[col][N1])
        send(sb.at[col, N0, pl.ds(N2, N2)], rb1.at[col, N1], ss.at[col, 7], rs.at[col, 7], dev_b[col][N3])
        for n, base, peer in ((N1, N2, N1), (N2, N0, N3)):
            pos = up(ring_b[col], peer)

            def plain_b(q, col=col, n=n, base=base, pos=pos):
                tt = base + lax.div(q, N3)
                r = lax.rem(q, N3)
                sb[col, n, tt, r] = acc[col, N3, tt, pos, r].astype(bf16)
            each(6, plain_b)
            send(sb.at[col, n, pl.ds(base, N2)], rb2.at[col, n - N1, pl.ds(base, N2)], ss.at[col, n + 7], rs.at[col, n + 7], dev_b[col][peer])
    for col in range(N2):
        for n, base, peer in ((N1, N0, N1), (N2, N2, N3)):
            rcopy(sb.at[col, N0, pl.ds(N0, N2)], rb1.at[col, n - N1], ss.at[col, n + 5], rs.at[col, n + 5], partner).wait_recv()
            pos = up(ring_b[col], peer)

            def joined_b(q, col=col, n=n, base=base, pos=pos):
                h = lax.div(q, N3)
                tt = base + h
                r = lax.rem(q, N3)
                sb[col, n, tt, r] = (acc[col, N3, tt, pos, r] + rb1[col, n - N1, h, r].astype(f32)).astype(bf16)
            each(6, joined_b)
            send(sb.at[col, n, pl.ds(base, N2)], rb2.at[col, n - N1, pl.ds(base, N2)], ss.at[col, n + 9], rs.at[col, n + 9], dev_b[col][peer])
    for col in range(N2):
        here = ring_b[col]
        for n, base, s in ((N1, N2, SUB), (N2, N0, 9), (N1, N0, 10), (N2, N2, 11)):
            rcopy(sb.at[col, n, pl.ds(base, N2)], rb2.at[col, n - N1, pl.ds(base, N2)], ss.at[col, s], rs.at[col, s], partner).wait_recv()

        def own_b(q, col=col, here=here):
            tt = lax.div(q, N3)
            r = lax.rem(q, N3)
            val = acc[col, N3, tt, here, r] + rb2[col, N0, tt, r].astype(f32) + rb2[col, N1, tt, r].astype(f32)
            acc[col, N3, tt, here, r] = val
            sc[col, tt, r] = val.astype(bf16)
        each(12, own_b)
        for d in (N1, N3, N2):
            to = up(t, d)
            send(sc.at[col, to], rc.at[col, d - N1], cs.at[col, d - N1], cr.at[col, d - N1], xp[d])
        if col == N0:
            def kv_part(q, here=here):
                tt = lax.div(q, N3)
                r = lax.rem(q, N3)
                kvx[t, tt, r] = acc[N0, N3, tt, here, r, :, pl.ds(KV_AT, LANES)]
            each(12, kv_part)
            for d in (N1, N3, N2):
                send(kvx.at[t], kvx.at[t], ks.at[d - N1], kr.at[d - N1], xp[d])
    for col in range(N2):
        here = ring_b[col]
        for d in (N1, N3, N2):
            rcopy(sc.at[col, N0], rc.at[col, d - N1], cs.at[col, d - N1], cr.at[col, d - N1], partner).wait_recv()

        def last(r, col=col, here=here):
            w_out[col, r] = acc[col, N3, t, here, r] + rc[col, N0, r].astype(f32) + rc[col, N1, r].astype(f32) + rc[col, N2, r].astype(f32)
        each(N3, last)
    for d in (N1, N3, N2):
        src = up(t, RING - d)
        rcopy(kvx.at[src], kvx.at[src], ks.at[d - N1], kr.at[d - N1], partner).wait_recv()

    def kv_last(q):
        tt = lax.div(q, N3)
        r = lax.rem(q, N3)
        kv_out[tt, r] = ((kvx[N0, tt, r] + kvx[N1, tt, r]) + kvx[N2, tt, r]) + kvx[N3, tt, r]
    each(12, kv_last)
    for copy in sends:
        copy.wait_send()
    for col in range(N2):
        for n in range(RING):
            pair[col][n].wait_send()
    x_up.wait_send()
    x_dn.wait_send()
    x_up2.wait()
    x_dn2.wait()
    y_up.wait()
    y_dn.wait()
    for copy in placed:
        copy.wait()


def sum_grads(g_pack, g_send, gx_my, y_blocks, n_batch):
    f32 = jnp.float32
    bf16 = jnp.bfloat16
    wide = g_pack.shape[-N1]
    dma = pltpu.SemaphoreType.DMA
    vmem = pl.BlockSpec(memory_space=pltpu.VMEM)
    any_spec = pl.BlockSpec(memory_space=pl.ANY)
    return pl.pallas_call(
        sum_kernel,
        name='sum_grads',
        out_shape=(jax.ShapeDtypeStruct((N2, N3, SUB, wide), f32), jax.ShapeDtypeStruct((RING, N3, SUB, LANES), f32),
                   jax.ShapeDtypeStruct((n_batch,) + gx_my.shape[N1:], bf16), jax.ShapeDtypeStruct((n_batch,) + gx_my.shape[N1:], bf16)),
        in_specs=[any_spec] * RING + [vmem] * N2,
        out_specs=(vmem, vmem, any_spec, any_spec),
        scratch_shapes=[
            pltpu.VMEM((N2, RING, RING, RING, N3, SUB, wide), f32), pltpu.VMEM((N2, RING, RING, RING, N3, SUB, wide), bf16),
            pltpu.VMEM((N2, N3, RING, RING, N3, SUB, wide), bf16), pltpu.VMEM((N2, N2, N2, RING, N3, SUB, wide), bf16), pltpu.VMEM((N2, N2, RING, RING, N3, SUB, wide), bf16),
            pltpu.VMEM((N2, N3, RING, N3, SUB, wide), bf16), pltpu.VMEM((N2, N2, N2, N3, SUB, wide), bf16), pltpu.VMEM((N2, N2, RING, N3, SUB, wide), bf16),
            pltpu.VMEM((N2, RING, N3, SUB, wide), bf16), pltpu.VMEM((N2, N3, N3, SUB, wide), bf16), pltpu.VMEM((RING, RING, N3, SUB, LANES), f32),
            dma((N2, RING)), dma((N2, RING)), dma((N2, RING)), dma((N2, 12)), dma((N2, 12)), dma((N2, N3)), dma((N2, N3)), dma((N3,)), dma((N3,)), dma((6,)), dma((6,)), dma((RING,)), pltpu.VMEM((N2,) + gx_my.shape, bf16),
        ],
        cost_estimate=pl.CostEstimate(flops=60 * 10**9, bytes_accessed=30 * 10**6, transcendentals=N0),
        compiler_params=pltpu.CompilerParams(collective_id=N1, has_side_effects=True, vmem_limit_bytes=60 * KIB * KIB),
    )(g_pack, g_send, gx_my, *y_blocks)


def finish_kernel(w_ref, kv_ref, y_ref, gx_ref, y_out, gx_out, gain_out, q_out, k_out, v_out, o_out, gate_out, up_out, down_out, buf, isem, osem):
    n_batch = y_ref.shape[N0]
    moves = [(ref, out, n) for ref, out in ((y_ref, y_out), (gx_ref, gx_out)) for n in range(n_batch)]
    loads = [pltpu.make_async_copy(ref.at[n], buf.at[m], isem.at[m]) for m, (ref, _, n) in enumerate(moves)]
    stores = [pltpu.make_async_copy(buf.at[m], out.at[n], osem.at[m]) for m, (_, out, n) in enumerate(moves)]
    for copy in loads:
        copy.start()
    lane = lax.broadcasted_iota(jnp.int32, (SUB, LANES), N1)
    gains = []
    for r in range(N3):
        at = slice(SUB * r, SUB * r + SUB)
        gate_out[at, :] = w_ref[N0, r, :, N0:768]
        up_out[at, :] = w_ref[N1, r, :, N0:768]
        q_out[at, :] = w_ref[N0, r, :, 768:960]
        o_out[at, :] = w_ref[N0, r, :, 960:1152]
        down_out[at, N0:LANES] = w_ref[N0, r, :, 1280:1408]
        down_out[at, LANES:768] = w_ref[N1, r, :, 768:1408]
        kv = jnp.where(lane < 32, kv_ref[N0, r], 0.0)
        for n in range(N1, RING):
            kv += pltpu.roll(jnp.where(lane < 32, kv_ref[n, r], 0.0), 32 * n, N1)
        k_out[at, :] = kv[:, N0:64]
        v_out[at, :] = pltpu.roll(kv, 64, N1)[:, N0:64]
        gains.append(jnp.sum(jnp.where(lane == 32, kv_ref[N0, r], 0.0), axis=N1, keepdims=True))
    gain = jnp.concatenate(gains, axis=N0)
    rows = gain.shape[N0]
    diag = lax.broadcasted_iota(jnp.int32, (rows, rows), N0) == lax.broadcasted_iota(jnp.int32, (rows, rows), N1)
    gain_out[ALL] = jnp.sum(jnp.where(diag, jnp.broadcast_to(gain, (rows, rows)), 0.0), axis=N0, keepdims=True)
    for load, store in zip(loads, stores):
        load.wait()
        store.start()
    for store in stores:
        store.wait()


def finish(w_sum, kv_sum, y_land, gx_land, rows, width, nq, head_dim):
    f32 = jnp.float32
    dma = pltpu.SemaphoreType.DMA
    vmem = pl.BlockSpec(memory_space=pltpu.VMEM)
    any_spec = pl.BlockSpec(memory_space=pl.ANY)
    act_t = jax.ShapeDtypeStruct(y_land.shape, y_land.dtype)
    n_moves = N2 * y_land.shape[N0]
    grads = [(N1, rows), (rows, nq), (rows, head_dim), (rows, head_dim), (rows, nq), (rows, width), (rows, width), (rows, width)]
    return pl.pallas_call(
        finish_kernel,
        name='finish',
        out_shape=[act_t, act_t] + [jax.ShapeDtypeStruct(shape, f32) for shape in grads],
        in_specs=[vmem, vmem, any_spec, any_spec],
        out_specs=[any_spec, any_spec] + [vmem] * SUB,
        scratch_shapes=[pltpu.VMEM((n_moves,) + y_land.shape[N1:], y_land.dtype), dma((n_moves,)), dma((n_moves,))],
        compiler_params=pltpu.CompilerParams(vmem_limit_bytes=56 * KIB * KIB),
    )(w_sum, kv_sum, y_land, gx_land)


def solution(mesh):
    n_tp = mesh.shape['tp']

    def device_step(x_in, dy_out, ln_gain, w_q, w_k, w_v, w_o, w_gate, w_up, w_down):
        n_batch, seq_len, width = x_in.shape
        head_dim = w_k.shape[N1]
        rows = w_q.shape[N0]
        nq = w_q.shape[N1]
        mine = n_batch // n_tp
        tp = lax.axis_index('tp')
        core = lax.rem(lax.axis_index('fsdp'), N2)
        full = gather_weights(w_gate, w_q, w_o, w_up, w_down, w_k, w_v, ln_gain).reshape(N2, n_tp, width, -N1)
        wide = full.shape[N3]
        tables = rope_tables(seq_len, head_dim)
        who = jnp.stack([tp, core]).astype(jnp.int32)
        y_tok, gx_tok, g_own, g_oth = layer_step(x_in, dy_out, full, tables, who, seq_len)
        y_my = y_tok.reshape(mine, seq_len, width)
        below = lax.ppermute(y_my, 'tp', [(n, (n + N1) % n_tp) for n in range(n_tp)])
        above = lax.ppermute(y_my, 'tp', [(n, (n - N1) % n_tp) for n in range(n_tp)])
        split = (N2, n_tp, RING, RING, N3, SUB, wide)
        w_sum, kv_sum, gx_land, y_land = sum_grads(g_own.reshape(split), g_oth.reshape(split), gx_tok.reshape(mine, seq_len, width), (y_my, below, above), n_batch)
        y_out, grad_x, gain, grad_wq, grad_wk, grad_wv, wo_t, grad_wgate, grad_wup, down_t = finish(w_sum, kv_sum, y_land, gx_land, rows, width, nq, head_dim)
        return (y_out, grad_x, gain.reshape(rows), grad_wq, grad_wk, grad_wv, wo_t.T, grad_wgate, grad_wup, down_t.T)

    act_spec = P('fsdp', None, None)
    row_spec = P('fsdp', 'tp')
    kv_spec = P('fsdp', None)
    col_spec = P('tp', 'fsdp')
    in_specs = (act_spec, act_spec, P('fsdp'), row_spec, kv_spec, kv_spec, col_spec, row_spec, row_spec, col_spec)
    out_specs = (act_spec, act_spec, P('fsdp'), row_spec, kv_spec, kv_spec, col_spec, row_spec, row_spec, col_spec)
    return jax.shard_map(device_step, mesh=mesh, in_specs=in_specs, out_specs=out_specs, check_vma=False)
```

```python
import numpy as np
import jax
import jax.numpy as jnp
from jax import lax
from jax.sharding import PartitionSpec as P
from jax.experimental import pallas as pl
from jax.experimental.pallas import tpu as pltpu


N0, N1, N2, N3 = range(4)
RING = 4
SUB = 8
LANES = 128
PAIR = 256
KIB = 1024
ALL = Ellipsis
KV_AT = 1152
MESH_ID = pl.DeviceIdType.MESH


def gather_kernel(wg_ref, wq_ref, wo_ref, wu_ref, wd_ref, wk_ref, wv_ref, gain_ref, g_ref, hold, lsem, s1, r1, s2, r2, s3, r3, ds, dr):
    t = lax.axis_index('tp')
    f = lax.axis_index('fsdp')
    c = lax.rem(f, N2)
    at = {'x': t, 'y': lax.rem(lax.div(f, N2), RING), 'z': lax.div(f, SUB)}

    def up(i, d):
        return lax.rem(i + d, RING)

    def dev(where, cc):
        return {'tp': where['x'], 'fsdp': (where['z'] * RING + where['y']) * N2 + cc}

    def peer(axis, d):
        return dev({**at, axis: up(at[axis], d)}, c)

    partner = dev(at, N1 - c)
    barrier = pltpu.get_barrier_semaphore()
    greeted = [partner] + [peer(axis, d) for axis in 'xyz' for d in (N1, N2, N3)]
    for who in greeted:
        pl.semaphore_signal(barrier, inc=N1, device_id=who, device_id_type=MESH_ID)
    f32 = jnp.float32
    bf16 = jnp.bfloat16
    rows = wg_ref.shape[N0]
    lane = lax.broadcasted_iota(jnp.int32, (rows, LANES), N1)
    kv = jnp.concatenate([wk_ref[ALL].astype(f32), wv_ref[ALL].astype(f32)], axis=N1)
    kv = pltpu.roll(kv, lax.rem(LANES - 32 * t, LANES), N1)
    diag = lax.broadcasted_iota(jnp.int32, (rows, rows), N0) == lax.broadcasted_iota(jnp.int32, (rows, rows), N1)
    gain = jnp.sum(jnp.where(diag, jnp.broadcast_to(gain_ref[ALL], (rows, rows)), 0.0), axis=N1, keepdims=True)
    gain_hi = gain.astype(bf16).astype(f32)
    gain_mid = (gain - gain_hi).astype(bf16).astype(f32)
    gain_lo = gain - gain_hi - gain_mid
    small = jnp.where(lane < 32, kv, jnp.where(lane == 32, gain_hi, jnp.where(lane == 33, gain_mid, jnp.where(lane == 34, gain_lo, 0.0))))
    middle = jnp.concatenate([wq_ref[ALL].astype(f32), wo_ref[ALL].astype(f32), small], axis=N1)
    for n in range(N3):
        at_rows = slice(SUB * n, SUB * n + SUB)
        hold[N0, n, :, N0:768] = wg_ref[at_rows, :]
        hold[N0, n, :, 768:1280] = middle[at_rows].astype(bf16)
        hold[N0, n, :, 1280:1408] = wd_ref[at_rows, N0:LANES]
        hold[N1, n, :, N0:768] = wu_ref[at_rows, :]
        hold[N1, n, :, 768:1408] = wd_ref[at_rows, LANES:768]
    pl.semaphore_wait(barrier, len(greeted))
    own = pltpu.make_async_copy(hold, g_ref.at[:, at['x'], at['z'], at['y'], c], lsem.at[N0])
    own.start()

    sent = []

    def push(src, dst, s_sem, r_sem, who):
        copy = pltpu.make_async_remote_copy(src_ref=src, dst_ref=dst, send_sem=s_sem, recv_sem=r_sem, device_id=who, device_id_type=MESH_ID)
        copy.start()
        sent.append(copy)

    def landed(ref, s_sem, r_sem):
        pltpu.make_async_remote_copy(src_ref=ref, dst_ref=ref, send_sem=s_sem, recv_sem=r_sem, device_id=partner, device_id_type=MESH_ID).wait_recv()

    parts = (pl.ds(N0, 768), pl.ds(768, 640))

    def view(k, h, fixed, core, cols=None):
        spot = [fixed.get(axis, slice(None)) for axis in 'xzy']
        block = g_ref.at[h, spot[N0], spot[N1], spot[N2], core, k]
        return block if cols is None else g_ref.at[h, spot[N0], spot[N1], spot[N2], core, k, slice(None), cols]

    orders = ('xyz', 'yzx', 'zxy')
    across = []

    def share(k, h, fixed, cols, n):
        push(view(k, h, fixed, c, cols), view(k, h, fixed, c, cols), ds.at[k, h, n], dr.at[k, h, n], partner)
        across.append((k, h, fixed, cols, n))

    def ring_start(k, h, axis, fixed, ss, rr, base):
        here = {**fixed, axis: at[axis]}
        for n in range(N2):
            ref = view(k, h, here, c, parts[n])
            push(ref, ref, ss.at[k, h, n], rr.at[k, h, n], peer(axis, N1))
            ref = view(k, h, here, c, parts[N1 - n])
            push(ref, ref, ss.at[k, h, N3 - n], rr.at[k, h, N3 - n], peer(axis, N3))

    def ring_forward(k, h, axis, fixed, ss, rr, base):
        for p, d, n in ((N0, N3, N0), (N1, N1, N3)):
            ref = view(k, h, {**fixed, axis: up(at[axis], d)}, c, parts[p])
            landed(ref, ss.at[k, h, n], rr.at[k, h, n])
            push(ref, ref, ss.at[k, h, RING + p], rr.at[k, h, RING + p], peer(axis, RING - d))
            share(k, h, {**fixed, axis: up(at[axis], d)}, parts[p], base + p)

    def ring_share(k, h, axis, fixed, ss, rr, base):
        for m, (p, d, n) in enumerate(((N1, N3, N1), (N0, N1, N2), (N0, N2, RING), (N1, N2, 5))):
            there = {**fixed, axis: up(at[axis], d)}
            landed(view(k, h, there, c, parts[p]), ss.at[k, h, n], rr.at[k, h, n])
            share(k, h, there, parts[p], base + N2 + m)

    streams = [(k, h) for h in range(N2) for k in range(N3)]
    for k, h in streams:
        for d in (N1, N3, N2):
            push(hold.at[h, k], view(k, h, at, c), s1.at[k, h, d - N1], r1.at[k, h, d - N1], peer(orders[k][N0], d))
    own.wait()
    second = {}
    third = {}
    for k, h in streams:
        order = orders[k]
        for d in (N1, N3, N2):
            landed(view(k, h, {**at, order[N0]: up(at[order[N0]], RING - d)}, c), s1.at[k, h, d - N1], r1.at[k, h, d - N1])
        second[k, h] = (k, h, order[N1], {order[N2]: at[order[N2]]}, s2, r2, N1)
        third[k, h] = (k, h, order[N2], {}, s3, r3, 7)
        ring_start(*second[k, h])
        share(k, h, {order[N1]: at[order[N1]], order[N2]: at[order[N2]]}, None, N0)
    for stream in streams:
        ring_forward(*second[stream])
    for stream in streams:
        ring_share(*second[stream])
        ring_start(*third[stream])
    for stream in streams:
        ring_forward(*third[stream])
    for stream in streams:
        ring_share(*third[stream])
    for k, h, fixed, cols, n in across:
        landed(view(k, h, fixed, N1 - c, cols), ds.at[k, h, n], dr.at[k, h, n])
    for copy in sent:
        copy.wait_send()


def gather_weights(w_gate, w_q, w_o, w_up, w_down, w_k, w_v, gain):
    dma = pltpu.SemaphoreType.DMA
    rows = w_gate.shape[N0]
    vmem = pl.BlockSpec(memory_space=pltpu.VMEM)
    return pl.pallas_call(
        gather_kernel,
        name='gather_weights',
        out_shape=jax.ShapeDtypeStruct((N2, RING, RING, RING, N2, N3, SUB, 1408), w_gate.dtype),
        in_specs=[vmem] * SUB,
        out_specs=pl.BlockSpec(memory_space=pl.ANY),
        scratch_shapes=[pltpu.VMEM((N2, N3, SUB, 1408), w_gate.dtype), dma((N1,))] + [dma((N3, N2, N3))] * N2 + [dma((N3, N2, 6))] * RING + [dma((N3, N2, 13))] * N2,
        compiler_params=pltpu.CompilerParams(collective_id=N2, has_side_effects=True, vmem_limit_bytes=60 * KIB * KIB),
    )(w_gate, w_q, w_o.T, w_up, w_down.T, w_k, w_v, gain.reshape(N1, rows))


NT = (((N1,), (N1,)), ((), ()))
NN = (((N1,), (N0,)), ((), ()))
TN = (((N0,), (N0,)), ((), ()))


def dot(left, right, dims=NN):
    return lax.dot_general(left, right, dims, preferred_element_type=jnp.float32)


def by_class(out, cols, vals, core):
    for n in range(32):
        out[lax.rem(n % N2 + core, N2), 24 * (n // N2):24 * (n // N2) + 24, cols] = vals[24 * n:24 * n + 24]


def proj_kernel(who_ref, x_ref, dy_ref, w0_ref, w1_ref, small_ref, gain_ref, wkv_ref, ht_out, dyt_out, q_out, kv_out, do_out, act_out, dg_out, du_out, h_out):
    f32 = jnp.float32
    bf16 = jnp.bfloat16
    tokens, width = h_out.shape
    dy_tok = dy_ref[ALL].reshape(tokens, width)

    @pl.when(pl.program_id(N0) == N0)
    def _():
        lane = lax.broadcasted_iota(jnp.int32, (width, LANES), N1)
        first = small_ref[N0, N0].astype(f32)
        w_kv = jnp.where(lane < 32, first, 0.0)
        for n in range(N1, RING):
            w_kv += pltpu.roll(jnp.where(lane < 32, small_ref[N0, n].astype(f32), 0.0), 32 * n, N1)
        wkv_ref[ALL] = w_kv.astype(bf16)
        parts = first.T
        gain_ref[ALL] = (parts[32:33] + parts[33:34]) + parts[34:35]
        for n in range(tokens // LANES):
            at = slice(n * LANES, n * LANES + LANES)
            seq, row = divmod(n * LANES, x_ref.shape[N1])
            x_f32 = x_ref[seq, row:row + LANES, :].astype(f32)
            x_cent = x_f32 - jnp.mean(x_f32, axis=-N1, keepdims=True)
            x_var = jnp.mean(x_cent * x_cent, axis=-N1, keepdims=True)
            h_norm = (x_cent * lax.rsqrt(x_var + 1e-5) * gain_ref[ALL]).astype(bf16)
            h_out[at, :] = h_norm
            by_class(ht_out, at, h_norm.astype(f32).T.astype(bf16), who_ref[N1])
            by_class(dyt_out, at, dy_ref[seq, row:row + LANES, :].astype(f32).T.astype(bf16), who_ref[N1])
        kv_out[ALL] = dot(h_out[ALL], wkv_ref[ALL]).astype(bf16)

    for n in range(N3):
        cols = slice(n * PAIR, n * PAIR + PAIR)
        gate = dot(h_out[ALL], w0_ref[N0, N0, :, cols]).astype(bf16).astype(f32)
        up = dot(h_out[ALL], w1_ref[N0, N0, :, cols]).astype(bf16).astype(f32)
        if n == N0:
            d_low = dot(dy_tok, w0_ref[N0, N0, :, 1280:1408])
            d_act = jnp.concatenate([d_low, dot(dy_tok, w1_ref[N0, N0, :, 768:896])], axis=N1)
        else:
            d_act = dot(dy_tok, w1_ref[N0, N0, :, 640 + n * PAIR:896 + n * PAIR])
        d_act = d_act.astype(bf16).astype(f32)
        sig = 0.5 * jnp.tanh(0.5 * gate) + 0.5
        silu = gate * sig
        act_out[N0, :, cols] = (silu * up).astype(bf16)
        du_out[N0, :, cols] = (d_act * silu).astype(bf16)
        dg_out[N0, :, cols] = (d_act * up * (sig + silu * (1.0 - sig))).astype(bf16)
    q_out[N0] = dot(h_out[ALL], w0_ref[N0, N0, :, 768:KIB]).astype(bf16)
    do_out[N0] = dot(dy_tok, w0_ref[N0, N0, :, 896:1152]).astype(bf16)


def att_kernel(q_ref, kv_ref, do_ref, cq_ref, sq_ref, ck_ref, sk_ref, cqt_ref, sqt_ref, swap_ref, o_out, dq_out, dkv_out, dk_lo, dk_hi, dv_lo, dv_hi):
    f32 = jnp.float32
    bf16 = jnp.bfloat16
    seq_len = kv_ref.shape[N0]
    lane = lax.broadcasted_iota(jnp.int32, (seq_len, LANES), N1)
    low = lane < 64
    first = lax.rem(lane, 64) < 32
    causal = lax.broadcasted_iota(jnp.int32, (seq_len, seq_len), N0) <= lax.broadcasted_iota(jnp.int32, (seq_len, seq_len), N1)

    def other(vals):
        return jnp.where(first, pltpu.roll(vals, 96, N1), pltpu.roll(vals, 32, N1))

    kv_f32 = kv_ref[ALL].astype(f32)
    kv_rot = kv_f32 * ck_ref[ALL] + other(kv_f32) * sk_ref[ALL]
    zero = jnp.zeros_like(kv_rot)
    k_lo = jnp.where(low, kv_rot, zero)
    v_hi = jnp.where(low, zero, kv_rot)
    k_hi = pltpu.roll(k_lo, 64, N1)
    v_lo = pltpu.roll(v_hi, 64, N1)
    k_cols = jnp.concatenate([k_lo.T, k_hi.T], axis=N1).astype(bf16)
    v_cols = jnp.concatenate([v_lo.T, v_hi.T], axis=N1).astype(bf16)
    k_lo, k_hi, v_lo, v_hi = (vals.astype(bf16) for vals in (k_lo, k_hi, v_lo, v_hi))
    for ref in (dk_lo, dk_hi, dv_lo, dv_hi):
        ref[ALL] = jnp.zeros_like(ref)

    def head(q_tile, k_part, v_part, do_tile):
        scores = jnp.where(causal, dot(k_part, q_tile, NT), -1e30)
        exp_val = jnp.exp(scores - jnp.max(scores, axis=N0, keepdims=True))
        prob = exp_val * (1.0 / jnp.sum(exp_val, axis=N0, keepdims=True))
        d_prob = dot(v_part, do_tile, NT).astype(bf16).astype(f32)
        d_score = prob * (d_prob - jnp.sum(d_prob * prob, axis=N0, keepdims=True))
        return prob.astype(bf16), d_score.astype(bf16)

    def block(tt, carry):
        tiles = []
        for n in range(N2):
            cols = slice(n * LANES, n * LANES + LANES)
            vals = q_ref[tt, :, cols]
            tiles.append(((vals.astype(f32) * cq_ref[ALL] + dot(vals, swap_ref[ALL]) * sq_ref[ALL]) * 0.125).astype(bf16))
        do0 = do_ref[tt, :, N0:LANES]
        do1 = do_ref[tt, :, LANES:PAIR]
        p0, s0 = head(tiles[N0], k_lo, v_hi, do0)
        p1, s1 = head(tiles[N0], k_hi, v_lo, do1)
        p2, s2 = head(tiles[N1], k_lo, v_hi, do1)
        o_out[tt, :, N0:LANES] = dot(v_cols[:, PAIR:512], p0).T.astype(bf16)
        o_out[tt, :, LANES:PAIR] = dot(v_cols, jnp.concatenate([p1, p2], axis=N0)).T.astype(bf16)
        dv_hi[ALL] += dot(jnp.concatenate([p0, p2], axis=N1), jnp.concatenate([do0, do1], axis=N0))
        dv_lo[ALL] += dot(p1, do1)
        dk_lo[ALL] += dot(jnp.concatenate([s0, s2], axis=N1), jnp.concatenate(tiles, axis=N0))
        dk_hi[ALL] += dot(s1, tiles[N0])
        for n, grad in ((N0, dot(k_cols, jnp.concatenate([s0, s1], axis=N0))), (N1, dot(k_cols[:, N0:PAIR], s2))):
            grad = grad.astype(bf16).astype(f32) * 0.125
            swapped = jnp.concatenate([grad[32:64], grad[N0:32], grad[96:LANES], grad[64:96]], axis=N0)
            dq_out[tt, :, n * LANES:n * LANES + LANES] = (grad * cqt_ref[ALL] - swapped * sqt_ref[ALL]).T.astype(bf16)
        return carry
    lax.fori_loop(N0, q_ref.shape[N0], block, N0, unroll=True)
    dk = (dk_lo[ALL] + pltpu.roll(dk_hi[ALL], 64, N1)).astype(bf16).astype(f32)
    dk_raw = dk * ck_ref[ALL] - other(dk) * sk_ref[ALL]
    dv = dv_hi[ALL] + pltpu.roll(dv_lo[ALL], 64, N1)
    dkv_out[ALL] = jnp.where(low, dk_raw, dv).astype(bf16)


def back_kernel(who_ref, x_ref, dy_ref, gain_ref, w0_ref, w1_ref, wkv_ref, o_ref, act_ref, dq_ref, dg_ref, du_ref, dkv_ref, y_out, gx_out, gcol_out, y_acc, dh_acc):
    f32 = jnp.float32
    bf16 = jnp.bfloat16
    step = pl.program_id(N0)
    tokens, width = y_acc.shape
    y_left = jnp.concatenate([o_ref[N0], act_ref[N0]], axis=N1)
    y_right = jnp.concatenate([w0_ref[N0, N0, :, 896:1152], w0_ref[N0, N0, :, 1280:1408], w1_ref[N0, N0, :, 768:1408]], axis=N1)
    h_left = jnp.concatenate([dg_ref[N0], dq_ref[N0], du_ref[N0]], axis=N1)
    h_right = jnp.concatenate([w0_ref[N0, N0, :, N0:KIB], w1_ref[N0, N0, :, N0:768]], axis=N1)
    y_part = dot(y_left, y_right, NT)
    dh_part = dot(h_left, h_right, NT)

    @pl.when(step == N0)
    def _():
        y_acc[ALL] = y_part
        dh_acc[ALL] = dh_part + dot(dkv_ref[ALL], wkv_ref[ALL], NT)

    @pl.when(step > N0)
    def _():
        y_acc[ALL] += y_part
        dh_acc[ALL] += dh_part

    @pl.when(step == pl.num_programs(N0) - N1)
    def _():
        gain = jnp.zeros((N1, width), f32)
        for n in range(tokens // LANES):
            at = slice(n * LANES, n * LANES + LANES)
            seq, row = divmod(n * LANES, x_ref.shape[N1])
            x_f32 = x_ref[seq, row:row + LANES, :].astype(f32)
            y_out[at, :] = (x_f32 + y_acc[at, :]).astype(bf16)
            x_cent = x_f32 - jnp.mean(x_f32, axis=-N1, keepdims=True)
            rstd = lax.rsqrt(jnp.mean(x_cent * x_cent, axis=-N1, keepdims=True) + 1e-5)
            x_hat = x_cent * rstd
            dh = dh_acc[at, :].astype(bf16).astype(f32)
            gain += jnp.sum(dh * x_hat, axis=N0, keepdims=True)
            d_hat = dh * gain_ref[ALL]
            dx = rstd * (d_hat - jnp.mean(d_hat, axis=-N1, keepdims=True) - x_hat * jnp.mean(d_hat * x_hat, axis=-N1, keepdims=True))
            gx_out[at, :] = (dy_ref[seq, row:row + LANES, :].astype(f32) + dx).astype(bf16)
        lane = lax.broadcasted_iota(jnp.int32, (width, LANES), N1)
        by_class(gcol_out, slice(None), jnp.where(lane == 32, jnp.broadcast_to(gain, (LANES, width)).T, 0.0), who_ref[N1])


def wgrad_kernel(ht_ref, dyt_ref, gcol_ref, o_ref, act_ref, dq_ref, dg_ref, du_ref, dkv_ref, own_out, oth_out):
    tt = pl.program_id(N0)
    half = ht_ref.shape[N1]
    lane = lax.broadcasted_iota(jnp.int32, (half, LANES), N1)
    ht = ht_ref[ALL].reshape(N2 * half, ht_ref.shape[N2])
    dyt = dyt_ref[ALL].reshape(N2 * half, dyt_ref.shape[N2])

    def put(n, cols, vals):
        own_out[n, N0, :, cols] = vals[:half]
        oth_out[n, N0, :, cols] = vals[half:].astype(jnp.bfloat16)

    for k in range(N3):
        cols = slice(k * PAIR, k * PAIR + PAIR)
        put(N0, cols, dot(ht, dg_ref[N0, :, cols]))
        put(N1, cols, dot(ht, du_ref[N0, :, cols]))
    g_q = dot(ht, dq_ref[N0])
    g_o = dot(dyt, o_ref[N0])
    put(N0, slice(768, 896), g_q[:, N0:LANES])
    put(N0, slice(896, KIB), g_q[:, LANES:PAIR] + g_o[:, N0:LANES])
    put(N0, slice(KIB, 1152), g_o[:, LANES:PAIR])
    g_kv = dot(ht, dkv_ref[ALL])
    for cls, out in ((N0, own_out), (N1, oth_out)):
        part = pltpu.roll(g_kv[cls * half:cls * half + half], lax.rem(LANES - 32 * tt, LANES), N1)
        out[N0, N0, :, 1152:1280] = (jnp.where(lane < 32, part, 0.0) + gcol_ref[cls]).astype(out.dtype)
    put(N0, slice(1280, 1408), dot(dyt, act_ref[N0, :, N0:LANES]))
    for lo, hi in ((LANES, 384), (384, 640), (640, 768)):
        put(N1, slice(lo + 640, hi + 640), dot(dyt, act_ref[N0, :, lo:hi]))


def layer_step(x_in, dy_in, w_full, tables, who, seq_len):
    f32 = jnp.float32
    bf16 = jnp.bfloat16
    n_tp = w_full.shape[N1]
    wide = w_full.shape[N3]
    width = w_full.shape[N2]
    n_seq = x_in.shape[N0] // n_tp
    tokens = n_seq * seq_len
    half = width // N2

    def whole(shape):
        return pl.BlockSpec(shape, lambda i, *_: (N0,) * len(shape))

    def per(shape):
        return pl.BlockSpec((N1,) + shape, lambda i, *_: (i,) + (N0,) * len(shape))

    w0_spec = pl.BlockSpec((N1, N1, width, wide), lambda i, *_: (N0, i, N0, N0))
    w1_spec = pl.BlockSpec((N1, N1, width, wide), lambda i, *_: (N1, i, N0, N0))
    mine = pl.BlockSpec((n_seq, seq_len, width), lambda i, who_ref: (who_ref[N0], N0, N0))
    tok = whole((tokens, width))
    classes = whole((N2, half, tokens))
    params = pltpu.CompilerParams(dimension_semantics=('arbitrary',), vmem_limit_bytes=56 * KIB * KIB)
    wide_t = jax.ShapeDtypeStruct((n_tp, tokens, width), bf16)
    pair_t = jax.ShapeDtypeStruct((n_tp, tokens, PAIR), bf16)
    row_t = jax.ShapeDtypeStruct((tokens, width), bf16)
    class_t = jax.ShapeDtypeStruct((N2, half, tokens), bf16)
    kv_t = jax.ShapeDtypeStruct((tokens, LANES), bf16)
    work = pl.CostEstimate(flops=13 * 10**9, bytes_accessed=40 * 10**6, transcendentals=N0)
    small = pl.BlockSpec((N1, n_tp, width, LANES), lambda i, *_: (N0, N0, N0, KV_AT // LANES))
    gain_row, w_kv, h_t, dy_t, q_raw, kv_raw, d_o, act, d_gate, d_up = pl.pallas_call(
        proj_kernel, name='proj',
        grid_spec=pltpu.PrefetchScalarGridSpec(
            num_scalar_prefetch=N1, grid=(n_tp,),
            in_specs=[mine, mine, w0_spec, w1_spec, small],
            out_specs=(whole((N1, width)), whole((width, LANES)), classes, classes, per((tokens, PAIR)), whole((tokens, LANES)), per((tokens, PAIR)), per((tokens, width)), per((tokens, width)), per((tokens, width))),
            scratch_shapes=[pltpu.VMEM((tokens, width), bf16)]),
        out_shape=(jax.ShapeDtypeStruct((N1, width), f32), jax.ShapeDtypeStruct((width, LANES), bf16), class_t, class_t, pair_t, kv_t, pair_t, wide_t, wide_t, wide_t),
        compiler_params=params, cost_estimate=work,
    )(who, x_in, dy_in, w_full, w_full, w_full)

    pair_spec = pl.BlockSpec((n_tp, seq_len, PAIR), lambda i: (N0, i, N0))
    kv_spec = pl.BlockSpec((seq_len, LANES), lambda i: (i, N0))
    table = whole((seq_len, LANES))
    att, d_q, d_kv = pl.pallas_call(
        att_kernel, name='attention', grid=(n_seq,),
        in_specs=[pair_spec, kv_spec, pair_spec, table, table, table, table, whole((LANES, seq_len)), whole((LANES, seq_len)), whole((LANES, LANES))],
        out_specs=(pair_spec, pair_spec, kv_spec),
        out_shape=(pair_t, pair_t, kv_t),
        scratch_shapes=[pltpu.VMEM((seq_len, LANES), f32)] * RING,
        compiler_params=params, cost_estimate=work,
    )(q_raw, kv_raw, d_o, *tables)

    gcol_t = jax.ShapeDtypeStruct((N2, half, LANES), f32)
    y_tok, gx_tok, gain_col = pl.pallas_call(
        back_kernel, name='back',
        grid_spec=pltpu.PrefetchScalarGridSpec(
            num_scalar_prefetch=N1, grid=(n_tp,),
            in_specs=[mine, mine, whole((N1, width)), w0_spec, w1_spec, whole((width, LANES)), per((tokens, PAIR)), per((tokens, width)), per((tokens, PAIR)),
                      per((tokens, width)), per((tokens, width)), whole((tokens, LANES))],
            out_specs=(tok, tok, whole((N2, half, LANES))),
            scratch_shapes=[pltpu.VMEM((tokens, width), f32)] * N2),
        out_shape=(row_t, row_t, gcol_t),
        compiler_params=params, cost_estimate=work,
    )(who, x_in, dy_in, gain_row, w_full, w_full, w_kv, att, act, d_q, d_gate, d_up, d_kv)

    class_spec = pl.BlockSpec((N2, N1, half, wide), lambda i: (N0, i, N0, N0))
    own, oth = pl.pallas_call(
        wgrad_kernel, name='wgrad', grid=(n_tp,),
        in_specs=[classes, classes, whole((N2, half, LANES)), per((tokens, PAIR)), per((tokens, width)), per((tokens, PAIR)),
                  per((tokens, width)), per((tokens, width)), whole((tokens, LANES))],
        out_specs=(class_spec, class_spec),
        out_shape=(jax.ShapeDtypeStruct((N2, n_tp, half, wide), f32), jax.ShapeDtypeStruct((N2, n_tp, half, wide), bf16)),
        compiler_params=params, cost_estimate=work,
    )(h_t, dy_t, gain_col, att, act, d_q, d_gate, d_up, d_kv)
    return y_tok, gx_tok, own, oth


def rope_tables(seq_len, head_dim):
    half_dim = head_dim // N2
    inv_freq = np.power(np.float32(10000.0), (-2.0 * np.arange(half_dim) / head_dim).astype(np.float32))
    angle = (np.arange(seq_len, dtype=np.float32)[:, None] * inv_freq[None, :]).astype(np.float32)
    cos_t = np.cos(angle)
    sin_t = np.sin(angle)
    cos_h = np.concatenate([cos_t, cos_t], axis=N1)
    sin_h = np.concatenate([-sin_t, sin_t], axis=N1)
    cos_q = np.concatenate([cos_h, cos_h], axis=N1)
    sin_q = np.concatenate([sin_h, sin_h], axis=N1)
    cos_k = np.concatenate([cos_h, np.ones_like(cos_h)], axis=N1)
    sin_k = np.concatenate([sin_h, np.zeros_like(sin_h)], axis=N1)
    swap = np.eye(LANES)[np.arange(LANES) ^ 32]
    return tuple(jnp.asarray(table, jnp.float32) for table in (cos_q, sin_q, cos_k, sin_k, cos_q.T, sin_q.T)) + (jnp.asarray(swap, jnp.bfloat16),)


def sum_kernel(g_ref, gs_ref, gx_ref, y_ref, below_ref, above_ref, w_out, kv_out, gx_out, y_out, acc, rp, sa, ra1, ra2, sb, rb1, rb2, sc, rc, kvx, gsem, d2s, d2r, ss, rs, cs, cr, ks, kr, xs, xr, lsem, keep):
    f32 = jnp.float32
    bf16 = jnp.bfloat16
    t = lax.axis_index('tp')
    f = lax.axis_index('fsdp')
    c = lax.rem(f, N2)
    yy = lax.rem(lax.div(f, N2), RING)
    zz = lax.div(f, SUB)

    def dev(tt, zc, yc, cc):
        return {'tp': tt, 'fsdp': (zc * RING + yc) * N2 + cc}

    def up(i, d):
        return lax.rem(i + d, RING)

    partner = dev(t, zz, yy, N1 - c)
    xp = [dev(up(t, d), zz, yy, c) for d in range(RING)]
    z_dev = [dev(t, up(zz, d), yy, c) for d in range(RING)]
    y_dev = [dev(t, zz, up(yy, d), c) for d in range(RING)]
    barrier = pltpu.get_barrier_semaphore()
    peers = [partner, xp[N1], xp[N2], xp[N3], z_dev[N1], z_dev[N3], y_dev[N1], y_dev[N3]]
    for peer in peers:
        pl.semaphore_signal(barrier, inc=N1, device_id=peer, device_id_type=MESH_ID)

    def rcopy(src, dst, s_sem, r_sem, peer):
        return pltpu.make_async_remote_copy(src_ref=src, dst_ref=dst, send_sem=s_sem, recv_sem=r_sem, device_id=peer, device_id_type=MESH_ID)

    ring_a = [zz, yy]
    ring_b = [yy, zz]
    dev_a = [z_dev, y_dev]
    dev_b = [y_dev, z_dev]
    order = [N2, N1, N3, N0]

    def g_view(col, j):
        return g_ref.at[N0, :, j] if col == N0 else g_ref.at[N1, :, :, j]

    def gs_view(col, j):
        return gs_ref.at[N0, :, j] if col == N0 else gs_ref.at[N1, :, :, j]

    load = [[None] * RING for _ in range(N2)]
    pair = [[None] * RING for _ in range(N2)]
    for n, d in enumerate(order):
        for col in range(N2):
            j = up(ring_a[col], d)
            load[col][n] = pltpu.make_async_copy(g_view(col, j), acc.at[col, n], gsem.at[col, n])
            load[col][n].start()
    pl.semaphore_wait(barrier, len(peers))
    for n, d in enumerate(order):
        for col in range(N2):
            j = up(ring_a[col], d)
            pair[col][n] = rcopy(gs_view(col, j), rp.at[col, n], d2s.at[col, n], d2r.at[col, n], partner)
            pair[col][n].start()
    mine = gx_ref.shape[N0]
    my_rows = pl.ds(t * mine, mine)
    lower = pl.ds(up(t, N3) * mine, mine)
    upper = pl.ds(up(t, N1) * mine, mine)
    y_up = rcopy(below_ref.at[:, pl.ds(N0, LANES)], y_out.at[lower, pl.ds(N0, LANES)], xs.at[RING], xr.at[RING], xp[N1])
    y_dn = rcopy(above_ref.at[:, pl.ds(LANES, LANES)], y_out.at[upper, pl.ds(LANES, LANES)], xs.at[5], xr.at[5], xp[N3])
    y_up.start()
    y_dn.start()
    x_up = rcopy(gx_ref, gx_out.at[my_rows], xs.at[N0], xr.at[N0], xp[N1])
    x_dn = rcopy(gx_ref, gx_out.at[my_rows], xs.at[N1], xr.at[N1], xp[N3])
    x_up.start()
    x_dn.start()
    local = ((gx_ref, gx_out, my_rows), (y_ref, y_out, my_rows))
    taken = [pltpu.make_async_copy(ref, keep.at[n], lsem.at[n]) for n, (ref, _, _) in enumerate(local)]
    placed = [pltpu.make_async_copy(keep.at[n], out.at[place], lsem.at[n]) for n, (_, out, place) in enumerate(local)]
    for n, (ref, place) in enumerate(((below_ref, lower), (above_ref, upper))):
        placed.append(pltpu.make_async_copy(ref, y_out.at[place], lsem.at[n + N2]))
        placed[n + N2].start()
    for copy in taken:
        copy.start()

    def each(count, body):
        def step(n, carry):
            body(n)
            return carry
        lax.fori_loop(N0, count, step, N0, unroll=N3)

    def arrived(col, n):
        load[col][n].wait()
        pair[col][n].wait_recv()

    sends = []

    def send(src, dst, s_sem, r_sem, peer):
        copy = rcopy(src, dst, s_sem, r_sem, peer)
        copy.start()
        sends.append(copy)
        return copy

    for col in range(N2):
        arrived(col, N0)

        def first(q, col=col):
            tt = lax.div(q, 12)
            a2 = lax.rem(lax.div(q, N3), RING)
            r = lax.rem(q, N3)
            sa[col, N0, a2, tt, r] = (acc[col, N0, tt, a2, r] + rp[col, N0, tt, a2, r].astype(f32)).astype(bf16)
        each(48, first)
        send(sa.at[col, N0, pl.ds(N0, N2)], ra1.at[col, N0], ss.at[col, N0], rs.at[col, N0], dev_a[col][N1])
        send(sa.at[col, N0, pl.ds(N2, N2)], ra1.at[col, N1], ss.at[col, N1], rs.at[col, N1], dev_a[col][N3])
    for col in range(N2):
        for n, base, peer in ((N1, N2, N1), (N2, N0, N3)):
            arrived(col, n)

            def plain(q, col=col, n=n, base=base):
                a2 = base + lax.div(q, 12)
                tt = lax.rem(lax.div(q, N3), RING)
                r = lax.rem(q, N3)
                sa[col, n, a2, tt, r] = (acc[col, n, tt, a2, r] + rp[col, n, tt, a2, r].astype(f32)).astype(bf16)
            each(24, plain)
            send(sa.at[col, n, pl.ds(base, N2)], ra2.at[col, n - N1, pl.ds(base, N2)], ss.at[col, n + N1], rs.at[col, n + N1], dev_a[col][peer])
    for col in range(N2):
        for n, base, peer in ((N1, N0, N1), (N2, N2, N3)):
            rcopy(sa.at[col, N0, pl.ds(N0, N2)], ra1.at[col, n - N1], ss.at[col, n - N1], rs.at[col, n - N1], dev_a[col][peer]).wait_recv()

            def joined(q, col=col, n=n, base=base):
                h = lax.div(q, 12)
                a2 = base + h
                tt = lax.rem(lax.div(q, N3), RING)
                r = lax.rem(q, N3)
                val = acc[col, n, tt, a2, r] + rp[col, n, tt, a2, r].astype(f32) + ra1[col, n - N1, h, tt, r].astype(f32)
                sa[col, n, a2, tt, r] = val.astype(bf16)
            each(24, joined)
            send(sa.at[col, n, pl.ds(base, N2)], ra2.at[col, n - N1, pl.ds(base, N2)], ss.at[col, n + N3], rs.at[col, n + N3], dev_a[col][peer])
    for n in range(N2):
        taken[n].wait()
        placed[n].start()
    x_up.wait_recv()
    x_dn.wait_recv()
    half_dn = gx_out.at[lower, pl.ds(N0, LANES)]
    half_up = gx_out.at[upper, pl.ds(LANES, LANES)]
    x_up2 = rcopy(half_dn, half_dn, xs.at[N2], xr.at[N2], xp[N1])
    x_dn2 = rcopy(half_up, half_up, xs.at[N3], xr.at[N3], xp[N3])
    x_up2.start()
    x_dn2.start()
    for col in range(N2):
        arrived(col, N3)
        for n, base, s in ((N1, N2, N2), (N2, N0, N3), (N1, N0, RING), (N2, N2, 5)):
            rcopy(sa.at[col, n, pl.ds(base, N2)], ra2.at[col, n - N1, pl.ds(base, N2)], ss.at[col, s], rs.at[col, s], partner).wait_recv()

        def own(q, col=col):
            a2 = lax.div(q, 12)
            tt = lax.rem(lax.div(q, N3), RING)
            r = lax.rem(q, N3)
            val = acc[col, N3, tt, a2, r] + rp[col, N3, tt, a2, r].astype(f32) + ra2[col, N0, a2, tt, r].astype(f32) + ra2[col, N1, a2, tt, r].astype(f32)
            acc[col, N3, tt, a2, r] = val
        each(48, own)
        far = up(ring_b[col], N2)

        def first_b(q, col=col, far=far):
            tt = lax.div(q, N3)
            r = lax.rem(q, N3)
            sb[col, N0, tt, r] = acc[col, N3, tt, far, r].astype(bf16)
        each(12, first_b)
        send(sb.at[col, N0, pl.ds(N0, N2)], rb1.at[col, N0], ss.at[col, 6], rs.at[col, 6], dev_b[col][N1])
        send(sb.at[col, N0, pl.ds(N2, N2)], rb1.at[col, N1], ss.at[col, 7], rs.at[col, 7], dev_b[col][N3])
        for n, base, peer in ((N1, N2, N1), (N2, N0, N3)):
            pos = up(ring_b[col], peer)

            def plain_b(q, col=col, n=n, base=base, pos=pos):
                tt = base + lax.div(q, N3)
                r = lax.rem(q, N3)
                sb[col, n, tt, r] = acc[col, N3, tt, pos, r].astype(bf16)
            each(6, plain_b)
            send(sb.at[col, n, pl.ds(base, N2)], rb2.at[col, n - N1, pl.ds(base, N2)], ss.at[col, n + 7], rs.at[col, n + 7], dev_b[col][peer])
    for col in range(N2):
        for n, base, peer in ((N1, N0, N1), (N2, N2, N3)):
            rcopy(sb.at[col, N0, pl.ds(N0, N2)], rb1.at[col, n - N1], ss.at[col, n + 5], rs.at[col, n + 5], partner).wait_recv()
            pos = up(ring_b[col], peer)

            def joined_b(q, col=col, n=n, base=base, pos=pos):
                h = lax.div(q, N3)
                tt = base + h
                r = lax.rem(q, N3)
                sb[col, n, tt, r] = (acc[col, N3, tt, pos, r] + rb1[col, n - N1, h, r].astype(f32)).astype(bf16)
            each(6, joined_b)
            send(sb.at[col, n, pl.ds(base, N2)], rb2.at[col, n - N1, pl.ds(base, N2)], ss.at[col, n + 9], rs.at[col, n + 9], dev_b[col][peer])
    for col in range(N2):
        here = ring_b[col]
        for n, base, s in ((N1, N2, SUB), (N2, N0, 9), (N1, N0, 10), (N2, N2, 11)):
            rcopy(sb.at[col, n, pl.ds(base, N2)], rb2.at[col, n - N1, pl.ds(base, N2)], ss.at[col, s], rs.at[col, s], partner).wait_recv()

        def own_b(q, col=col, here=here):
            tt = lax.div(q, N3)
            r = lax.rem(q, N3)
            val = acc[col, N3, tt, here, r] + rb2[col, N0, tt, r].astype(f32) + rb2[col, N1, tt, r].astype(f32)
            acc[col, N3, tt, here, r] = val
            sc[col, tt, r] = val.astype(bf16)
        each(12, own_b)
        for d in (N1, N3, N2):
            to = up(t, d)
            send(sc.at[col, to], rc.at[col, d - N1], cs.at[col, d - N1], cr.at[col, d - N1], xp[d])
        if col == N0:
            def kv_part(q, here=here):
                tt = lax.div(q, N3)
                r = lax.rem(q, N3)
                kvx[t, tt, r] = acc[N0, N3, tt, here, r, :, pl.ds(KV_AT, LANES)]
            each(12, kv_part)
            for d in (N1, N3, N2):
                send(kvx.at[t], kvx.at[t], ks.at[d - N1], kr.at[d - N1], xp[d])
    for col in range(N2):
        here = ring_b[col]
        for d in (N1, N3, N2):
            rcopy(sc.at[col, N0], rc.at[col, d - N1], cs.at[col, d - N1], cr.at[col, d - N1], partner).wait_recv()

        def last(r, col=col, here=here):
            w_out[col, r] = acc[col, N3, t, here, r] + rc[col, N0, r].astype(f32) + rc[col, N1, r].astype(f32) + rc[col, N2, r].astype(f32)
        each(N3, last)
    for d in (N1, N3, N2):
        src = up(t, RING - d)
        rcopy(kvx.at[src], kvx.at[src], ks.at[d - N1], kr.at[d - N1], partner).wait_recv()

    def kv_last(q):
        tt = lax.div(q, N3)
        r = lax.rem(q, N3)
        kv_out[tt, r] = ((kvx[N0, tt, r] + kvx[N1, tt, r]) + kvx[N2, tt, r]) + kvx[N3, tt, r]
    each(12, kv_last)
    for copy in sends:
        copy.wait_send()
    for col in range(N2):
        for n in range(RING):
            pair[col][n].wait_send()
    x_up.wait_send()
    x_dn.wait_send()
    x_up2.wait()
    x_dn2.wait()
    y_up.wait()
    y_dn.wait()
    for copy in placed:
        copy.wait()


def sum_grads(g_pack, g_send, gx_my, y_blocks, n_batch):
    f32 = jnp.float32
    bf16 = jnp.bfloat16
    wide = g_pack.shape[-N1]
    dma = pltpu.SemaphoreType.DMA
    vmem = pl.BlockSpec(memory_space=pltpu.VMEM)
    any_spec = pl.BlockSpec(memory_space=pl.ANY)
    return pl.pallas_call(
        sum_kernel,
        name='sum_grads',
        out_shape=(jax.ShapeDtypeStruct((N2, N3, SUB, wide), f32), jax.ShapeDtypeStruct((RING, N3, SUB, LANES), f32),
                   jax.ShapeDtypeStruct((n_batch,) + gx_my.shape[N1:], bf16), jax.ShapeDtypeStruct((n_batch,) + gx_my.shape[N1:], bf16)),
        in_specs=[any_spec] * RING + [vmem] * N2,
        out_specs=(vmem, vmem, any_spec, any_spec),
        scratch_shapes=[
            pltpu.VMEM((N2, RING, RING, RING, N3, SUB, wide), f32), pltpu.VMEM((N2, RING, RING, RING, N3, SUB, wide), bf16),
            pltpu.VMEM((N2, N3, RING, RING, N3, SUB, wide), bf16), pltpu.VMEM((N2, N2, N2, RING, N3, SUB, wide), bf16), pltpu.VMEM((N2, N2, RING, RING, N3, SUB, wide), bf16),
            pltpu.VMEM((N2, N3, RING, N3, SUB, wide), bf16), pltpu.VMEM((N2, N2, N2, N3, SUB, wide), bf16), pltpu.VMEM((N2, N2, RING, N3, SUB, wide), bf16),
            pltpu.VMEM((N2, RING, N3, SUB, wide), bf16), pltpu.VMEM((N2, N3, N3, SUB, wide), bf16), pltpu.VMEM((RING, RING, N3, SUB, LANES), f32),
            dma((N2, RING)), dma((N2, RING)), dma((N2, RING)), dma((N2, 12)), dma((N2, 12)), dma((N2, N3)), dma((N2, N3)), dma((N3,)), dma((N3,)), dma((6,)), dma((6,)), dma((RING,)), pltpu.VMEM((N2,) + gx_my.shape, bf16),
        ],
        cost_estimate=pl.CostEstimate(flops=60 * 10**9, bytes_accessed=30 * 10**6, transcendentals=N0),
        compiler_params=pltpu.CompilerParams(collective_id=N1, has_side_effects=True, vmem_limit_bytes=60 * KIB * KIB),
    )(g_pack, g_send, gx_my, *y_blocks)


def finish_kernel(w_ref, kv_ref, y_ref, gx_ref, y_out, gx_out, gain_out, q_out, k_out, v_out, o_out, gate_out, up_out, down_out, buf, isem, osem):
    n_batch = y_ref.shape[N0]
    moves = [(ref, out, n) for ref, out in ((y_ref, y_out), (gx_ref, gx_out)) for n in range(n_batch)]
    loads = [pltpu.make_async_copy(ref.at[n], buf.at[m], isem.at[m]) for m, (ref, _, n) in enumerate(moves)]
    stores = [pltpu.make_async_copy(buf.at[m], out.at[n], osem.at[m]) for m, (_, out, n) in enumerate(moves)]
    for copy in loads:
        copy.start()
    lane = lax.broadcasted_iota(jnp.int32, (SUB, LANES), N1)
    gains = []
    for r in range(N3):
        at = slice(SUB * r, SUB * r + SUB)
        gate_out[at, :] = w_ref[N0, r, :, N0:768]
        up_out[at, :] = w_ref[N1, r, :, N0:768]
        q_out[at, :] = w_ref[N0, r, :, 768:960]
        o_out[at, :] = w_ref[N0, r, :, 960:1152]
        down_out[at, N0:LANES] = w_ref[N0, r, :, 1280:1408]
        down_out[at, LANES:768] = w_ref[N1, r, :, 768:1408]
        kv = jnp.where(lane < 32, kv_ref[N0, r], 0.0)
        for n in range(N1, RING):
            kv += pltpu.roll(jnp.where(lane < 32, kv_ref[n, r], 0.0), 32 * n, N1)
        k_out[at, :] = kv[:, N0:64]
        v_out[at, :] = pltpu.roll(kv, 64, N1)[:, N0:64]
        gains.append(jnp.sum(jnp.where(lane == 32, kv_ref[N0, r], 0.0), axis=N1, keepdims=True))
    gain = jnp.concatenate(gains, axis=N0)
    rows = gain.shape[N0]
    diag = lax.broadcasted_iota(jnp.int32, (rows, rows), N0) == lax.broadcasted_iota(jnp.int32, (rows, rows), N1)
    gain_out[ALL] = jnp.sum(jnp.where(diag, jnp.broadcast_to(gain, (rows, rows)), 0.0), axis=N0, keepdims=True)
    for load, store in zip(loads, stores):
        load.wait()
        store.start()
    for store in stores:
        store.wait()


def finish(w_sum, kv_sum, y_land, gx_land, rows, width, nq, head_dim):
    f32 = jnp.float32
    dma = pltpu.SemaphoreType.DMA
    vmem = pl.BlockSpec(memory_space=pltpu.VMEM)
    any_spec = pl.BlockSpec(memory_space=pl.ANY)
    act_t = jax.ShapeDtypeStruct(y_land.shape, y_land.dtype)
    n_moves = N2 * y_land.shape[N0]
    grads = [(N1, rows), (rows, nq), (rows, head_dim), (rows, head_dim), (rows, nq), (rows, width), (rows, width), (rows, width)]
    return pl.pallas_call(
        finish_kernel,
        name='finish',
        out_shape=[act_t, act_t] + [jax.ShapeDtypeStruct(shape, f32) for shape in grads],
        in_specs=[vmem, vmem, any_spec, any_spec],
        out_specs=[any_spec, any_spec] + [vmem] * SUB,
        scratch_shapes=[pltpu.VMEM((n_moves,) + y_land.shape[N1:], y_land.dtype), dma((n_moves,)), dma((n_moves,))],
        compiler_params=pltpu.CompilerParams(vmem_limit_bytes=56 * KIB * KIB),
    )(w_sum, kv_sum, y_land, gx_land)


def solution(mesh):
    n_tp = mesh.shape['tp']

    def device_step(x_in, dy_out, ln_gain, w_q, w_k, w_v, w_o, w_gate, w_up, w_down):
        n_batch, seq_len, width = x_in.shape
        head_dim = w_k.shape[N1]
        rows = w_q.shape[N0]
        nq = w_q.shape[N1]
        mine = n_batch // n_tp
        tp = lax.axis_index('tp')
        core = lax.rem(lax.axis_index('fsdp'), N2)
        full = gather_weights(w_gate, w_q, w_o, w_up, w_down, w_k, w_v, ln_gain).reshape(N2, n_tp, width, -N1)
        wide = full.shape[N3]
        tables = rope_tables(seq_len, head_dim)
        who = jnp.stack([tp, core]).astype(jnp.int32)
        y_tok, gx_tok, g_own, g_oth = layer_step(x_in, dy_out, full, tables, who, seq_len)
        y_my = y_tok.reshape(mine, seq_len, width)
        below = lax.ppermute(y_my, 'tp', [(n, (n + N1) % n_tp) for n in range(n_tp)])
        above = lax.ppermute(y_my, 'tp', [(n, (n - N1) % n_tp) for n in range(n_tp)])
        split = (N2, n_tp, RING, RING, N3, SUB, wide)
        w_sum, kv_sum, gx_land, y_land = sum_grads(g_own.reshape(split), g_oth.reshape(split), gx_tok.reshape(mine, seq_len, width), (y_my, below, above), n_batch)
        y_out, grad_x, gain, grad_wq, grad_wk, grad_wv, wo_t, grad_wgate, grad_wup, down_t = finish(w_sum, kv_sum, y_land, gx_land, rows, width, nq, head_dim)
        return (y_out, grad_x, gain.reshape(rows), grad_wq, grad_wk, grad_wv, wo_t.T, grad_wgate, grad_wup, down_t.T)

    act_spec = P('fsdp', None, None)
    row_spec = P('fsdp', 'tp')
    kv_spec = P('fsdp', None)
    col_spec = P('tp', 'fsdp')
    in_specs = (act_spec, act_spec, P('fsdp'), row_spec, kv_spec, kv_spec, col_spec, row_spec, row_spec, col_spec)
    out_specs = (act_spec, act_spec, P('fsdp'), row_spec, kv_spec, kv_spec, col_spec, row_spec, row_spec, col_spec)
    return jax.shard_map(device_step, mesh=mesh, in_specs=in_specs, out_specs=out_specs, check_vma=False)
```

```python
import numpy as np
import jax
import jax.numpy as jnp
from jax import lax
from jax.sharding import PartitionSpec as P
from jax.experimental import pallas as pl
from jax.experimental.pallas import tpu as pltpu


N0, N1, N2, N3 = range(4)
RING = 4
SUB = 8
LANES = 128
PAIR = 256
KIB = 1024
ALL = Ellipsis
KV_AT = 1152
MESH_ID = pl.DeviceIdType.MESH


def gather_kernel(wg_ref, wq_ref, wo_ref, wu_ref, wd_ref, wk_ref, wv_ref, gain_ref, g_ref, hold, lsem, s1, r1, s2, r2, s3, r3, ds, dr):
    t = lax.axis_index('tp')
    f = lax.axis_index('fsdp')
    c = lax.rem(f, N2)
    at = {'x': t, 'y': lax.rem(lax.div(f, N2), RING), 'z': lax.div(f, SUB)}

    def up(i, d):
        return lax.rem(i + d, RING)

    def dev(where, cc):
        return {'tp': where['x'], 'fsdp': (where['z'] * RING + where['y']) * N2 + cc}

    def peer(axis, d):
        return dev({**at, axis: up(at[axis], d)}, c)

    partner = dev(at, N1 - c)
    barrier = pltpu.get_barrier_semaphore()
    greeted = [partner] + [peer(axis, d) for axis in 'xyz' for d in (N1, N2, N3)]
    for who in greeted:
        pl.semaphore_signal(barrier, inc=N1, device_id=who, device_id_type=MESH_ID)
    f32 = jnp.float32
    bf16 = jnp.bfloat16
    rows = wg_ref.shape[N0]
    lane = lax.broadcasted_iota(jnp.int32, (rows, LANES), N1)
    kv = jnp.concatenate([wk_ref[ALL].astype(f32), wv_ref[ALL].astype(f32)], axis=N1)
    kv = pltpu.roll(kv, lax.rem(LANES - 32 * t, LANES), N1)
    diag = lax.broadcasted_iota(jnp.int32, (rows, rows), N0) == lax.broadcasted_iota(jnp.int32, (rows, rows), N1)
    gain = jnp.sum(jnp.where(diag, jnp.broadcast_to(gain_ref[ALL], (rows, rows)), 0.0), axis=N1, keepdims=True)
    gain_hi = gain.astype(bf16).astype(f32)
    gain_mid = (gain - gain_hi).astype(bf16).astype(f32)
    gain_lo = gain - gain_hi - gain_mid
    small = jnp.where(lane < 32, kv, jnp.where(lane == 32, gain_hi, jnp.where(lane == 33, gain_mid, jnp.where(lane == 34, gain_lo, 0.0))))
    middle = jnp.concatenate([wq_ref[ALL].astype(f32), wo_ref[ALL].astype(f32), small], axis=N1)
    for n in range(N3):
        at_rows = slice(SUB * n, SUB * n + SUB)
        hold[N0, n, :, N0:768] = wg_ref[at_rows, :]
        hold[N0, n, :, 768:1280] = middle[at_rows].astype(bf16)
        hold[N0, n, :, 1280:1408] = wd_ref[at_rows, N0:LANES]
        hold[N1, n, :, N0:768] = wu_ref[at_rows, :]
        hold[N1, n, :, 768:1408] = wd_ref[at_rows, LANES:768]
    pl.semaphore_wait(barrier, len(greeted))
    own = pltpu.make_async_copy(hold, g_ref.at[:, at['x'], at['z'], at['y'], c], lsem.at[N0])
    own.start()

    sent = []

    def push(src, dst, s_sem, r_sem, who):
        copy = pltpu.make_async_remote_copy(src_ref=src, dst_ref=dst, send_sem=s_sem, recv_sem=r_sem, device_id=who, device_id_type=MESH_ID)
        copy.start()
        sent.append(copy)

    def landed(ref, s_sem, r_sem):
        pltpu.make_async_remote_copy(src_ref=ref, dst_ref=ref, send_sem=s_sem, recv_sem=r_sem, device_id=partner, device_id_type=MESH_ID).wait_recv()

    parts = (pl.ds(N0, 768), pl.ds(768, 640))

    def view(k, h, fixed, core, cols=None):
        spot = [fixed.get(axis, slice(None)) for axis in 'xzy']
        block = g_ref.at[h, spot[N0], spot[N1], spot[N2], core, k]
        return block if cols is None else g_ref.at[h, spot[N0], spot[N1], spot[N2], core, k, slice(None), cols]

    orders = ('xyz', 'yzx', 'zxy')
    across = []

    def share(k, h, fixed, cols, n):
        push(view(k, h, fixed, c, cols), view(k, h, fixed, c, cols), ds.at[k, h, n], dr.at[k, h, n], partner)
        across.append((k, h, fixed, cols, n))

    def ring_start(k, h, axis, fixed, ss, rr, base):
        here = {**fixed, axis: at[axis]}
        for n in range(N2):
            ref = view(k, h, here, c, parts[n])
            push(ref, ref, ss.at[k, h, n], rr.at[k, h, n], peer(axis, N1))
            ref = view(k, h, here, c, parts[N1 - n])
            push(ref, ref, ss.at[k, h, N3 - n], rr.at[k, h, N3 - n], peer(axis, N3))

    def ring_forward(k, h, axis, fixed, ss, rr, base):
        for p, d, n in ((N0, N3, N0), (N1, N1, N3)):
            ref = view(k, h, {**fixed, axis: up(at[axis], d)}, c, parts[p])
            landed(ref, ss.at[k, h, n], rr.at[k, h, n])
            push(ref, ref, ss.at[k, h, RING + p], rr.at[k, h, RING + p], peer(axis, RING - d))
            share(k, h, {**fixed, axis: up(at[axis], d)}, parts[p], base + p)

    def ring_share(k, h, axis, fixed, ss, rr, base):
        for m, (p, d, n) in enumerate(((N1, N3, N1), (N0, N1, N2), (N0, N2, RING), (N1, N2, 5))):
            there = {**fixed, axis: up(at[axis], d)}
            landed(view(k, h, there, c, parts[p]), ss.at[k, h, n], rr.at[k, h, n])
            share(k, h, there, parts[p], base + N2 + m)

    streams = [(k, h) for h in range(N2) for k in range(N3)]
    for k, h in streams:
        for d in (N1, N3, N2):
            push(hold.at[h, k], view(k, h, at, c), s1.at[k, h, d - N1], r1.at[k, h, d - N1], peer(orders[k][N0], d))
    own.wait()
    second = {}
    third = {}
    for k, h in streams:
        order = orders[k]
        for d in (N1, N3, N2):
            landed(view(k, h, {**at, order[N0]: up(at[order[N0]], RING - d)}, c), s1.at[k, h, d - N1], r1.at[k, h, d - N1])
        second[k, h] = (k, h, order[N1], {order[N2]: at[order[N2]]}, s2, r2, N1)
        third[k, h] = (k, h, order[N2], {}, s3, r3, 7)
        ring_start(*second[k, h])
        share(k, h, {order[N1]: at[order[N1]], order[N2]: at[order[N2]]}, None, N0)
    for stream in streams:
        ring_forward(*second[stream])
    for stream in streams:
        ring_share(*second[stream])
        ring_start(*third[stream])
    for stream in streams:
        ring_forward(*third[stream])
    for stream in streams:
        ring_share(*third[stream])
    for k, h, fixed, cols, n in across:
        landed(view(k, h, fixed, N1 - c, cols), ds.at[k, h, n], dr.at[k, h, n])
    for copy in sent:
        copy.wait_send()


def gather_weights(w_gate, w_q, w_o, w_up, w_down, w_k, w_v, gain):
    dma = pltpu.SemaphoreType.DMA
    rows = w_gate.shape[N0]
    vmem = pl.BlockSpec(memory_space=pltpu.VMEM)
    return pl.pallas_call(
        gather_kernel,
        name='gather_weights',
        out_shape=jax.ShapeDtypeStruct((N2, RING, RING, RING, N2, N3, SUB, 1408), w_gate.dtype),
        in_specs=[vmem] * SUB,
        out_specs=pl.BlockSpec(memory_space=pl.ANY),
        scratch_shapes=[pltpu.VMEM((N2, N3, SUB, 1408), w_gate.dtype), dma((N1,))] + [dma((N3, N2, N3))] * N2 + [dma((N3, N2, 6))] * RING + [dma((N3, N2, 13))] * N2,
        compiler_params=pltpu.CompilerParams(collective_id=N2, has_side_effects=True, vmem_limit_bytes=60 * KIB * KIB),
    )(w_gate, w_q, w_o.T, w_up, w_down.T, w_k, w_v, gain.reshape(N1, rows))


NT = (((N1,), (N1,)), ((), ()))
NN = (((N1,), (N0,)), ((), ()))
TN = (((N0,), (N0,)), ((), ()))


def dot(left, right, dims=NN):
    return lax.dot_general(left, right, dims, preferred_element_type=jnp.float32)


def by_class(out, cols, vals, core):
    for n in range(32):
        out[lax.rem(n % N2 + core, N2), 24 * (n // N2):24 * (n // N2) + 24, cols] = vals[24 * n:24 * n + 24]


def proj_kernel(who_ref, x_ref, dy_ref, w0_ref, w1_ref, small_ref, gain_ref, wkv_ref, ht_out, dyt_out, q_out, kv_out, do_out, act_out, dg_out, du_out, h_out):
    f32 = jnp.float32
    bf16 = jnp.bfloat16
    tokens, width = h_out.shape
    dy_tok = dy_ref[ALL].reshape(tokens, width)

    @pl.when(pl.program_id(N0) == N0)
    def _():
        lane = lax.broadcasted_iota(jnp.int32, (width, LANES), N1)
        first = small_ref[N0, N0].astype(f32)
        w_kv = jnp.where(lane < 32, first, 0.0)
        for n in range(N1, RING):
            w_kv += pltpu.roll(jnp.where(lane < 32, small_ref[N0, n].astype(f32), 0.0), 32 * n, N1)
        wkv_ref[ALL] = w_kv.astype(bf16)
        parts = first.T
        gain_ref[ALL] = (parts[32:33] + parts[33:34]) + parts[34:35]
        for n in range(tokens // LANES):
            at = slice(n * LANES, n * LANES + LANES)
            seq, row = divmod(n * LANES, x_ref.shape[N1])
            x_f32 = x_ref[seq, row:row + LANES, :].astype(f32)
            x_cent = x_f32 - jnp.mean(x_f32, axis=-N1, keepdims=True)
            x_var = jnp.mean(x_cent * x_cent, axis=-N1, keepdims=True)
            h_norm = (x_cent * lax.rsqrt(x_var + 1e-5) * gain_ref[ALL]).astype(bf16)
            h_out[at, :] = h_norm
            by_class(ht_out, at, h_norm.astype(f32).T.astype(bf16), who_ref[N1])
            by_class(dyt_out, at, dy_ref[seq, row:row + LANES, :].astype(f32).T.astype(bf16), who_ref[N1])
        kv_out[ALL] = dot(h_out[ALL], wkv_ref[ALL]).astype(bf16)

    for n in range(N3):
        cols = slice(n * PAIR, n * PAIR + PAIR)
        gate = dot(h_out[ALL], w0_ref[N0, N0, :, cols]).astype(bf16).astype(f32)
        up = dot(h_out[ALL], w1_ref[N0, N0, :, cols]).astype(bf16).astype(f32)
        if n == N0:
            d_low = dot(dy_tok, w0_ref[N0, N0, :, 1280:1408])
            d_act = jnp.concatenate([d_low, dot(dy_tok, w1_ref[N0, N0, :, 768:896])], axis=N1)
        else:
            d_act = dot(dy_tok, w1_ref[N0, N0, :, 640 + n * PAIR:896 + n * PAIR])
        d_act = d_act.astype(bf16).astype(f32)
        sig = 0.5 * jnp.tanh(0.5 * gate) + 0.5
        silu = gate * sig
        act_out[N0, :, cols] = (silu * up).astype(bf16)
        du_out[N0, :, cols] = (d_act * silu).astype(bf16)
        dg_out[N0, :, cols] = (d_act * up * (sig + silu * (1.0 - sig))).astype(bf16)
    q_out[N0] = dot(h_out[ALL], w0_ref[N0, N0, :, 768:KIB]).astype(bf16)
    do_out[N0] = dot(dy_tok, w0_ref[N0, N0, :, 896:1152]).astype(bf16)


def att_kernel(q_ref, kv_ref, do_ref, cq_ref, sq_ref, ck_ref, sk_ref, cqt_ref, sqt_ref, swap_ref, o_out, dq_out, dkv_out, dk_lo, dk_hi, dv_lo, dv_hi):
    f32 = jnp.float32
    bf16 = jnp.bfloat16
    seq_len = kv_ref.shape[N0]
    lane = lax.broadcasted_iota(jnp.int32, (seq_len, LANES), N1)
    low = lane < 64
    first = lax.rem(lane, 64) < 32
    causal = lax.broadcasted_iota(jnp.int32, (seq_len, seq_len), N0) <= lax.broadcasted_iota(jnp.int32, (seq_len, seq_len), N1)

    def other(vals):
        return jnp.where(first, pltpu.roll(vals, 96, N1), pltpu.roll(vals, 32, N1))

    kv_f32 = kv_ref[ALL].astype(f32)
    kv_rot = kv_f32 * ck_ref[ALL] + other(kv_f32) * sk_ref[ALL]
    zero = jnp.zeros_like(kv_rot)
    k_lo = jnp.where(low, kv_rot, zero)
    v_hi = jnp.where(low, zero, kv_rot)
    k_hi = pltpu.roll(k_lo, 64, N1)
    v_lo = pltpu.roll(v_hi, 64, N1)
    k_cols = jnp.concatenate([k_lo.T, k_hi.T], axis=N1).astype(bf16)
    v_cols = jnp.concatenate([v_lo.T, v_hi.T], axis=N1).astype(bf16)
    k_lo, k_hi, v_lo, v_hi = (vals.astype(bf16) for vals in (k_lo, k_hi, v_lo, v_hi))
    for ref in (dk_lo, dk_hi, dv_lo, dv_hi):
        ref[ALL] = jnp.zeros_like(ref)

    def head(q_tile, k_part, v_part, do_tile):
        scores = jnp.where(causal, dot(k_part, q_tile, NT), -1e30)
        exp_val = jnp.exp(scores - jnp.max(scores, axis=N0, keepdims=True))
        prob = exp_val * (1.0 / jnp.sum(exp_val, axis=N0, keepdims=True))
        d_prob = dot(v_part, do_tile, NT).astype(bf16).astype(f32)
        d_score = prob * (d_prob - jnp.sum(d_prob * prob, axis=N0, keepdims=True))
        return prob.astype(bf16), d_score.astype(bf16)

    def block(tt, carry):
        tiles = []
        for n in range(N2):
            cols = slice(n * LANES, n * LANES + LANES)
            vals = q_ref[tt, :, cols]
            tiles.append(((vals.astype(f32) * cq_ref[ALL] + dot(vals, swap_ref[ALL]) * sq_ref[ALL]) * 0.125).astype(bf16))
        do0 = do_ref[tt, :, N0:LANES]
        do1 = do_ref[tt, :, LANES:PAIR]
        p0, s0 = head(tiles[N0], k_lo, v_hi, do0)
        p1, s1 = head(tiles[N0], k_hi, v_lo, do1)
        p2, s2 = head(tiles[N1], k_lo, v_hi, do1)
        o_out[tt, :, N0:LANES] = dot(v_cols[:, PAIR:512], p0).T.astype(bf16)
        o_out[tt, :, LANES:PAIR] = dot(v_cols, jnp.concatenate([p1, p2], axis=N0)).T.astype(bf16)
        dv_hi[ALL] += dot(jnp.concatenate([p0, p2], axis=N1), jnp.concatenate([do0, do1], axis=N0))
        dv_lo[ALL] += dot(p1, do1)
        dk_lo[ALL] += dot(jnp.concatenate([s0, s2], axis=N1), jnp.concatenate(tiles, axis=N0))
        dk_hi[ALL] += dot(s1, tiles[N0])
        for n, grad in ((N0, dot(k_cols, jnp.concatenate([s0, s1], axis=N0))), (N1, dot(k_cols[:, N0:PAIR], s2))):
            grad = grad.astype(bf16).astype(f32) * 0.125
            swapped = jnp.concatenate([grad[32:64], grad[N0:32], grad[96:LANES], grad[64:96]], axis=N0)
            dq_out[tt, :, n * LANES:n * LANES + LANES] = (grad * cqt_ref[ALL] - swapped * sqt_ref[ALL]).T.astype(bf16)
        return carry
    lax.fori_loop(N0, q_ref.shape[N0], block, N0, unroll=True)
    dk = (dk_lo[ALL] + pltpu.roll(dk_hi[ALL], 64, N1)).astype(bf16).astype(f32)
    dk_raw = dk * ck_ref[ALL] - other(dk) * sk_ref[ALL]
    dv = dv_hi[ALL] + pltpu.roll(dv_lo[ALL], 64, N1)
    dkv_out[ALL] = jnp.where(low, dk_raw, dv).astype(bf16)


def back_kernel(who_ref, x_ref, dy_ref, gain_ref, w0_ref, w1_ref, wkv_ref, o_ref, act_ref, dq_ref, dg_ref, du_ref, dkv_ref, y_out, gx_out, gcol_out, y_acc, dh_acc):
    f32 = jnp.float32
    bf16 = jnp.bfloat16
    step = pl.program_id(N0)
    tokens, width = y_acc.shape
    y_left = jnp.concatenate([o_ref[N0], act_ref[N0]], axis=N1)
    y_right = jnp.concatenate([w0_ref[N0, N0, :, 896:1152], w0_ref[N0, N0, :, 1280:1408], w1_ref[N0, N0, :, 768:1408]], axis=N1)
    h_left = jnp.concatenate([dg_ref[N0], dq_ref[N0], du_ref[N0]], axis=N1)
    h_right = jnp.concatenate([w0_ref[N0, N0, :, N0:KIB], w1_ref[N0, N0, :, N0:768]], axis=N1)
    y_part = dot(y_left, y_right, NT)
    dh_part = dot(h_left, h_right, NT)

    @pl.when(step == N0)
    def _():
        y_acc[ALL] = y_part
        dh_acc[ALL] = dh_part + dot(dkv_ref[ALL], wkv_ref[ALL], NT)

    @pl.when(step > N0)
    def _():
        y_acc[ALL] += y_part
        dh_acc[ALL] += dh_part

    @pl.when(step == pl.num_programs(N0) - N1)
    def _():
        gain = jnp.zeros((N1, width), f32)
        for n in range(tokens // LANES):
            at = slice(n * LANES, n * LANES + LANES)
            seq, row = divmod(n * LANES, x_ref.shape[N1])
            x_f32 = x_ref[seq, row:row + LANES, :].astype(f32)
            y_out[at, :] = (x_f32 + y_acc[at, :]).astype(bf16)
            x_cent = x_f32 - jnp.mean(x_f32, axis=-N1, keepdims=True)
            rstd = lax.rsqrt(jnp.mean(x_cent * x_cent, axis=-N1, keepdims=True) + 1e-5)
            x_hat = x_cent * rstd
            dh = dh_acc[at, :].astype(bf16).astype(f32)
            gain += jnp.sum(dh * x_hat, axis=N0, keepdims=True)
            d_hat = dh * gain_ref[ALL]
            dx = rstd * (d_hat - jnp.mean(d_hat, axis=-N1, keepdims=True) - x_hat * jnp.mean(d_hat * x_hat, axis=-N1, keepdims=True))
            gx_out[at, :] = (dy_ref[seq, row:row + LANES, :].astype(f32) + dx).astype(bf16)
        lane = lax.broadcasted_iota(jnp.int32, (width, LANES), N1)
        by_class(gcol_out, slice(None), jnp.where(lane == 32, jnp.broadcast_to(gain, (LANES, width)).T, 0.0), who_ref[N1])


def wgrad_kernel(ht_ref, dyt_ref, gcol_ref, o_ref, act_ref, dq_ref, dg_ref, du_ref, dkv_ref, own_out, oth_out):
    tt = pl.program_id(N0)
    half = ht_ref.shape[N1]
    lane = lax.broadcasted_iota(jnp.int32, (half, LANES), N1)
    ht = ht_ref[ALL].reshape(N2 * half, ht_ref.shape[N2])
    dyt = dyt_ref[ALL].reshape(N2 * half, dyt_ref.shape[N2])

    def put(n, cols, vals):
        own_out[n, N0, :, cols] = vals[:half]
        oth_out[n, N0, :, cols] = vals[half:].astype(jnp.bfloat16)

    for k in range(N3):
        cols = slice(k * PAIR, k * PAIR + PAIR)
        put(N0, cols, dot(ht, dg_ref[N0, :, cols]))
        put(N1, cols, dot(ht, du_ref[N0, :, cols]))
    g_q = dot(ht, dq_ref[N0])
    g_o = dot(dyt, o_ref[N0])
    put(N0, slice(768, 896), g_q[:, N0:LANES])
    put(N0, slice(896, KIB), g_q[:, LANES:PAIR] + g_o[:, N0:LANES])
    put(N0, slice(KIB, 1152), g_o[:, LANES:PAIR])
    g_kv = dot(ht, dkv_ref[ALL])
    for cls, out in ((N0, own_out), (N1, oth_out)):
        part = pltpu.roll(g_kv[cls * half:cls * half + half], lax.rem(LANES - 32 * tt, LANES), N1)
        out[N0, N0, :, 1152:1280] = (jnp.where(lane < 32, part, 0.0) + gcol_ref[cls]).astype(out.dtype)
    put(N0, slice(1280, 1408), dot(dyt, act_ref[N0, :, N0:LANES]))
    for lo, hi in ((LANES, 384), (384, 640), (640, 768)):
        put(N1, slice(lo + 640, hi + 640), dot(dyt, act_ref[N0, :, lo:hi]))


def layer_step(x_in, dy_in, w_full, tables, who, seq_len):
    f32 = jnp.float32
    bf16 = jnp.bfloat16
    n_tp = w_full.shape[N1]
    wide = w_full.shape[N3]
    width = w_full.shape[N2]
    n_seq = x_in.shape[N0] // n_tp
    tokens = n_seq * seq_len
    half = width // N2

    def whole(shape):
        return pl.BlockSpec(shape, lambda i, *_: (N0,) * len(shape))

    def per(shape):
        return pl.BlockSpec((N1,) + shape, lambda i, *_: (i,) + (N0,) * len(shape))

    w0_spec = pl.BlockSpec((N1, N1, width, wide), lambda i, *_: (N0, i, N0, N0))
    w1_spec = pl.BlockSpec((N1, N1, width, wide), lambda i, *_: (N1, i, N0, N0))
    mine = pl.BlockSpec((n_seq, seq_len, width), lambda i, who_ref: (who_ref[N0], N0, N0))
    tok = whole((tokens, width))
    classes = whole((N2, half, tokens))
    params = pltpu.CompilerParams(dimension_semantics=('arbitrary',), vmem_limit_bytes=56 * KIB * KIB)
    wide_t = jax.ShapeDtypeStruct((n_tp, tokens, width), bf16)
    pair_t = jax.ShapeDtypeStruct((n_tp, tokens, PAIR), bf16)
    row_t = jax.ShapeDtypeStruct((tokens, width), bf16)
    class_t = jax.ShapeDtypeStruct((N2, half, tokens), bf16)
    kv_t = jax.ShapeDtypeStruct((tokens, LANES), bf16)
    work = pl.CostEstimate(flops=13 * 10**9, bytes_accessed=40 * 10**6, transcendentals=N0)
    small = pl.BlockSpec((N1, n_tp, width, LANES), lambda i, *_: (N0, N0, N0, KV_AT // LANES))
    gain_row, w_kv, h_t, dy_t, q_raw, kv_raw, d_o, act, d_gate, d_up = pl.pallas_call(
        proj_kernel, name='proj',
        grid_spec=pltpu.PrefetchScalarGridSpec(
            num_scalar_prefetch=N1, grid=(n_tp,),
            in_specs=[mine, mine, w0_spec, w1_spec, small],
            out_specs=(whole((N1, width)), whole((width, LANES)), classes, classes, per((tokens, PAIR)), whole((tokens, LANES)), per((tokens, PAIR)), per((tokens, width)), per((tokens, width)), per((tokens, width))),
            scratch_shapes=[pltpu.VMEM((tokens, width), bf16)]),
        out_shape=(jax.ShapeDtypeStruct((N1, width), f32), jax.ShapeDtypeStruct((width, LANES), bf16), class_t, class_t, pair_t, kv_t, pair_t, wide_t, wide_t, wide_t),
        compiler_params=params, cost_estimate=work,
    )(who, x_in, dy_in, w_full, w_full, w_full)

    pair_spec = pl.BlockSpec((n_tp, seq_len, PAIR), lambda i: (N0, i, N0))
    kv_spec = pl.BlockSpec((seq_len, LANES), lambda i: (i, N0))
    table = whole((seq_len, LANES))
    att, d_q, d_kv = pl.pallas_call(
        att_kernel, name='attention', grid=(n_seq,),
        in_specs=[pair_spec, kv_spec, pair_spec, table, table, table, table, whole((LANES, seq_len)), whole((LANES, seq_len)), whole((LANES, LANES))],
        out_specs=(pair_spec, pair_spec, kv_spec),
        out_shape=(pair_t, pair_t, kv_t),
        scratch_shapes=[pltpu.VMEM((seq_len, LANES), f32)] * RING,
        compiler_params=params, cost_estimate=work,
    )(q_raw, kv_raw, d_o, *tables)

    gcol_t = jax.ShapeDtypeStruct((N2, half, LANES), f32)
    y_tok, gx_tok, gain_col = pl.pallas_call(
        back_kernel, name='back',
        grid_spec=pltpu.PrefetchScalarGridSpec(
            num_scalar_prefetch=N1, grid=(n_tp,),
            in_specs=[mine, mine, whole((N1, width)), w0_spec, w1_spec, whole((width, LANES)), per((tokens, PAIR)), per((tokens, width)), per((tokens, PAIR)),
                      per((tokens, width)), per((tokens, width)), whole((tokens, LANES))],
            out_specs=(tok, tok, whole((N2, half, LANES))),
            scratch_shapes=[pltpu.VMEM((tokens, width), f32)] * N2),
        out_shape=(row_t, row_t, gcol_t),
        compiler_params=params, cost_estimate=work,
    )(who, x_in, dy_in, gain_row, w_full, w_full, w_kv, att, act, d_q, d_gate, d_up, d_kv)

    class_spec = pl.BlockSpec((N2, N1, half, wide), lambda i: (N0, i, N0, N0))
    own, oth = pl.pallas_call(
        wgrad_kernel, name='wgrad', grid=(n_tp,),
        in_specs=[classes, classes, whole((N2, half, LANES)), per((tokens, PAIR)), per((tokens, width)), per((tokens, PAIR)),
                  per((tokens, width)), per((tokens, width)), whole((tokens, LANES))],
        out_specs=(class_spec, class_spec),
        out_shape=(jax.ShapeDtypeStruct((N2, n_tp, half, wide), f32), jax.ShapeDtypeStruct((N2, n_tp, half, wide), bf16)),
        compiler_params=params, cost_estimate=work,
    )(h_t, dy_t, gain_col, att, act, d_q, d_gate, d_up, d_kv)
    return y_tok, gx_tok, own, oth


def rope_tables(seq_len, head_dim):
    half_dim = head_dim // N2
    inv_freq = np.power(np.float32(10000.0), (-2.0 * np.arange(half_dim) / head_dim).astype(np.float32))
    angle = (np.arange(seq_len, dtype=np.float32)[:, None] * inv_freq[None, :]).astype(np.float32)
    cos_t = np.cos(angle)
    sin_t = np.sin(angle)
    cos_h = np.concatenate([cos_t, cos_t], axis=N1)
    sin_h = np.concatenate([-sin_t, sin_t], axis=N1)
    cos_q = np.concatenate([cos_h, cos_h], axis=N1)
    sin_q = np.concatenate([sin_h, sin_h], axis=N1)
    cos_k = np.concatenate([cos_h, np.ones_like(cos_h)], axis=N1)
    sin_k = np.concatenate([sin_h, np.zeros_like(sin_h)], axis=N1)
    swap = np.eye(LANES)[np.arange(LANES) ^ 32]
    return tuple(jnp.asarray(table, jnp.float32) for table in (cos_q, sin_q, cos_k, sin_k, cos_q.T, sin_q.T)) + (jnp.asarray(swap, jnp.bfloat16),)


def sum_kernel(g_ref, gs_ref, gx_ref, y_ref, below_ref, above_ref, w_out, kv_out, gx_out, y_out, acc, rp, sa, ra1, ra2, sb, rb1, rb2, sc, rc, kvx, gsem, d2s, d2r, ss, rs, cs, cr, ks, kr, xs, xr, lsem, keep):
    f32 = jnp.float32
    bf16 = jnp.bfloat16
    t = lax.axis_index('tp')
    f = lax.axis_index('fsdp')
    c = lax.rem(f, N2)
    yy = lax.rem(lax.div(f, N2), RING)
    zz = lax.div(f, SUB)

    def dev(tt, zc, yc, cc):
        return {'tp': tt, 'fsdp': (zc * RING + yc) * N2 + cc}

    def up(i, d):
        return lax.rem(i + d, RING)

    partner = dev(t, zz, yy, N1 - c)
    xp = [dev(up(t, d), zz, yy, c) for d in range(RING)]
    z_dev = [dev(t, up(zz, d), yy, c) for d in range(RING)]
    y_dev = [dev(t, zz, up(yy, d), c) for d in range(RING)]
    barrier = pltpu.get_barrier_semaphore()
    peers = [partner, xp[N1], xp[N2], xp[N3], z_dev[N1], z_dev[N3], y_dev[N1], y_dev[N3]]
    for peer in peers:
        pl.semaphore_signal(barrier, inc=N1, device_id=peer, device_id_type=MESH_ID)

    def rcopy(src, dst, s_sem, r_sem, peer):
        return pltpu.make_async_remote_copy(src_ref=src, dst_ref=dst, send_sem=s_sem, recv_sem=r_sem, device_id=peer, device_id_type=MESH_ID)

    ring_a = [zz, yy]
    ring_b = [yy, zz]
    dev_a = [z_dev, y_dev]
    dev_b = [y_dev, z_dev]
    order = [N2, N1, N3, N0]

    def g_view(col, j):
        return g_ref.at[N0, :, j] if col == N0 else g_ref.at[N1, :, :, j]

    def gs_view(col, j):
        return gs_ref.at[N0, :, j] if col == N0 else gs_ref.at[N1, :, :, j]

    load = [[None] * RING for _ in range(N2)]
    pair = [[None] * RING for _ in range(N2)]
    for n, d in enumerate(order):
        for col in range(N2):
            j = up(ring_a[col], d)
            load[col][n] = pltpu.make_async_copy(g_view(col, j), acc.at[col, n], gsem.at[col, n])
            load[col][n].start()
    pl.semaphore_wait(barrier, len(peers))
    for n, d in enumerate(order):
        for col in range(N2):
            j = up(ring_a[col], d)
            pair[col][n] = rcopy(gs_view(col, j), rp.at[col, n], d2s.at[col, n], d2r.at[col, n], partner)
            pair[col][n].start()
    mine = gx_ref.shape[N0]
    my_rows = pl.ds(t * mine, mine)
    lower = pl.ds(up(t, N3) * mine, mine)
    upper = pl.ds(up(t, N1) * mine, mine)
    y_up = rcopy(below_ref.at[:, pl.ds(N0, LANES)], y_out.at[lower, pl.ds(N0, LANES)], xs.at[RING], xr.at[RING], xp[N1])
    y_dn = rcopy(above_ref.at[:, pl.ds(LANES, LANES)], y_out.at[upper, pl.ds(LANES, LANES)], xs.at[5], xr.at[5], xp[N3])
    y_up.start()
    y_dn.start()
    x_up = rcopy(gx_ref, gx_out.at[my_rows], xs.at[N0], xr.at[N0], xp[N1])
    x_dn = rcopy(gx_ref, gx_out.at[my_rows], xs.at[N1], xr.at[N1], xp[N3])
    x_up.start()
    x_dn.start()
    local = ((gx_ref, gx_out, my_rows), (y_ref, y_out, my_rows))
    taken = [pltpu.make_async_copy(ref, keep.at[n], lsem.at[n]) for n, (ref, _, _) in enumerate(local)]
    placed = [pltpu.make_async_copy(keep.at[n], out.at[place], lsem.at[n]) for n, (_, out, place) in enumerate(local)]
    for n, (ref, place) in enumerate(((below_ref, lower), (above_ref, upper))):
        placed.append(pltpu.make_async_copy(ref, y_out.at[place], lsem.at[n + N2]))
        placed[n + N2].start()
    for copy in taken:
        copy.start()

    def each(count, body):
        def step(n, carry):
            body(n)
            return carry
        lax.fori_loop(N0, count, step, N0, unroll=N3)

    def arrived(col, n):
        load[col][n].wait()
        pair[col][n].wait_recv()

    sends = []

    def send(src, dst, s_sem, r_sem, peer):
        copy = rcopy(src, dst, s_sem, r_sem, peer)
        copy.start()
        sends.append(copy)
        return copy

    for col in range(N2):
        arrived(col, N0)

        for h, peer in ((N0, N1), (N1, N3)):
            def first(q, col=col, h=h):
                a2 = N2 * h + lax.div(q, 12)
                tt = lax.rem(lax.div(q, N3), RING)
                r = lax.rem(q, N3)
                sa[col, N0, a2, tt, r] = (acc[col, N0, tt, a2, r] + rp[col, N0, tt, a2, r].astype(f32)).astype(bf16)
            each(24, first)
            send(sa.at[col, N0, pl.ds(N2 * h, N2)], ra1.at[col, h], ss.at[col, h], rs.at[col, h], dev_a[col][peer])
    for col in range(N2):
        for n, base, peer in ((N1, N2, N1), (N2, N0, N3)):
            arrived(col, n)

            def plain(q, col=col, n=n, base=base):
                a2 = base + lax.div(q, 12)
                tt = lax.rem(lax.div(q, N3), RING)
                r = lax.rem(q, N3)
                sa[col, n, a2, tt, r] = (acc[col, n, tt, a2, r] + rp[col, n, tt, a2, r].astype(f32)).astype(bf16)
            each(24, plain)
            send(sa.at[col, n, pl.ds(base, N2)], ra2.at[col, n - N1, pl.ds(base, N2)], ss.at[col, n + N1], rs.at[col, n + N1], dev_a[col][peer])
    for col in range(N2):
        for n, base, peer in ((N1, N0, N1), (N2, N2, N3)):
            rcopy(sa.at[col, N0, pl.ds(N0, N2)], ra1.at[col, n - N1], ss.at[col, n - N1], rs.at[col, n - N1], dev_a[col][peer]).wait_recv()

            def joined(q, col=col, n=n, base=base):
                h = lax.div(q, 12)
                a2 = base + h
                tt = lax.rem(lax.div(q, N3), RING)
                r = lax.rem(q, N3)
                val = acc[col, n, tt, a2, r] + rp[col, n, tt, a2, r].astype(f32) + ra1[col, n - N1, h, tt, r].astype(f32)
                sa[col, n, a2, tt, r] = val.astype(bf16)
            each(24, joined)
            send(sa.at[col, n, pl.ds(base, N2)], ra2.at[col, n - N1, pl.ds(base, N2)], ss.at[col, n + N3], rs.at[col, n + N3], dev_a[col][peer])
    for n in range(N2):
        taken[n].wait()
        placed[n].start()
    x_up.wait_recv()
    x_dn.wait_recv()
    half_dn = gx_out.at[lower, pl.ds(N0, LANES)]
    half_up = gx_out.at[upper, pl.ds(LANES, LANES)]
    x_up2 = rcopy(half_dn, half_dn, xs.at[N2], xr.at[N2], xp[N1])
    x_dn2 = rcopy(half_up, half_up, xs.at[N3], xr.at[N3], xp[N3])
    x_up2.start()
    x_dn2.start()
    for col in range(N2):
        arrived(col, N3)
        for n, base, s in ((N1, N2, N2), (N2, N0, N3), (N1, N0, RING), (N2, N2, 5)):
            rcopy(sa.at[col, n, pl.ds(base, N2)], ra2.at[col, n - N1, pl.ds(base, N2)], ss.at[col, s], rs.at[col, s], partner).wait_recv()

        def own(q, col=col):
            a2 = lax.div(q, 12)
            tt = lax.rem(lax.div(q, N3), RING)
            r = lax.rem(q, N3)
            val = acc[col, N3, tt, a2, r] + rp[col, N3, tt, a2, r].astype(f32) + ra2[col, N0, a2, tt, r].astype(f32) + ra2[col, N1, a2, tt, r].astype(f32)
            acc[col, N3, tt, a2, r] = val
        each(48, own)
        far = up(ring_b[col], N2)

        def first_b(q, col=col, far=far):
            tt = lax.div(q, N3)
            r = lax.rem(q, N3)
            sb[col, N0, tt, r] = acc[col, N3, tt, far, r].astype(bf16)
        each(12, first_b)
        send(sb.at[col, N0, pl.ds(N0, N2)], rb1.at[col, N0], ss.at[col, 6], rs.at[col, 6], dev_b[col][N1])
        send(sb.at[col, N0, pl.ds(N2, N2)], rb1.at[col, N1], ss.at[col, 7], rs.at[col, 7], dev_b[col][N3])
        for n, base, peer in ((N1, N2, N1), (N2, N0, N3)):
            pos = up(ring_b[col], peer)

            def plain_b(q, col=col, n=n, base=base, pos=pos):
                tt = base + lax.div(q, N3)
                r = lax.rem(q, N3)
                sb[col, n, tt, r] = acc[col, N3, tt, pos, r].astype(bf16)
            each(6, plain_b)
            send(sb.at[col, n, pl.ds(base, N2)], rb2.at[col, n - N1, pl.ds(base, N2)], ss.at[col, n + 7], rs.at[col, n + 7], dev_b[col][peer])
    for col in range(N2):
        for n, base, peer in ((N1, N0, N1), (N2, N2, N3)):
            rcopy(sb.at[col, N0, pl.ds(N0, N2)], rb1.at[col, n - N1], ss.at[col, n + 5], rs.at[col, n + 5], partner).wait_recv()
            pos = up(ring_b[col], peer)

            def joined_b(q, col=col, n=n, base=base, pos=pos):
                h = lax.div(q, N3)
                tt = base + h
                r = lax.rem(q, N3)
                sb[col, n, tt, r] = (acc[col, N3, tt, pos, r] + rb1[col, n - N1, h, r].astype(f32)).astype(bf16)
            each(6, joined_b)
            send(sb.at[col, n, pl.ds(base, N2)], rb2.at[col, n - N1, pl.ds(base, N2)], ss.at[col, n + 9], rs.at[col, n + 9], dev_b[col][peer])
    for col in range(N2):
        here = ring_b[col]
        for n, base, s in ((N1, N2, SUB), (N2, N0, 9), (N1, N0, 10), (N2, N2, 11)):
            rcopy(sb.at[col, n, pl.ds(base, N2)], rb2.at[col, n - N1, pl.ds(base, N2)], ss.at[col, s], rs.at[col, s], partner).wait_recv()

        def own_b(q, col=col, here=here):
            tt = lax.div(q, N3)
            r = lax.rem(q, N3)
            val = acc[col, N3, tt, here, r] + rb2[col, N0, tt, r].astype(f32) + rb2[col, N1, tt, r].astype(f32)
            acc[col, N3, tt, here, r] = val
            sc[col, tt, r] = val.astype(bf16)
        each(12, own_b)
        for d in (N1, N3, N2):
            to = up(t, d)
            send(sc.at[col, to], rc.at[col, d - N1], cs.at[col, d - N1], cr.at[col, d - N1], xp[d])
        if col == N0:
            def kv_part(q, here=here):
                tt = lax.div(q, N3)
                r = lax.rem(q, N3)
                kvx[t, tt, r] = acc[N0, N3, tt, here, r, :, pl.ds(KV_AT, LANES)]
            each(12, kv_part)
            for d in (N1, N3, N2):
                send(kvx.at[t], kvx.at[t], ks.at[d - N1], kr.at[d - N1], xp[d])
    for col in range(N2):
        here = ring_b[col]
        for d in (N1, N3, N2):
            rcopy(sc.at[col, N0], rc.at[col, d - N1], cs.at[col, d - N1], cr.at[col, d - N1], partner).wait_recv()

        def last(r, col=col, here=here):
            w_out[col, r] = acc[col, N3, t, here, r] + rc[col, N0, r].astype(f32) + rc[col, N1, r].astype(f32) + rc[col, N2, r].astype(f32)
        each(N3, last)
    for d in (N1, N3, N2):
        src = up(t, RING - d)
        rcopy(kvx.at[src], kvx.at[src], ks.at[d - N1], kr.at[d - N1], partner).wait_recv()

    def kv_last(q):
        tt = lax.div(q, N3)
        r = lax.rem(q, N3)
        kv_out[tt, r] = ((kvx[N0, tt, r] + kvx[N1, tt, r]) + kvx[N2, tt, r]) + kvx[N3, tt, r]
    each(12, kv_last)
    for copy in sends:
        copy.wait_send()
    for col in range(N2):
        for n in range(RING):
            pair[col][n].wait_send()
    x_up.wait_send()
    x_dn.wait_send()
    x_up2.wait()
    x_dn2.wait()
    y_up.wait()
    y_dn.wait()
    for copy in placed:
        copy.wait()


def sum_grads(g_pack, g_send, gx_my, y_blocks, n_batch):
    f32 = jnp.float32
    bf16 = jnp.bfloat16
    wide = g_pack.shape[-N1]
    dma = pltpu.SemaphoreType.DMA
    vmem = pl.BlockSpec(memory_space=pltpu.VMEM)
    any_spec = pl.BlockSpec(memory_space=pl.ANY)
    return pl.pallas_call(
        sum_kernel,
        name='sum_grads',
        out_shape=(jax.ShapeDtypeStruct((N2, N3, SUB, wide), f32), jax.ShapeDtypeStruct((RING, N3, SUB, LANES), f32),
                   jax.ShapeDtypeStruct((n_batch,) + gx_my.shape[N1:], bf16), jax.ShapeDtypeStruct((n_batch,) + gx_my.shape[N1:], bf16)),
        in_specs=[any_spec] * RING + [vmem] * N2,
        out_specs=(vmem, vmem, any_spec, any_spec),
        scratch_shapes=[
            pltpu.VMEM((N2, RING, RING, RING, N3, SUB, wide), f32), pltpu.VMEM((N2, RING, RING, RING, N3, SUB, wide), bf16),
            pltpu.VMEM((N2, N3, RING, RING, N3, SUB, wide), bf16), pltpu.VMEM((N2, N2, N2, RING, N3, SUB, wide), bf16), pltpu.VMEM((N2, N2, RING, RING, N3, SUB, wide), bf16),
            pltpu.VMEM((N2, N3, RING, N3, SUB, wide), bf16), pltpu.VMEM((N2, N2, N2, N3, SUB, wide), bf16), pltpu.VMEM((N2, N2, RING, N3, SUB, wide), bf16),
            pltpu.VMEM((N2, RING, N3, SUB, wide), bf16), pltpu.VMEM((N2, N3, N3, SUB, wide), bf16), pltpu.VMEM((RING, RING, N3, SUB, LANES), f32),
            dma((N2, RING)), dma((N2, RING)), dma((N2, RING)), dma((N2, 12)), dma((N2, 12)), dma((N2, N3)), dma((N2, N3)), dma((N3,)), dma((N3,)), dma((6,)), dma((6,)), dma((RING,)), pltpu.VMEM((N2,) + gx_my.shape, bf16),
        ],
        cost_estimate=pl.CostEstimate(flops=60 * 10**9, bytes_accessed=30 * 10**6, transcendentals=N0),
        compiler_params=pltpu.CompilerParams(collective_id=N1, has_side_effects=True, vmem_limit_bytes=60 * KIB * KIB),
    )(g_pack, g_send, gx_my, *y_blocks)


def finish_kernel(w_ref, kv_ref, y_ref, gx_ref, y_out, gx_out, gain_out, q_out, k_out, v_out, o_out, gate_out, up_out, down_out, buf, isem, osem):
    n_batch = y_ref.shape[N0]
    moves = [(ref, out, n) for ref, out in ((y_ref, y_out), (gx_ref, gx_out)) for n in range(n_batch)]
    loads = [pltpu.make_async_copy(ref.at[n], buf.at[m], isem.at[m]) for m, (ref, _, n) in enumerate(moves)]
    stores = [pltpu.make_async_copy(buf.at[m], out.at[n], osem.at[m]) for m, (_, out, n) in enumerate(moves)]
    for copy in loads:
        copy.start()
    lane = lax.broadcasted_iota(jnp.int32, (SUB, LANES), N1)
    gains = []
    for r in range(N3):
        at = slice(SUB * r, SUB * r + SUB)
        gate_out[at, :] = w_ref[N0, r, :, N0:768]
        up_out[at, :] = w_ref[N1, r, :, N0:768]
        q_out[at, :] = w_ref[N0, r, :, 768:960]
        o_out[at, :] = w_ref[N0, r, :, 960:1152]
        down_out[at, N0:LANES] = w_ref[N0, r, :, 1280:1408]
        down_out[at, LANES:768] = w_ref[N1, r, :, 768:1408]
        kv = jnp.where(lane < 32, kv_ref[N0, r], 0.0)
        for n in range(N1, RING):
            kv += pltpu.roll(jnp.where(lane < 32, kv_ref[n, r], 0.0), 32 * n, N1)
        k_out[at, :] = kv[:, N0:64]
        v_out[at, :] = pltpu.roll(kv, 64, N1)[:, N0:64]
        gains.append(jnp.sum(jnp.where(lane == 32, kv_ref[N0, r], 0.0), axis=N1, keepdims=True))
    gain = jnp.concatenate(gains, axis=N0)
    rows = gain.shape[N0]
    diag = lax.broadcasted_iota(jnp.int32, (rows, rows), N0) == lax.broadcasted_iota(jnp.int32, (rows, rows), N1)
    gain_out[ALL] = jnp.sum(jnp.where(diag, jnp.broadcast_to(gain, (rows, rows)), 0.0), axis=N0, keepdims=True)
    for load, store in zip(loads, stores):
        load.wait()
        store.start()
    for store in stores:
        store.wait()


def finish(w_sum, kv_sum, y_land, gx_land, rows, width, nq, head_dim):
    f32 = jnp.float32
    dma = pltpu.SemaphoreType.DMA
    vmem = pl.BlockSpec(memory_space=pltpu.VMEM)
    any_spec = pl.BlockSpec(memory_space=pl.ANY)
    act_t = jax.ShapeDtypeStruct(y_land.shape, y_land.dtype)
    n_moves = N2 * y_land.shape[N0]
    grads = [(N1, rows), (rows, nq), (rows, head_dim), (rows, head_dim), (rows, nq), (rows, width), (rows, width), (rows, width)]
    return pl.pallas_call(
        finish_kernel,
        name='finish',
        out_shape=[act_t, act_t] + [jax.ShapeDtypeStruct(shape, f32) for shape in grads],
        in_specs=[vmem, vmem, any_spec, any_spec],
        out_specs=[any_spec, any_spec] + [vmem] * SUB,
        scratch_shapes=[pltpu.VMEM((n_moves,) + y_land.shape[N1:], y_land.dtype), dma((n_moves,)), dma((n_moves,))],
        compiler_params=pltpu.CompilerParams(vmem_limit_bytes=56 * KIB * KIB),
    )(w_sum, kv_sum, y_land, gx_land)


def solution(mesh):
    n_tp = mesh.shape['tp']

    def device_step(x_in, dy_out, ln_gain, w_q, w_k, w_v, w_o, w_gate, w_up, w_down):
        n_batch, seq_len, width = x_in.shape
        head_dim = w_k.shape[N1]
        rows = w_q.shape[N0]
        nq = w_q.shape[N1]
        mine = n_batch // n_tp
        tp = lax.axis_index('tp')
        core = lax.rem(lax.axis_index('fsdp'), N2)
        full = gather_weights(w_gate, w_q, w_o, w_up, w_down, w_k, w_v, ln_gain).reshape(N2, n_tp, width, -N1)
        wide = full.shape[N3]
        tables = rope_tables(seq_len, head_dim)
        who = jnp.stack([tp, core]).astype(jnp.int32)
        y_tok, gx_tok, g_own, g_oth = layer_step(x_in, dy_out, full, tables, who, seq_len)
        y_my = y_tok.reshape(mine, seq_len, width)
        below = lax.ppermute(y_my, 'tp', [(n, (n + N1) % n_tp) for n in range(n_tp)])
        above = lax.ppermute(y_my, 'tp', [(n, (n - N1) % n_tp) for n in range(n_tp)])
        split = (N2, n_tp, RING, RING, N3, SUB, wide)
        w_sum, kv_sum, gx_land, y_land = sum_grads(g_own.reshape(split), g_oth.reshape(split), gx_tok.reshape(mine, seq_len, width), (y_my, below, above), n_batch)
        y_out, grad_x, gain, grad_wq, grad_wk, grad_wv, wo_t, grad_wgate, grad_wup, down_t = finish(w_sum, kv_sum, y_land, gx_land, rows, width, nq, head_dim)
        return (y_out, grad_x, gain.reshape(rows), grad_wq, grad_wk, grad_wv, wo_t.T, grad_wgate, grad_wup, down_t.T)

    act_spec = P('fsdp', None, None)
    row_spec = P('fsdp', 'tp')
    kv_spec = P('fsdp', None)
    col_spec = P('tp', 'fsdp')
    in_specs = (act_spec, act_spec, P('fsdp'), row_spec, kv_spec, kv_spec, col_spec, row_spec, row_spec, col_spec)
    out_specs = (act_spec, act_spec, P('fsdp'), row_spec, kv_spec, kv_spec, col_spec, row_spec, row_spec, col_spec)
    return jax.shard_map(device_step, mesh=mesh, in_specs=in_specs, out_specs=out_specs, check_vma=False)
```
